32 devices in a mesh: dp: 8 (over y, x, core), mp: 4 (over z).
Axes of the slice: x: 2, y: 2, z: 4, core: 2. Of those that a mesh axis runs over, the one named last changes fastest.
Arguments:
- tokens: bfloat16 [5120, 768], P('dp'), may hold values from -6 to 6
- segment_ids: int32 [8, 640], P('dp'), may hold values from 0 to 3, never falling along the last dimension, each value on 1 to 320 neighbouring positions
- token_types: int32 [8, 640], P('dp'), may hold values 0 or 1
- q_weight: bfloat16 [4, 768, 768], P(None, None, 'mp'), may hold values from -0.21875 to 0.21875
- k_weight: bfloat16 [768, 768], P(None, 'mp'), may hold values from -0.21875 to 0.21875
- v_weight: bfloat16 [768, 768], P(None, 'mp'), may hold values from -0.21875 to 0.21875
- o_weight: bfloat16 [768, 768], P('mp'), may hold values from -2.5 to 2.5
- o_bias: float32 [768], replicated, may hold values from -1.5 to 1.5
- norm1_gain: float32 [768], replicated, may hold values from 0.25 to 1.75
- norm1_shift: float32 [768], replicated, may hold values from -1.5 to 1.5
- in_weight: bfloat16 [768, 3072], P(None, 'mp'), may hold values from -0.21875 to 0.21875
- in_bias: float32 [3072], P('mp'), may hold values from -1.5 to 1.5
- out_weight: bfloat16 [3072, 768], P('mp'), may hold values from -0.109375 to 0.109375
- out_bias: float32 [768], replicated, may hold values from -1.5 to 1.5
- norm2_gain: float32 [768], replicated, may hold values from 0.25 to 1.75
- norm2_shift: float32 [768], replicated, may hold values from -1.5 to 1.5
- cotangent: bfloat16 [5120, 768], P('dp'), may hold values from -6 to 6
Outputs:
- layer_out: bfloat16 [5120, 768], P('dp')
- tokens_grad: bfloat16 [5120, 768], P('dp')
- q_grad: float32 [4, 768, 768], P(None, 'dp', 'mp')
- k_grad: float32 [768, 768], P('dp', 'mp')
- v_grad: float32 [768, 768], P('dp', 'mp')
- o_grad: float32 [768, 768], P('mp', 'dp')
- o_bias_grad: float32 [768], replicated
- norm1_gain_grad: float32 [768], replicated
- norm1_shift_grad: float32 [768], replicated
- in_grad: float32 [768, 3072], P('dp', 'mp')
- in_bias_grad: float32 [3072], P('mp')
- out_grad: float32 [3072, 768], P('mp', 'dp')
- out_bias_grad: float32 [768], replicated
- norm2_gain_grad: float32 [768], replicated
- norm2_shift_grad: float32 [768], replicated
The draws below stay inside these ranges and needn't reach their ends.
Inputs may be any that keep to these rules, and one draw needn't show every extreme that they name: `segment_ids`: a sequence's rows with equal ids form one run.
All inputs are finite; a program needn't handle non-finite values. No bound on the sum of `token_types` on one device may be relied on, other than what follows from the above.
Results may differ from the reference program's by a relative error of at most 0.019.
Values may be sent and summed in bfloat16 or wider, within the bound.
A program may use at most 128 MiB of HBM per device.

```python
import math
import jax
import jax.numpy as jnp
import numpy as np
from jax import lax

D = 768
HEADS = 12
HD = 64
FF = 3072
SEQ_LEN = 640
SEQ_DEV = 1
SEQS = 8
TOKENS = 5120
N_DP = 8


def plant(array, key, least, high):
    extent = array.shape
    index_at = [jax.random.randint(jax.random.fold_in(key, axis), (), 0, extent[axis]) for axis in range(len(extent))]
    array = array.at[tuple(index_at)].set(least)
    longest = extent.index(max(extent))
    index_at[longest] = (index_at[longest] + 1) % extent[longest]
    return array.at[tuple(index_at)].set(high)


def spiked(values, key, source, target, shards_of, factor):
    def block_of(position):
        return (jnp.arange(values.shape[position]) // (values.shape[position] // shards_of)).reshape((-1,) + (1,) * (values.ndim - 1 - position))

    first = jax.random.permutation(key, shards_of)[block_of(target)]
    second = (block_of(target) + shards_of // 2) % shards_of
    return jnp.where((block_of(source) == first) | (block_of(source) == second), factor * values, values)


def levels(stream_key, dims, shards, smallest, top_value):
    level = 1.0
    for dim, parts in shards:
        steps = jax.random.uniform(jax.random.fold_in(jax.random.fold_in(stream_key, 6), dim), (parts,), jnp.float32, smallest / len(shards), top_value / len(shards))
        level = level * jnp.repeat(jnp.exp(steps), dims[dim] // parts).reshape((-1,) + (1,) * (len(dims) - 1 - dim))
    return level


def length_profile(number_of, total, reach, slope):
    loads = [(1 << 20) // math.isqrt(rank ** slope) + 1 for rank in range(2, number_of + 1)]
    surplus, holding = total - reach - (number_of - 1), [1] * (number_of - 1)
    while surplus > 0:
        candidates = [i for i in range(number_of - 1) if holding[i] < reach]
        whole, budget = sum([loads[i] for i in candidates]), surplus
        for i in candidates:
            more = min(reach - holding[i], max(1, budget * loads[i] // whole), surplus)
            holding[i] = holding[i] + more
            surplus = surplus - more
    return np.array([reach] + holding)


def uneven_parts(key, number_of, total, bound, slope):
    if number_of == 2:
        one = jax.random.randint(key, (), max(1, total - bound), min(bound, total - 1) + 1)
        return jnp.stack([one, total - one])
    tallies = jnp.asarray(length_profile(number_of, total, bound, slope), jnp.int32)
    pairs = (number_of - 1) // 2
    donor, receiver = tallies[1:1 + 2 * pairs:2], tallies[2:2 + 2 * pairs:2]
    margin = jnp.minimum(donor - 1, bound - receiver)
    passed = jax.random.randint(jax.random.fold_in(key, 1), (pairs,), 0, 1 << 20) % (margin + 1)
    tallies = tallies.at[1:1 + 2 * pairs:2].set(donor - passed).at[2:2 + 2 * pairs:2].set(receiver + passed)
    return tallies[jax.random.permutation(jax.random.fold_in(key, 2), number_of)]


def noise(stream_key, extent, scale, bound, cuts=(), dtype=jnp.bfloat16):
    level = levels(stream_key, extent, cuts, -0.22, 0.18) if cuts else 1.0
    values = jax.random.normal(stream_key, extent, jnp.float32) * scale * level
    return jnp.minimum(jnp.maximum(values, -bound), bound).astype(dtype)


def bell_draw_with(stream_key, extent, scale, bound, split, heavy, held_as=jnp.bfloat16):
    entries = scale * jax.random.normal(stream_key, extent, jnp.float32)
    if split:
        entries = entries * levels(stream_key, extent, split, -0.22, 0.18)
    return jnp.clip(spiked(entries, jax.random.fold_in(stream_key, 3), *heavy), -bound, bound).astype(held_as)


def setup_inputs(seed: int = 0) -> dict:
    splits = jax.random.split(jax.random.key(seed), 18)
    return {
        "tokens": noise(splits[0], (TOKENS, D), 1.0, 6.0, ((0, 8),)),
        "segment_ids": jax.vmap(lambda own: jnp.searchsorted(jnp.cumsum(uneven_parts(own, 4, SEQ_LEN, SEQ_LEN // 2, 1)), jnp.arange(SEQ_LEN), side="right"))(jax.random.split(splits[1], SEQS)).reshape((SEQS, SEQ_LEN)).astype(jnp.int32),
        "token_types": plant((jax.random.randint(splits[2], (SEQS, SEQ_LEN), 0, 5) < 1).astype(jnp.int32), jax.random.fold_in(splits[2], 1), 0, 1),
        "q_weight": noise(splits[3], (4, D, D), D ** -0.5, 0.21875, ((2, 4),)),
        "k_weight": noise(splits[4], (D, D), D ** -0.5, 0.21875, ((1, 4),)),
        "v_weight": noise(splits[5], (D, D), D ** -0.5, 0.21875, ((1, 4),)),
        "o_weight": noise(splits[6], (D, D), (max(D // 128, 1)) ** -0.5, 2.5, ((0, 4),)),
        "o_bias": noise(splits[7], (D,), 0.3, 1.5, (), jnp.float32),
        "norm1_gain": jnp.clip(1.0 + 0.15 * jax.random.normal(splits[8], (D,), jnp.float32), 0.25, 1.75),
        "norm1_shift": noise(splits[9], (D,), 0.3, 1.5, (), jnp.float32),
        "in_weight": noise(splits[10], (D, FF), D ** -0.5, 0.21875, ((1, 4),)),
        "in_bias": noise(splits[11], (FF,), 0.3, 1.5, ((0, 4),), jnp.float32),
        "out_weight": noise(splits[12], (FF, D), FF ** -0.5, 0.109375, ((0, 4),)),
        "out_bias": noise(splits[13], (D,), 0.3, 1.5, (), jnp.float32),
        "norm2_gain": jnp.clip(1.0 + 0.15 * jax.random.normal(splits[14], (D,), jnp.float32), 0.25, 1.75),
        "norm2_shift": noise(splits[15], (D,), 0.3, 1.5, (), jnp.float32),
        "cotangent": bell_draw_with(splits[16], (TOKENS, D), 1.0, 6.0, ((0, 8),), (0, 1, 8, 2.0)),
    }


@jax.custom_vjp
def low(v):
    return lax.optimization_barrier(v.astype(jnp.bfloat16)).astype(jnp.float32)

@jax.custom_vjp
def low_back(v):
    return v

def low_keep(v):
    return (low(v), None)

def low_pass(kept, grad):
    return (grad,)

def back_keep(v):
    return (v, None)

def back_low(kept, grad):
    return (low(grad),)
low.defvjp(low_keep, low_pass)
low_back.defvjp(back_keep, back_low)
precise = lax.Precision.HIGHEST
norm_epsilon = 1e-05

def matmul(left, right):
    return jnp.dot(left, right, precision=precise, preferred_element_type=jnp.float32)

def layer_norm(inputs, gain, shift):
    average = lax.optimization_barrier(jnp.mean(inputs, axis=-1, keepdims=True))
    centred = inputs - average
    spread = lax.optimization_barrier(jnp.mean(centred * centred, axis=-1, keepdims=True))
    return centred * lax.rsqrt(spread + norm_epsilon) * gain + shift

def forward(weights_all, rows_in, segments, kinds):
    q_weight, k_weight, v_weight, o_weight, o_bias, norm1_gain, norm1_shift, in_weight, in_bias, out_weight, out_bias, norm2_gain, norm2_shift = weights_all
    row_count = rows_in.shape[0]
    groups = segments.shape[0]
    length = segments.shape[1]
    queries = low_back(low(jnp.einsum('rd,tdc->trc', rows_in, q_weight, precision=precise)))
    keys = low_back(low(matmul(rows_in, k_weight)))
    values = low_back(low(matmul(rows_in, v_weight)))
    entity = kinds == 1
    query_four = queries.reshape(4, groups, length, HEADS, HD)
    chooser = entity[:, :, None, None]
    query_word = jnp.where(chooser, query_four[2], query_four[0])
    query_ent = jnp.where(chooser, query_four[3], query_four[1])
    key_heads = keys.reshape(groups, length, HEADS, HD)
    value_heads = values.reshape(groups, length, HEADS, HD)
    raw_word = jnp.einsum('gqhc,gkhc->ghqk', query_word, key_heads, precision=precise)
    raw_ent = jnp.einsum('gqhc,gkhc->ghqk', query_ent, key_heads, precision=precise)
    raw_all = low_back(jnp.where(entity[:, None, None, :], raw_ent, raw_word))
    same_doc = (segments[:, :, None] == segments[:, None, :])[:, None]
    scores = jnp.where(same_doc, raw_all * HD ** (-0.5), -1000000000.0)
    attention = jax.nn.softmax(scores, axis=-1)
    mixed = jnp.einsum('ghqk,gkhc->gqhc', low(attention), value_heads, precision=precise)
    mixed = low_back(low(mixed.reshape(row_count, HEADS * HD)))
    branch = low_back(matmul(mixed, o_weight)) + o_bias
    hidden = layer_norm(rows_in + branch, norm1_gain, norm1_shift)
    inner_pre = low_back(matmul(low(hidden), in_weight)) + in_bias
    activated = low(jax.nn.gelu(inner_pre, approximate=False))
    ffn_out = low_back(matmul(activated, out_weight)) + out_bias
    return layer_norm(hidden + ffn_out, norm2_gain, norm2_shift)

def reference(tokens, segment_ids, token_types, q_weight, k_weight, v_weight, o_weight, o_bias, norm1_gain, norm1_shift, in_weight, in_bias, out_weight, out_bias, norm2_gain, norm2_shift, cotangent):
    weights_all = tuple((w.astype(jnp.float32) for w in (q_weight, k_weight, v_weight, o_weight, o_bias, norm1_gain, norm1_shift, in_weight, in_bias, out_weight, out_bias, norm2_gain, norm2_shift)))
    row_block = SEQ_DEV * SEQ_LEN
    block_tokens = tokens.astype(jnp.float32).reshape(N_DP, row_block, D)
    block_cot = cotangent.astype(jnp.float32).reshape(N_DP, row_block, D)
    block_segs = segment_ids.reshape(N_DP, SEQ_DEV, SEQ_LEN)
    block_kinds = token_types.reshape(N_DP, SEQ_DEV, SEQ_LEN)

    def one_group(totals, pieces):
        rows_in, segments, kinds, grad_out = pieces
        result, pull = jax.vjp(lambda weights_now, rows_now: forward(weights_now, rows_now, segments, kinds), weights_all, rows_in)
        weight_grads, input_grad = pull(grad_out)
        totals = jax.tree.map(lambda first, second: first + second, totals, weight_grads)
        return (totals, (result.astype(jnp.bfloat16), input_grad.astype(jnp.bfloat16)))
    initial = jax.tree.map(jnp.zeros_like, weights_all)
    grads, (outputs, input_grads) = lax.scan(one_group, initial, (block_tokens, block_segs, block_kinds, block_cot))
    layer_out = outputs.reshape(TOKENS, D)
    tokens_grad = input_grads.reshape(TOKENS, D)
    return (layer_out, tokens_grad, grads[0], grads[1], grads[2], grads[3], grads[4], grads[5], grads[6], grads[7], grads[8], grads[9], grads[10], grads[11], grads[12])
```

```python
import functools

import jax
import jax.numpy as jnp
from jax import lax
from jax.experimental import pallas as pl
from jax.experimental.pallas import tpu as pltpu
from jax.sharding import PartitionSpec as P

HD = 64
LINE = 4
VMEM_LIMIT = 60 * 1024 * 1024

norm_epsilon = 1e-05


def remote(src, dst, send_sem, recv_sem, **axes):
    return pltpu.make_async_remote_copy(
        src_ref=src,
        dst_ref=dst,
        send_sem=send_sem,
        recv_sem=recv_sem,
        device_id=axes,
        device_id_type=pl.DeviceIdType.MESH,
    )


class LineReduce:
    def __init__(self, part, carry, single, summed, out, send, recv):
        self.part, self.carry, self.single, self.summed, self.out = part, carry, single, summed, out
        me = lax.axis_index("mp")
        self.me = me
        left = me < 2
        self.is_mid = jnp.logical_or(me == 1, me == 2)
        self.is_end = jnp.logical_not(self.is_mid)
        self.mid = jnp.where(left, 1, 2)
        self.end = jnp.where(left, 0, 3)
        self.far_mid = 3 - self.mid
        self.far_end = 3 - self.end
        self.send, self.recv = send, recv

    def end_sends(self):
        return (
            remote(self.part.at[self.far_end], self.carry.at[0], self.send.at[0], self.recv.at[2], mp=self.mid),
            remote(self.part.at[self.far_mid], self.carry.at[1], self.send.at[1], self.recv.at[3], mp=self.mid),
            remote(self.part.at[self.mid], self.single, self.send.at[2], self.recv.at[0], mp=self.mid),
        )

    def mid_sends(self):
        return (
            remote(self.part.at[self.end], self.single, self.send.at[0], self.recv.at[0], mp=self.end),
            remote(self.carry.at[0], self.summed, self.send.at[1], self.recv.at[1], mp=self.far_end),
            remote(self.carry.at[1], self.summed, self.send.at[2], self.recv.at[1], mp=self.far_mid),
        )

    def gather(self, block, slot, target):
        return remote(self.out.at[block], self.out.at[block], self.send.at[slot], self.recv.at[4 + block], mp=target)

    def start(self):
        @pl.when(self.is_end)
        def _():
            for copy in self.end_sends():
                copy.start()

        @pl.when(self.is_mid)
        def _():
            self.mid_sends()[0].start()

    def forward(self):
        @pl.when(self.is_mid)
        def _():
            sends = self.mid_sends()
            for i, block in ((0, self.far_end), (1, self.far_mid)):
                remote(self.carry.at[i], self.carry.at[i], self.send.at[0], self.recv.at[2 + i], mp=self.end).wait_recv()
                total = self.carry[i].astype(jnp.float32) + self.part[block].astype(jnp.float32)
                self.carry[i] = total.astype(jnp.bfloat16)
                sends[1 + i].start()

    def total(self):
        remote(self.single, self.single, self.send.at[0], self.recv.at[0], mp=self.mid).wait_recv()
        remote(self.summed, self.summed, self.send.at[0], self.recv.at[1], mp=self.mid).wait_recv()
        return (
            self.part[self.me].astype(jnp.float32)
            + self.single[...].astype(jnp.float32)
            + self.summed[...].astype(jnp.float32)
        )

    def spread(self):
        @pl.when(self.is_end)
        def _():
            self.gather(self.me, 3, self.mid).start()

        @pl.when(self.is_mid)
        def _():
            self.gather(self.me, 3, self.end).start()
            self.gather(self.me, 4, self.far_mid).start()

    def wait_block(self, block):
        self.gather(block, 3, self.mid).wait_recv()

    def relay(self):
        @pl.when(self.is_mid)
        def _():
            self.wait_block(self.end)
            self.gather(self.end, 5, self.far_mid).start()
            self.wait_block(self.far_mid)
            self.gather(self.far_mid, 6, self.end).start()
            self.wait_block(self.far_end)
            self.gather(self.far_end, 7, self.end).start()

    def arrive(self):
        @pl.when(self.is_end)
        def _():
            self.wait_block(self.mid)
            self.wait_block(self.far_mid)
            self.wait_block(self.far_end)

    def drain(self):
        @pl.when(self.is_end)
        def _():
            for copy in self.end_sends():
                copy.wait_send()
            self.gather(self.me, 3, self.mid).wait_send()

        @pl.when(self.is_mid)
        def _():
            for copy in self.mid_sends():
                copy.wait_send()
            for slot in range(3, 8):
                self.gather(self.me, slot, self.end).wait_send()


def line_scratch(halves, rows, width):
    block = pltpu.VMEM((halves, rows, width), jnp.bfloat16)
    return [
        pltpu.VMEM((halves, 2, rows, width), jnp.bfloat16),
        block,
        block,
        pltpu.SemaphoreType.DMA((halves, 8)),
        pltpu.SemaphoreType.DMA((halves, 8)),
    ]


def mp_barrier():
    barrier = pltpu.get_barrier_semaphore()
    me = lax.axis_index("mp")
    for step in range(1, LINE):
        pl.semaphore_signal(
            barrier, inc=1, device_id={"mp": lax.rem(me + step, LINE)}, device_id_type=pl.DeviceIdType.MESH
        )
    pl.semaphore_wait(barrier, LINE - 1)


def line_kernel(halves, part, out, carry, single, summed, send, recv):
    mp_barrier()
    lines = [
        LineReduce(part.at[h], carry.at[h], single.at[h], summed.at[h], out.at[h], send.at[h], recv.at[h])
        for h in range(halves)
    ]
    for line in lines:
        line.start()
    for line in lines:
        line.forward()
        out_block = line.total().astype(jnp.bfloat16)
        line.out[line.me] = out_block
        line.spread()
    for line in lines:
        line.relay()
    for line in lines:
        line.arrive()
    for line in lines:
        line.drain()


def line_sum(part, ident):
    rows, width = part.shape
    halves = 2
    block = rows // (halves * LINE)
    part = part.reshape(halves, LINE, block, width)
    out = pl.pallas_call(
        functools.partial(line_kernel, halves),
        out_shape=jax.ShapeDtypeStruct(part.shape, jnp.bfloat16),
        in_specs=[pl.BlockSpec(memory_space=pltpu.VMEM)],
        out_specs=pl.BlockSpec(memory_space=pltpu.VMEM),
        scratch_shapes=line_scratch(halves, block, width),
        compiler_params=pltpu.CompilerParams(
            collective_id=ident, has_side_effects=True, vmem_limit_bytes=VMEM_LIMIT
        ),
    )(part)
    return out.reshape(rows, width)


def plane_kernel(grads, small, out, small_out, sums, r1, mid2, r2a, r2b, s3a, s3b, r3a, r3b, small_in, send, recv):
    dp = lax.axis_index("dp")
    core = lax.rem(dp, 2)
    x = lax.rem(dp // 2, 2)
    y = dp // 4
    across = dp + 1 - 2 * core
    over_x = dp + 2 - 4 * x
    over_y = dp + 4 - 8 * y
    partners = (across, over_x, over_y)
    barrier = pltpu.get_barrier_semaphore()
    for partner in partners:
        pl.semaphore_signal(barrier, inc=1, device_id={"dp": partner}, device_id_type=pl.DeviceIdType.MESH)
    pl.semaphore_wait(barrier, 3)
    half = r2a.shape[2]
    low, high = pl.ds(0, half), pl.ds(half, out.shape[1] - half)

    first = [
        remote(grads.at[2 * k + 1 - core], r1.at[k], send.at[k], recv.at[k], dp=across) for k in range(4)
    ]
    tiny = [
        remote(small_out if s else small, small_in.at[s], send.at[10 + s], recv.at[10 + s], dp=partners[s])
        for s in range(3)
    ]
    for copy in first:
        copy.start()
    tiny[0].start()
    for k in range(4):
        first[k].wait_recv()
        total = grads[2 * k + core].astype(jnp.float32) + r1[k].astype(jnp.float32)
        sums[k] = total
        mid2[k] = total.astype(jnp.bfloat16)
    second = [
        remote(mid2.at[2 * j + 1 - x, :, low], r2a.at[j], send.at[4 + j], recv.at[4 + j], dp=over_x)
        for j in range(2)
    ] + [
        remote(mid2.at[2 * (1 - y) + j, :, high], r2b.at[j], send.at[6 + j], recv.at[6 + j], dp=over_y)
        for j in range(2)
    ]
    for copy in second:
        copy.start()
    tiny[0].wait()
    small_out[...] = small[...] + small_in[0]
    tiny[1].start()
    third = [
        remote(s3a, r3a, send.at[8], recv.at[8], dp=over_y),
        remote(s3b, r3b, send.at[9], recv.at[9], dp=over_x),
    ]
    for copy in second:
        copy.wait_recv()
    s3a[...] = (sums[2 * (1 - y) + x, :, low] + r2a[1 - y].astype(jnp.float32)).astype(jnp.bfloat16)
    third[0].start()
    s3b[...] = (sums[2 * y + 1 - x, :, high] + r2b[1 - x].astype(jnp.float32)).astype(jnp.bfloat16)
    third[1].start()
    tiny[1].wait()
    small_out[...] = small_out[...] + small_in[1]
    tiny[2].start()
    third[0].wait_recv()
    out[:, low] = sums[2 * y + x, :, low] + r2a[y].astype(jnp.float32) + r3a[...].astype(jnp.float32)
    third[1].wait_recv()
    out[:, high] = sums[2 * y + x, :, high] + r2b[x].astype(jnp.float32) + r3b[...].astype(jnp.float32)
    tiny[2].wait()
    small_out[...] = small_out[...] + small_in[2]
    for copy in first + second + third:
        copy.wait_send()


def plane_sum(grads, small, ident):
    blocks, rows, width = grads.shape
    half = (width // 128 + 1) // 2 * 128
    rest = width - half
    low = jnp.bfloat16
    vm = pl.BlockSpec(memory_space=pltpu.VMEM)
    return pl.pallas_call(
        plane_kernel,
        out_shape=(
            jax.ShapeDtypeStruct((rows, width), jnp.float32),
            jax.ShapeDtypeStruct(small.shape, jnp.float32),
        ),
        in_specs=[vm, vm],
        out_specs=(vm, vm),
        scratch_shapes=[
            pltpu.VMEM((4, rows, width), jnp.float32),
            pltpu.VMEM((4, rows, width), low),
            pltpu.VMEM((4, rows, width), low),
            pltpu.VMEM((2, rows, half), low),
            pltpu.VMEM((2, rows, rest), low),
            pltpu.VMEM((rows, half), low),
            pltpu.VMEM((rows, rest), low),
            pltpu.VMEM((rows, half), low),
            pltpu.VMEM((rows, rest), low),
            pltpu.VMEM((3,) + small.shape, jnp.float32),
            pltpu.SemaphoreType.DMA((13,)),
            pltpu.SemaphoreType.DMA((13,)),
        ],
        compiler_params=pltpu.CompilerParams(
            collective_id=ident, has_side_effects=True, vmem_limit_bytes=VMEM_LIMIT
        ),
    )(grads, small)


def layer_norm(inputs, gain, shift):
    average = jnp.mean(inputs, axis=-1, keepdims=True)
    centred = inputs - average
    spread = jnp.mean(centred * centred, axis=-1, keepdims=True)
    return centred * lax.rsqrt(spread + norm_epsilon) * gain + shift


def gelu_exact(inputs):
    return jax.nn.gelu(inputs, approximate=False)


def matmul(left, right):
    return jnp.dot(left, right, preferred_element_type=jnp.float32)


def local(
    tokens,
    segment_ids,
    token_types,
    q_weight,
    k_weight,
    v_weight,
    o_weight,
    o_bias,
    norm1_gain,
    norm1_shift,
    in_weight,
    in_bias,
    out_weight,
    out_bias,
    norm2_gain,
    norm2_shift,
    cotangent,
):
    row_count = tokens.shape[0]
    groups, length = segment_ids.shape
    local_width = k_weight.shape[1]
    head_count = local_width // HD
    score_scale = HD ** (-0.5)
    entity = token_types == 1
    chooser = entity[:, :, None, None]
    key_entity = entity[:, None, None, :]
    same_doc = (segment_ids[:, :, None] == segment_ids[:, None, :])[:, None]
    queries = jnp.einsum(
        "rd,tdc->trc", tokens, q_weight, preferred_element_type=jnp.float32
    ).astype(jnp.bfloat16)
    keys = matmul(tokens, k_weight).astype(jnp.bfloat16)
    values = matmul(tokens, v_weight).astype(jnp.bfloat16)
    query_four = queries.reshape(4, groups, length, head_count, HD)
    query_word = jnp.where(chooser, query_four[2], query_four[0])
    query_ent = jnp.where(chooser, query_four[3], query_four[1])
    key_heads = keys.reshape(groups, length, head_count, HD)
    value_heads = values.reshape(groups, length, head_count, HD)

    def scores_now():
        raw_word = jnp.einsum(
            "gqhc,gkhc->ghqk", query_word, key_heads, preferred_element_type=jnp.float32
        )
        raw_ent = jnp.einsum(
            "gqhc,gkhc->ghqk", query_ent, key_heads, preferred_element_type=jnp.float32
        )
        raw_all = jnp.where(key_entity, raw_ent, raw_word)
        return jnp.where(same_doc, raw_all * score_scale, -1000000000.0)

    scores = scores_now()
    highest = jnp.max(scores, axis=-1, keepdims=True)
    log_total = highest + jnp.log(jnp.sum(jnp.exp(scores - highest), axis=-1, keepdims=True))
    attention_low = jnp.exp(scores - log_total).astype(jnp.bfloat16)
    mixed = jnp.einsum(
        "ghqk,gkhc->gqhc", attention_low, value_heads, preferred_element_type=jnp.float32
    )
    mixed = mixed.reshape(row_count, local_width).astype(jnp.bfloat16)
    token_wide = tokens.astype(jnp.float32)
    branch = line_sum(matmul(mixed, o_weight).astype(jnp.bfloat16), 0).astype(jnp.float32) + o_bias
    hidden, norm1_pull = jax.vjp(layer_norm, token_wide + branch, norm1_gain, norm1_shift)
    hidden_low = hidden.astype(jnp.bfloat16)
    inner_pre = matmul(hidden_low, in_weight) + in_bias
    activated, gelu_pull = jax.vjp(gelu_exact, inner_pre)
    activated_low = activated.astype(jnp.bfloat16)
    ffn_out = (
        line_sum(matmul(activated_low, out_weight).astype(jnp.bfloat16), 0).astype(jnp.float32)
        + out_bias
    )
    result, norm2_pull = jax.vjp(layer_norm, hidden + ffn_out, norm2_gain, norm2_shift)
    layer_out = result.astype(jnp.bfloat16)
    d_res2, d_gain2, d_shift2 = norm2_pull(cotangent.astype(jnp.float32))
    d_out_bias = jnp.sum(d_res2, axis=0)
    grad_ffn = d_res2.astype(jnp.bfloat16)
    d_out_weight = matmul(grad_ffn.T, activated_low)
    (d_inner,) = gelu_pull(matmul(grad_ffn, out_weight.T))
    d_in_bias = jnp.sum(d_inner, axis=0)
    inner_low = d_inner.astype(jnp.bfloat16)
    d_in_weight = matmul(hidden_low.T, inner_low)
    d_hidden = d_res2 + line_sum(matmul(inner_low, in_weight.T).astype(jnp.bfloat16), 0).astype(
        jnp.float32
    )
    d_res1, d_gain1, d_shift1 = norm1_pull(d_hidden)
    d_o_bias = jnp.sum(d_res1, axis=0)
    grad_branch = d_res1.astype(jnp.bfloat16)
    d_o_weight = matmul(grad_branch.T, mixed)
    d_mixed = matmul(grad_branch, o_weight.T).astype(jnp.bfloat16)
    mixed_heads = d_mixed.reshape(groups, length, head_count, HD)
    attention = jnp.exp(scores_now() - log_total)
    d_probs = jnp.einsum(
        "gqhc,gkhc->ghqk", mixed_heads, value_heads, preferred_element_type=jnp.float32
    )
    d_values = jnp.einsum(
        "ghqk,gqhc->gkhc",
        attention.astype(jnp.bfloat16),
        mixed_heads,
        preferred_element_type=jnp.float32,
    )
    row_delta = jnp.sum(attention * d_probs, axis=-1, keepdims=True)
    d_raw = (attention * (d_probs - row_delta) * score_scale).astype(jnp.bfloat16)
    nothing = jnp.zeros_like(d_raw)
    raw_word = jnp.where(key_entity, nothing, d_raw)
    raw_ent = jnp.where(key_entity, d_raw, nothing)
    d_query_word = jnp.einsum(
        "ghqk,gkhc->gqhc", raw_word, key_heads, preferred_element_type=jnp.float32
    )
    d_query_ent = jnp.einsum(
        "ghqk,gkhc->gqhc", raw_ent, key_heads, preferred_element_type=jnp.float32
    )
    d_keys = jnp.einsum(
        "ghqk,gqhc->gkhc", raw_word, query_word, preferred_element_type=jnp.float32
    ) + jnp.einsum("ghqk,gqhc->gkhc", raw_ent, query_ent, preferred_element_type=jnp.float32)
    empty_rows = jnp.zeros_like(d_query_word)
    d_queries = (
        jnp.stack(
            [
                jnp.where(chooser, empty_rows, d_query_word),
                jnp.where(chooser, empty_rows, d_query_ent),
                jnp.where(chooser, d_query_word, empty_rows),
                jnp.where(chooser, d_query_ent, empty_rows),
            ]
        )
        .reshape(4, row_count, local_width)
        .astype(jnp.bfloat16)
    )
    d_keys_low = d_keys.reshape(row_count, local_width).astype(jnp.bfloat16)
    d_values_low = d_values.reshape(row_count, local_width).astype(jnp.bfloat16)
    d_q_weight = jnp.einsum("rd,trc->tdc", tokens, d_queries, preferred_element_type=jnp.float32)
    d_k_weight = matmul(tokens.T, d_keys_low)
    d_v_weight = matmul(tokens.T, d_values_low)
    total = jnp.einsum("trc,tdc->rd", d_queries, q_weight, preferred_element_type=jnp.float32)
    total = total + matmul(d_keys_low, k_weight.T) + matmul(d_values_low, v_weight.T)
    total = total + d_res1 * 0.25
    tokens_grad = line_sum(total.astype(jnp.bfloat16), 0)
    small = (d_o_bias, d_gain1, d_shift1, d_in_bias, d_out_bias, d_gain2, d_shift2)
    n_dp = lax.axis_size("dp")
    if n_dp == 8:
        width = tokens.shape[1]
        pieces = [d_q_weight[t] for t in range(4)] + [d_k_weight, d_v_weight, d_o_weight, d_in_weight, d_out_weight]
        sizes = [p.shape[1] for p in pieces]
        packed = jnp.concatenate([p.astype(jnp.bfloat16) for p in pieces], axis=1)
        packed = jnp.pad(packed, ((0, 0), (0, -packed.shape[1] % 128)))
        packed = packed.reshape(n_dp, width // n_dp, packed.shape[1])
        small = jnp.stack(list(small) + [jnp.zeros_like(small[0])])
        packed, small = plane_sum(packed, small, 1)
        small = tuple(small[i] for i in range(7))
        pieces, at = [], 0
        for size in sizes:
            pieces.append(packed[:, at : at + size])
            at += size
        d_q_weight = jnp.stack(pieces[:4])
        d_k_weight, d_v_weight, d_o_weight, d_in_weight, d_out_weight = pieces[4:]
        d_o_weight, d_out_weight = d_o_weight.T, d_out_weight.T
    else:
        d_q_weight = lax.psum_scatter(d_q_weight, "dp", scatter_dimension=1, tiled=True)
        d_k_weight = lax.psum_scatter(d_k_weight, "dp", scatter_dimension=0, tiled=True)
        d_v_weight = lax.psum_scatter(d_v_weight, "dp", scatter_dimension=0, tiled=True)
        d_o_weight = lax.psum_scatter(d_o_weight.T, "dp", scatter_dimension=1, tiled=True)
        d_in_weight = lax.psum_scatter(d_in_weight, "dp", scatter_dimension=0, tiled=True)
        d_out_weight = lax.psum_scatter(d_out_weight.T, "dp", scatter_dimension=1, tiled=True)
        small = lax.psum(small, "dp")
    d_o_bias, d_gain1, d_shift1, d_in_bias, d_out_bias, d_gain2, d_shift2 = small
    return (
        layer_out,
        tokens_grad,
        d_q_weight,
        d_k_weight,
        d_v_weight,
        d_o_weight,
        d_o_bias,
        d_gain1,
        d_shift1,
        d_in_weight,
        d_in_bias,
        d_out_weight,
        d_out_bias,
        d_gain2,
        d_shift2,
    )


def solution(mesh):
    return jax.shard_map(
        local,
        mesh=mesh,
        in_specs=(
            P("dp", None),
            P("dp", None),
            P("dp", None),
            P(None, None, "mp"),
            P(None, "mp"),
            P(None, "mp"),
            P("mp", None),
            P(),
            P(),
            P(),
            P(None, "mp"),
            P("mp"),
            P("mp", None),
            P(),
            P(),
            P(),
            P("dp", None),
        ),
        out_specs=(
            P("dp", None),
            P("dp", None),
            P(None, "dp", "mp"),
            P("dp", "mp"),
            P("dp", "mp"),
            P("mp", "dp"),
            P(),
            P(),
            P(),
            P("dp", "mp"),
            P("mp"),
            P("mp", "dp"),
            P(),
            P(),
            P(),
        ),
        check_vma=False,
    )
```

```python
import functools
import math
import operator
import types

import jax
import jax.numpy as jnp
from jax import lax
from jax.experimental import pallas as pl
from jax.experimental.pallas import tpu as pltpu
from jax.sharding import PartitionSpec as P

HD = 64
LINE = 4
HALVES = 2
CHUNK = 32
VMEM_LIMIT = 67043328

norm_epsilon = 1e-05


def remote(src, dst, send_sem, recv_sem, **axes):
    return pltpu.make_async_remote_copy(
        src_ref=src,
        dst_ref=dst,
        send_sem=send_sem,
        recv_sem=recv_sem,
        device_id=axes,
        device_id_type=pl.DeviceIdType.MESH,
    )


class LineReduce:
    def __init__(self, part, carry, single, summed, out, send, recv):
        self.part, self.carry, self.single, self.summed, self.out = part, carry, single, summed, out
        me = lax.axis_index("mp")
        self.me = me
        left = me < 2
        self.is_mid = jnp.logical_or(me == 1, me == 2)
        self.is_end = jnp.logical_not(self.is_mid)
        self.mid = jnp.where(left, 1, 2)
        self.end = jnp.where(left, 0, 3)
        self.far_mid = 3 - self.mid
        self.far_end = 3 - self.end
        self.send, self.recv = send, recv

    def end_sends(self):
        return (
            remote(self.part.at[self.far_end], self.carry.at[0], self.send.at[0], self.recv.at[2], mp=self.mid),
            remote(self.part.at[self.far_mid], self.carry.at[1], self.send.at[1], self.recv.at[3], mp=self.mid),
            remote(self.part.at[self.mid], self.single, self.send.at[2], self.recv.at[0], mp=self.mid),
        )

    def mid_sends(self):
        return (
            remote(self.part.at[self.end], self.single, self.send.at[0], self.recv.at[0], mp=self.end),
            remote(self.carry.at[0], self.summed, self.send.at[1], self.recv.at[1], mp=self.far_end),
            remote(self.carry.at[1], self.summed, self.send.at[2], self.recv.at[1], mp=self.far_mid),
        )

    def gather(self, block, slot, target):
        return remote(self.out.at[block], self.out.at[block], self.send.at[slot], self.recv.at[4 + block], mp=target)

    def start(self):
        @pl.when(self.is_end)
        def _():
            for copy in self.end_sends():
                copy.start()

        @pl.when(self.is_mid)
        def _():
            self.mid_sends()[0].start()

    def forward(self):
        @pl.when(self.is_mid)
        def _():
            sends = self.mid_sends()
            for i, block in ((0, self.far_end), (1, self.far_mid)):
                remote(self.carry.at[i], self.carry.at[i], self.send.at[0], self.recv.at[2 + i], mp=self.end).wait_recv()
                total = self.carry[i].astype(jnp.float32) + self.part[block].astype(jnp.float32)
                self.carry[i] = total.astype(jnp.bfloat16)
                sends[1 + i].start()

    def total(self):
        remote(self.single, self.single, self.send.at[0], self.recv.at[0], mp=self.mid).wait_recv()
        remote(self.summed, self.summed, self.send.at[0], self.recv.at[1], mp=self.mid).wait_recv()
        return (
            self.part[self.me].astype(jnp.float32)
            + self.single[...].astype(jnp.float32)
            + self.summed[...].astype(jnp.float32)
        )

    def spread(self):
        @pl.when(self.is_end)
        def _():
            self.gather(self.me, 3, self.mid).start()

        @pl.when(self.is_mid)
        def _():
            self.gather(self.me, 3, self.end).start()
            self.gather(self.me, 4, self.far_mid).start()

    def wait_block(self, block):
        self.gather(block, 3, self.mid).wait_recv()

    def relay(self):
        @pl.when(self.is_mid)
        def _():
            self.wait_block(self.end)
            self.gather(self.end, 5, self.far_mid).start()
            self.wait_block(self.far_mid)
            self.gather(self.far_mid, 6, self.end).start()
            self.wait_block(self.far_end)
            self.gather(self.far_end, 7, self.end).start()

    def arrive(self):
        @pl.when(self.is_end)
        def _():
            self.wait_block(self.mid)
            self.wait_block(self.far_mid)
            self.wait_block(self.far_end)

    def drain(self):
        @pl.when(self.is_end)
        def _():
            for copy in self.end_sends():
                copy.wait_send()
            self.gather(self.me, 3, self.mid).wait_send()

        @pl.when(self.is_mid)
        def _():
            for copy in self.mid_sends():
                copy.wait_send()
            for slot in range(3, 8):
                self.gather(self.me, slot, self.end).wait_send()


def line_scratch(rows, width):
    block = pltpu.VMEM((HALVES, rows, width), jnp.bfloat16)
    return [
        pltpu.VMEM((HALVES, LINE, rows, width), jnp.bfloat16),
        pltpu.VMEM((HALVES, 2, rows, width), jnp.bfloat16),
        block,
        block,
        pltpu.SemaphoreType.DMA((HALVES, 8)),
        pltpu.SemaphoreType.DMA((HALVES, 8)),
    ]


class LineGather:
    def __init__(self, place, send, recv, out):
        self.place, self.send, self.recv, self.out = place, send, recv, out

    def copy(self, block, slot, target):
        return remote(self.out(block), self.out(block), self.send.at[slot], self.recv.at[block], mp=target)

    def spread(self):
        at = self.place

        @pl.when(at.is_end)
        def _():
            self.copy(at.me, 0, at.mid).start()

        @pl.when(at.is_mid)
        def _():
            self.copy(at.me, 0, at.end).start()
            self.copy(at.me, 1, at.far_mid).start()

    def relay(self):
        at = self.place

        @pl.when(at.is_mid)
        def _():
            self.copy(at.end, 2, at.far_mid).wait_recv()
            self.copy(at.end, 2, at.far_mid).start()
            self.copy(at.far_mid, 3, at.end).wait_recv()
            self.copy(at.far_mid, 3, at.end).start()
            self.copy(at.far_end, 4, at.end).wait_recv()
            self.copy(at.far_end, 4, at.end).start()

    def arrive(self):
        at = self.place

        @pl.when(at.is_end)
        def _():
            self.copy(at.mid, 0, at.mid).wait_recv()
            self.copy(at.far_mid, 0, at.mid).wait_recv()
            self.copy(at.far_end, 0, at.mid).wait_recv()

    def drain(self):
        at = self.place

        @pl.when(at.is_end)
        def _():
            self.copy(at.me, 0, at.mid).wait_send()

        @pl.when(at.is_mid)
        def _():
            for slot in range(5):
                self.copy(at.me, slot, at.end).wait_send()


class Place:
    def __init__(self):
        me = lax.axis_index("mp")
        self.me = me
        self.is_mid = jnp.logical_or(me == 1, me == 2)
        self.is_end = jnp.logical_not(self.is_mid)
        left = me < 2
        self.mid = jnp.where(left, 1, 2)
        self.end = jnp.where(left, 0, 3)
        self.far_mid = 3 - self.mid
        self.far_end = 3 - self.end


class PlaneReduce:
    def __init__(self, grads, r1, sums, mid2, r2a, r2b, s3a, s3b, r3a, r3b, send, recv):
        self.grads, self.r1, self.sums, self.mid2 = grads, r1, sums, mid2
        self.r2a, self.r2b, self.s3a, self.s3b, self.r3a, self.r3b = r2a, r2b, s3a, s3b, r3a, r3b
        dp = lax.axis_index("dp")
        self.core, self.x, self.y = lax.rem(dp, 2), lax.rem(dp // 2, 2), dp // 4
        across = dp + 1 - 2 * self.core
        over_x = dp + 2 - 4 * self.x
        over_y = dp + 4 - 8 * self.y
        half = r2a.shape[2]
        self.low, self.high = pl.ds(0, half), pl.ds(half, grads.shape[2] - half)
        self.first = [
            remote(grads.at[2 * k + 1 - self.core], r1.at[k], send.at[k], recv.at[k], dp=across) for k in range(4)
        ]
        self.second = [
            remote(mid2.at[2 * j + 1 - self.x, :, self.low], r2a.at[j], send.at[4 + j], recv.at[4 + j], dp=over_x)
            for j in range(2)
        ] + [
            remote(mid2.at[2 * (1 - self.y) + j, :, self.high], r2b.at[j], send.at[6 + j], recv.at[6 + j], dp=over_y)
            for j in range(2)
        ]
        self.third = [
            remote(s3a, r3a, send.at[8], recv.at[8], dp=over_y),
            remote(s3b, r3b, send.at[9], recv.at[9], dp=over_x),
        ]

    def start(self):
        for copy in self.first:
            copy.start()

    def step_one(self):
        for copy in self.first:
            copy.wait_recv()

        def body(k, carry):
            total = self.grads[2 * k + self.core].astype(jnp.float32) + self.r1[k].astype(jnp.float32)
            self.sums[k] = total
            self.mid2[k] = total.astype(jnp.bfloat16)
            return carry

        lax.fori_loop(0, 4, body, 0)
        for copy in self.second:
            copy.start()

    def step_two(self):
        for copy in self.second:
            copy.wait_recv()
        x, y = self.x, self.y
        self.s3a[...] = (
            self.sums[2 * (1 - y) + x, :, self.low] + self.r2a[1 - y].astype(jnp.float32)
        ).astype(jnp.bfloat16)
        self.third[0].start()
        self.s3b[...] = (
            self.sums[2 * y + 1 - x, :, self.high] + self.r2b[1 - x].astype(jnp.float32)
        ).astype(jnp.bfloat16)
        self.third[1].start()

    def finish(self):
        x, y = self.x, self.y
        for copy in self.third:
            copy.wait_recv()
        own = self.sums.at[2 * y + x]
        own[:, self.low] = own[:, self.low] + self.r2a[y].astype(jnp.float32) + self.r3a[...].astype(jnp.float32)
        own[:, self.high] = own[:, self.high] + self.r2b[x].astype(jnp.float32) + self.r3b[...].astype(jnp.float32)
        for copy in self.first + self.second + self.third:
            copy.wait_send()
        return own


def plane_scratch(rows, width):
    half = (width // 128 + 1) // 2 * 128
    rest = width - half
    low = jnp.bfloat16
    return [
        pltpu.VMEM((4, rows, width), low),
        pltpu.VMEM((4, rows, width), jnp.float32),
        pltpu.VMEM((4, rows, width), low),
        pltpu.VMEM((2, rows, half), low),
        pltpu.VMEM((2, rows, rest), low),
        pltpu.VMEM((rows, half), low),
        pltpu.VMEM((rows, rest), low),
        pltpu.VMEM((rows, half), low),
        pltpu.VMEM((rows, rest), low),
        pltpu.SemaphoreType.DMA((10,)),
        pltpu.SemaphoreType.DMA((10,)),
    ]


def dot(left, right, left_dim=1, right_dim=0):
    return lax.dot_general(
        left, right, (((left_dim,), (right_dim,)), ((), ())), preferred_element_type=jnp.float32
    )


def rows_loop(start, count, body):
    def step(i, carry):
        body(pl.ds(pl.multiple_of(start + i * CHUNK, CHUNK), CHUNK))
        return carry

    lax.fori_loop(0, count // CHUNK, step, 0)


def fold(value):
    return jnp.sum(value.reshape(value.shape[0] // 8, 8, value.shape[1]), axis=0)


def row_mean(value):
    return jnp.mean(value, axis=-1, keepdims=True)


def layer_kernel(planar, layout, *refs):
    r = types.SimpleNamespace(**functools.reduce(operator.or_, jax.tree.unflatten(layout, refs)))
    tokens, rows, width = r.tokens, r.tokens.shape[0], r.tokens.shape[1]
    local_width = r.k_weight.shape[0]
    heads = local_width // HD
    pair = 2 * HD
    hidden_width = r.in_weight.shape[1]
    half_rows = rows // HALVES
    block_rows = half_rows // LINE
    low, wide = jnp.bfloat16, jnp.float32
    at = Place()
    me = at.me
    dp = lax.axis_index("dp")
    core = lax.rem(dp, 2)
    across = dp + 1 - 2 * core

    barrier = pltpu.get_barrier_semaphore()
    peers = [{"mp": lax.rem(me + step, LINE)} for step in range(1, LINE)] + [{"dp": across}]
    if planar:
        x, y = lax.rem(dp // 2, 2), dp // 4
        over_x, over_y = dp + 2 - 4 * x, dp + 4 - 8 * y
        peers += [{"dp": over_x}, {"dp": over_y}]
    for peer in peers:
        pl.semaphore_signal(barrier, inc=1, device_id=peer, device_id_type=pl.DeviceIdType.MESH)
    pl.semaphore_wait(barrier, len(peers))

    ow, ow_send, ow_recv = r.ow, r.ow_send, r.ow_recv
    share = local_width // 2
    mine, other = pl.ds(core * share, share), pl.ds((1 - core) * share, share)
    ow_line = []
    for step in range(1, LINE):
        ow_line.append(
            remote(
                r.o_weight.at[mine],
                ow.at[me, mine],
                ow_send.at[step - 1],
                ow_recv.at[step - 1],
                mp=lax.rem(me + step, LINE),
            )
        )
    for copy in ow_line:
        copy.start()
    ow_swap = []
    for step in range(1, LINE):
        source = lax.rem(me + LINE - step, LINE)
        ow_swap.append(
            remote(ow.at[source, mine], ow.at[source, mine], ow_send.at[2 + step], ow_recv.at[2 + step], dp=across)
        )

    wa, wb, wk = r.wa, r.wb, r.wk
    for h in range(heads):
        cols = slice(h * HD, (h + 1) * HD)
        both = slice(h * pair, (h + 1) * pair)
        wa[both, :] = jnp.concatenate([r.q_weight[0, cols, :], r.q_weight[1, cols, :]], axis=0)
        wb[both, :] = jnp.concatenate([r.q_weight[2, cols, :], r.q_weight[3, cols, :]], axis=0)
        key_part = r.k_weight[cols, :]
        wk[both, :] = jnp.concatenate([key_part, key_part], axis=0)
    kind_wide, seg_wide = r.kind_wide, r.seg_wide
    kind_wide[...] = jnp.broadcast_to(r.kind_col[...], kind_wide.shape)
    seg_wide[...] = jnp.broadcast_to(r.seg_col[...], seg_wide.shape)
    qcat, kcat, vt = r.qcat, r.kcat, r.vt
    tok = tokens[...]
    q_plain = dot(tok, wa[...], 1, 1)
    q_entity = dot(tok, wb[...], 1, 1)
    entity = kind_wide[...] == 1
    upper = lax.broadcasted_iota(jnp.int32, (rows, pair), 1) >= HD
    for h in range(heads):
        both = slice(h * pair, (h + 1) * pair)
        qcat[:, both] = jnp.where(entity, q_entity[:, both], q_plain[:, both]).astype(low)
    keys = dot(tok, wk[...], 1, 1)
    for h in range(heads):
        both = slice(h * pair, (h + 1) * pair)
        kcat[:, both] = jnp.where(entity == upper, keys[:, both], 0.0).astype(low)
    vt[...] = dot(r.v_weight[...], tok, 1, 1).astype(low)

    st, pt, mx = r.st, r.pt, r.mx
    gathers = []
    scale = HD ** (-0.5)
    lane_tiles = rows // 128
    for h in range(heads):
        both = slice(h * pair, (h + 1) * pair)
        st[...] = dot(kcat[:, both], qcat[:, both], 1, 1)

        def soften(i, carry, h=h):
            cols = pl.ds(pl.multiple_of(i * 128, 128), 128)
            scores = jnp.where(seg_wide[...] == r.seg_row[:, cols], st[:, cols] * scale, -1000000000.0)
            shifted = jnp.exp(scores - jnp.max(scores, axis=0, keepdims=True))
            total = jnp.sum(shifted, axis=0, keepdims=True)
            pt[h, :, cols] = (shifted * (1.0 / total)).astype(low)
            return carry

        lax.fori_loop(0, lane_tiles, soften, 0)
        mx[me, h] = dot(vt[h * HD : (h + 1) * HD, :], pt[h]).astype(low)
        gather = LineGather(at, r.mx_send.at[h], r.mx_recv.at[h], lambda block, h=h: mx.at[block, h])
        gathers.append(gather)
        gather.spread()
        if h:
            gathers[h - 1].relay()
    for copy in ow_line:
        copy.wait_recv()
    for copy in ow_swap:
        copy.start()
    ow[me] = r.o_weight[...]
    tok_t = r.tok_t
    tok_t[...] = tokens[...].T
    gathers[-1].relay()
    for gather in gathers:
        gather.arrive()
    for copy in ow_swap:
        copy.wait_recv()

    xh1, rstd1, hl = r.xh1, r.rstd1, r.hl
    xh1[...] = dot(mx[...].reshape(LINE * local_width, rows), ow[...].reshape(LINE * local_width, width), 0, 0)

    def first_norm(at_rows):
        value = xh1[at_rows, :] + tokens[at_rows, :].astype(wide) + r.o_bias[...]
        centred = value - row_mean(value)
        scaled = lax.rsqrt(row_mean(centred * centred) + norm_epsilon)
        normal = centred * scaled
        xh1[at_rows, :] = normal
        rstd1[at_rows, :] = jnp.broadcast_to(scaled, (CHUNK, 128))
        hl[at_rows, :] = (normal * r.gain1[...] + r.shift1[...]).astype(low)

    act, gp, dr2, gf, il, tmp = r.act, r.gp, r.dr2, r.gf, r.il, r.tmp
    acc = r.acc
    acc[...] = jnp.zeros_like(acc)

    def make_lines(parts, out):
        part, carry, single, summed, send, recv = parts
        return [
            LineReduce(part.at[h], carry.at[h], single.at[h], summed.at[h], out.at[h], send.at[h], recv.at[h])
            for h in range(HALVES)
        ]

    ffn = make_lines(r.ffn, r.ffn_out)
    back = make_lines(r.back, r.back_out)
    grad = make_lines(r.grad, r.tokens_grad)

    def put_part(line, value):
        line.part[...] = value.astype(low).reshape(line.part.shape)

    root_half = math.sqrt(0.5)
    density = 1.0 / math.sqrt(2.0 * math.pi)

    def forward_half(h):
        here = pl.ds(h * half_rows, half_rows)
        rows_loop(h * half_rows, half_rows, first_norm)
        gp[here, :] = dot(hl[here, :], r.in_weight[...])

        def activate(at_rows):
            inner = gp[at_rows, :] + r.in_bias[...]
            gate = 0.5 + 0.5 * lax.erf(inner * root_half)
            act[at_rows, :] = (inner * gate).astype(low)
            gp[at_rows, :] = gate + inner * (density * jnp.exp(-0.5 * inner * inner))

        rows_loop(h * half_rows, half_rows, activate)
        put_part(ffn[h], dot(act[here, :], r.out_weight[...]))
        ffn[h].start()

    def settle(line):
        line.forward()
        line.out[me] = line.total().astype(low)
        line.spread()

    def backward_half(h):
        here = pl.ds(h * half_rows, half_rows)
        start = h * half_rows

        def second_norm(at_rows, from_rows):
            value = xh1[at_rows, :] * r.gain1[...] + r.shift1[...]
            value = value + tmp[from_rows, :] + r.out_bias[...]
            centred = value - row_mean(value)
            scaled = lax.rsqrt(row_mean(centred * centred) + norm_epsilon)
            normal = centred * scaled
            r.layer_out[at_rows, :] = (normal * r.gain2[...] + r.shift2[...]).astype(low)
            cot = r.cotangent[at_rows, :].astype(wide)
            acc[6] += fold(cot)
            acc[5] += fold(cot * normal)
            inside = cot * r.gain2[...]
            grad_in = scaled * (inside - row_mean(inside) - normal * row_mean(inside * normal))
            acc[4] += fold(grad_in)
            dr2[at_rows, :] = grad_in
            gf[at_rows, :] = grad_in.astype(low)

        def norm_step(i, carry):
            at_rows = pl.ds(pl.multiple_of(start + i * CHUNK, CHUNK), CHUNK)
            from_rows = pl.ds(pl.multiple_of(i * CHUNK, CHUNK), CHUNK)
            second_norm(at_rows, from_rows)
            return carry

        tmp[...] = ffn[h].out[...].reshape(half_rows, width).astype(wide)
        lax.fori_loop(0, half_rows // CHUNK, norm_step, 0)
        tmp[...] = dot(gf[here, :], r.out_weight[...], 1, 1)

        def inner_step(i, carry):
            at_rows = pl.ds(pl.multiple_of(start + i * CHUNK, CHUNK), CHUNK)
            from_rows = pl.ds(pl.multiple_of(i * CHUNK, CHUNK), CHUNK)
            d_inner = tmp[from_rows, :] * gp[at_rows, :]
            acc[3] += fold(d_inner)
            il[at_rows, :] = d_inner.astype(low)
            return carry

        lax.fori_loop(0, half_rows // CHUNK, inner_step, 0)
        put_part(back[h], dot(il[here, :], r.in_weight[...], 1, 1))
        back[h].start()

    gb = r.gb

    def last_norm(h):
        start = h * half_rows

        def step(i, carry):
            at_rows = pl.ds(pl.multiple_of(start + i * CHUNK, CHUNK), CHUNK)
            from_rows = pl.ds(pl.multiple_of(i * CHUNK, CHUNK), CHUNK)
            d_hidden = dr2[at_rows, :] + tmp[from_rows, :]
            normal = xh1[at_rows, :]
            acc[2] += fold(d_hidden)
            acc[1] += fold(d_hidden * normal)
            inside = d_hidden * r.gain1[...]
            grad_in = rstd1[at_rows, 0:1] * (inside - row_mean(inside) - normal * row_mean(inside * normal))
            acc[0] += fold(grad_in)
            dr2[at_rows, :] = grad_in
            gb[at_rows, :] = grad_in.astype(low)
            return carry

        tmp[...] = back[h].out[...].reshape(half_rows, width).astype(wide)
        lax.fori_loop(0, half_rows // CHUNK, step, 0)

    gfeed, gattn = r.gfeed, r.gattn
    blocks, per_block = gfeed.shape[0], gfeed.shape[1]

    def put_grad(packed, start, value):
        packed[:, :, start : start + value.shape[1]] = value.astype(low).reshape(blocks, per_block, value.shape[1])

    forward_half(0)
    forward_half(1)
    settle(ffn[0])
    settle(ffn[1])
    ffn[0].relay()
    ffn[0].arrive()
    backward_half(0)
    ffn[1].relay()
    ffn[1].arrive()
    backward_half(1)
    settle(back[0])
    put_grad(gfeed, hidden_width, dot(gf[...], act[...], 0, 0))
    settle(back[1])
    back[0].relay()
    put_grad(gfeed, 0, dot(hl[...], il[...], 0, 0))
    if planar:
        feed = PlaneReduce(gfeed, *r.feed)
        feed.start()
    back[0].arrive()
    last_norm(0)
    back[1].relay()
    back[1].arrive()
    last_norm(1)

    small = r.small
    for i in range(8):
        small[i : i + 1, :] = jnp.sum(acc[i], axis=0, keepdims=True)
    if planar:
        small_in, partners = r.small_in, (across, over_x, over_y)
        small_sum = r.small_sum
        tiny = [
            remote(
                small if s == 0 else small_sum.at[s - 1],
                small_in.at[s],
                r.small_send.at[s],
                r.small_recv.at[s],
                dp=partners[s],
            )
            for s in range(3)
        ]
        tiny[0].start()
        feed.step_one()

    dmt, ds = r.dmt, r.ds
    dqa, dqb, dkv = r.dqa, r.dqb, r.dkv
    dmt[...] = dot(r.o_weight[...], gb[...], 1, 1).astype(low)
    d_keys, d_values = [], []
    for h in range(heads):
        both = slice(h * pair, (h + 1) * pair)
        those = slice(h * HD, (h + 1) * HD)
        st[...] = dot(vt[those, :], dmt[those, :], 0, 0)

        def harden(i, carry, h=h):
            cols = pl.ds(pl.multiple_of(i * 128, 128), 128)
            prob = pt[h, :, cols].astype(wide)
            d_prob = st[:, cols]
            delta = jnp.sum(prob * d_prob, axis=0, keepdims=True)
            ds[:, cols] = (prob * (d_prob - delta) * scale).astype(low)
            return carry

        lax.fori_loop(0, lane_tiles, harden, 0)
        d_values.append(dot(pt[h], dmt[those, :], 1, 1).astype(low))
        d_key = dot(ds[...], qcat[:, both])
        d_keys.append(jnp.where(kind_wide[:, :HD] == 1, d_key[:, HD:], d_key[:, :HD]).astype(low))
        d_query = dot(kcat[:, both], ds[...], 0, 0).T
        dqa[:, both] = jnp.where(kind_wide[...] == 1, 0.0, d_query).astype(low)
        dqb[:, both] = jnp.where(kind_wide[...] == 1, d_query, 0.0).astype(low)
        if planar and h == 0:
            tiny[0].wait_recv()
            small_sum[0] = small[...] + small_in[0]
            tiny[1].start()
            feed.step_two()
        if planar and h == 1:
            tiny[1].wait_recv()
            small_sum[1] = small_sum[0] + small_in[1]
            tiny[2].start()
    dkv[...] = jnp.concatenate(d_keys + d_values, axis=1)
    wkv = jnp.concatenate([r.k_weight[...], r.v_weight[...]], axis=0)
    total = dot(dqa[...], wa[...]) + dot(dqb[...], wb[...]) + dot(dkv[...], wkv)
    total = total.astype(low).reshape(HALVES, LINE, block_rows, width)
    for h in range(HALVES):
        grad[h].part[...] = total[h]
        grad[h].start()
    put_grad(gattn, 0, dot(tok_t[...], dqa[...]))
    put_grad(gattn, 2 * local_width, dot(tok_t[...], dqb[...]))
    put_grad(gattn, 4 * local_width, dot(tok_t[...], dkv[...]))
    o_grad = dot(gb[...], mx[me].reshape(local_width, rows), 0, 1)
    pad = gattn.shape[2] - 7 * local_width
    put_grad(gattn, 6 * local_width, jnp.concatenate([o_grad, jnp.zeros((width, pad), wide)], axis=1))
    if planar:
        attn = PlaneReduce(gattn, *r.attn)
        attn.start()

    def settle_grad(h):
        line = grad[h]
        line.forward()
        own = pl.ds(pl.multiple_of(h * half_rows + me * block_rows, 16), block_rows)
        line.out[me] = (line.total() + dr2[own, :]).astype(low)
        line.spread()

    settle_grad(0)
    if planar:
        tiny[2].wait_recv()
        r.small_out[...] = small_sum[1] + small_in[2]
        feed_sum = feed.finish()
        r.in_grad[...] = feed_sum[:, :hidden_width]
        r.out_grad[...] = feed_sum[:, hidden_width:]
        attn.step_one()
    settle_grad(1)
    grad[0].relay()
    if planar:
        attn.step_two()
    grad[1].relay()
    if planar:
        attn_sum = attn.finish()
        for part in range(4):
            base = (part // 2) * 2 * local_width + (part % 2) * HD
            r.q_grad[part] = jnp.concatenate(
                [attn_sum[:, base + h * pair : base + h * pair + HD] for h in range(heads)], axis=1
            )
        both_grads = attn_sum[:, 4 * local_width : 6 * local_width]
        r.k_grad[...] = both_grads[:, :local_width]
        r.v_grad[...] = both_grads[:, local_width:]
        r.o_grad[...] = attn_sum[:, 6 * local_width : 7 * local_width].T
    else:
        r.small_out[...] = small[...]
        r.feed_out[...] = gfeed[...]
        r.attn_out[...] = gattn[...]
    for line in grad:
        line.arrive()
    for line in ffn + back + grad:
        line.drain()
    for gather in gathers:
        gather.drain()
    for copy in ow_line + ow_swap:
        copy.wait_send()
    if planar:
        for copy in tiny:
            copy.wait_send()


def local(
    tokens,
    segment_ids,
    token_types,
    q_weight,
    k_weight,
    v_weight,
    o_weight,
    o_bias,
    norm1_gain,
    norm1_shift,
    in_weight,
    in_bias,
    out_weight,
    out_bias,
    norm2_gain,
    norm2_shift,
    cotangent,
):
    rows, width = tokens.shape
    local_width = k_weight.shape[1]
    heads = local_width // HD
    hidden_width = in_weight.shape[1]
    n_dp = lax.axis_size("dp")
    planar = n_dp == 8
    blocks = 8
    per_block = width // blocks
    half_rows = rows // HALVES
    block_rows = half_rows // LINE
    low, wide = jnp.bfloat16, jnp.float32
    attn_width = -(-7 * local_width // 128) * 128
    args = dict(
        tokens=tokens,
        seg_col=segment_ids.reshape(rows, 1),
        seg_row=segment_ids.reshape(1, rows),
        kind_col=token_types.reshape(rows, 1),
        q_weight=q_weight.swapaxes(1, 2),
        k_weight=k_weight.T,
        v_weight=v_weight.T,
        o_weight=o_weight,
        o_bias=o_bias[None],
        gain1=norm1_gain[None],
        shift1=norm1_shift[None],
        in_weight=in_weight,
        in_bias=in_bias[None],
        out_weight=out_weight,
        out_bias=out_bias[None],
        gain2=norm2_gain[None],
        shift2=norm2_shift[None],
        cotangent=cotangent,
    )
    shaped = jax.ShapeDtypeStruct
    outs = dict(
        layer_out=shaped((rows, width), low),
        tokens_grad=shaped((HALVES, LINE, block_rows, width), low),
        small_out=shaped((8, width), wide),
    )
    if planar:
        outs |= dict(
            q_grad=shaped((4, per_block, local_width), wide),
            k_grad=shaped((per_block, local_width), wide),
            v_grad=shaped((per_block, local_width), wide),
            o_grad=shaped((local_width, per_block), wide),
            in_grad=shaped((per_block, hidden_width), wide),
            out_grad=shaped((per_block, hidden_width), wide),
        )
    else:
        outs |= dict(
            feed_out=shaped((blocks, per_block, 2 * hidden_width), low),
            attn_out=shaped((blocks, per_block, attn_width), low),
        )
    dma = pltpu.SemaphoreType.DMA
    scratch = dict(
        ow=pltpu.VMEM((LINE, local_width, width), low),
        ow_send=dma((6,)),
        ow_recv=dma((6,)),
        wa=pltpu.VMEM((2 * local_width, width), low),
        wb=pltpu.VMEM((2 * local_width, width), low),
        wk=pltpu.VMEM((2 * local_width, width), low),
        kind_wide=pltpu.VMEM((rows, 2 * HD), jnp.int32),
        seg_wide=pltpu.VMEM((rows, 2 * HD), jnp.int32),
        qcat=pltpu.VMEM((rows, 2 * local_width), low),
        kcat=pltpu.VMEM((rows, 2 * local_width), low),
        vt=pltpu.VMEM((local_width, rows), low),
        st=pltpu.VMEM((rows, rows), wide),
        pt=pltpu.VMEM((heads, rows, rows), low),
        mx=pltpu.VMEM((LINE, heads, HD, rows), low),
        mx_send=dma((heads, 5)),
        mx_recv=dma((heads, LINE)),
        tok_t=pltpu.VMEM((width, rows), low),
        xh1=pltpu.VMEM((rows, width), wide),
        rstd1=pltpu.VMEM((rows, 128), wide),
        hl=pltpu.VMEM((rows, width), low),
        act=pltpu.VMEM((rows, hidden_width), low),
        gp=pltpu.VMEM((rows, hidden_width), wide),
        dr2=pltpu.VMEM((rows, width), wide),
        gf=pltpu.VMEM((rows, width), low),
        il=pltpu.VMEM((rows, hidden_width), low),
        tmp=pltpu.VMEM((half_rows, width), wide),
        acc=pltpu.VMEM((8, 8, width), wide),
        gb=pltpu.VMEM((rows, width), low),
        ffn_out=pltpu.VMEM((HALVES, LINE, block_rows, width), low),
        back_out=pltpu.VMEM((HALVES, LINE, block_rows, width), low),
        gfeed=pltpu.VMEM((blocks, per_block, 2 * hidden_width), low),
        gattn=pltpu.VMEM((blocks, per_block, attn_width), low),
        small=pltpu.VMEM((8, width), wide),
        dmt=pltpu.VMEM((local_width, rows), low),
        ds=pltpu.VMEM((rows, rows), low),
        dqa=pltpu.VMEM((rows, 2 * local_width), low),
        dqb=pltpu.VMEM((rows, 2 * local_width), low),
        dkv=pltpu.VMEM((rows, 2 * local_width), low),
    )
    for name in ("ffn", "back", "grad"):
        scratch[name] = line_scratch(block_rows, width)
    if planar:
        scratch |= dict(
            feed=plane_scratch(per_block, 2 * hidden_width),
            attn=plane_scratch(per_block, attn_width),
            small_in=pltpu.VMEM((3, 8, width), wide),
            small_sum=pltpu.VMEM((2, 8, width), wide),
            small_send=dma((3,)),
            small_recv=dma((3,)),
        )
    layout = jax.tree.structure((args, outs, scratch))
    vm = pl.BlockSpec(memory_space=pltpu.VMEM)
    results = pl.pallas_call(
        functools.partial(layer_kernel, planar, layout),
        out_shape=jax.tree.leaves(outs),
        in_specs=[vm] * len(args),
        out_specs=[vm] * len(outs),
        scratch_shapes=jax.tree.leaves(scratch),
        compiler_params=pltpu.CompilerParams(
            collective_id=0, has_side_effects=True, vmem_limit_bytes=VMEM_LIMIT
        ),
    )(*jax.tree.leaves(args))
    res = types.SimpleNamespace(**jax.tree.unflatten(jax.tree.structure(outs), results))
    small = res.small_out
    if planar:
        grads = (res.q_grad, res.k_grad, res.v_grad, res.o_grad, res.in_grad, res.out_grad.T)
    else:
        feed = res.feed_out.astype(wide).reshape(width, 2 * hidden_width)
        attn = res.attn_out.astype(wide).reshape(width, attn_width)
        feed = lax.psum_scatter(feed, "dp", scatter_dimension=0, tiled=True)
        attn = lax.psum_scatter(attn, "dp", scatter_dimension=0, tiled=True)
        small = lax.psum(small, "dp")
        per = feed.shape[0]
        queries = attn[:, : 4 * local_width].reshape(per, 2, heads, 2, HD)
        queries = queries.transpose(1, 3, 0, 2, 4).reshape(4, per, local_width)
        grads = (
            queries,
            attn[:, 4 * local_width : 5 * local_width],
            attn[:, 5 * local_width : 6 * local_width],
            attn[:, 6 * local_width : 7 * local_width].T,
            feed[:, :hidden_width],
            feed[:, hidden_width:].T,
        )
    d_q, d_k, d_v, d_o, d_in, d_out = grads
    return (
        res.layer_out,
        res.tokens_grad.reshape(rows, width),
        d_q,
        d_k,
        d_v,
        d_o,
        small[0],
        small[1],
        small[2],
        d_in,
        small[3],
        d_out,
        small[4],
        small[5],
        small[6],
    )


def solution(mesh):
    return jax.shard_map(
        local,
        mesh=mesh,
        in_specs=(
            P("dp", None),
            P("dp", None),
            P("dp", None),
            P(None, None, "mp"),
            P(None, "mp"),
            P(None, "mp"),
            P("mp", None),
            P(),
            P(),
            P(),
            P(None, "mp"),
            P("mp"),
            P("mp", None),
            P(),
            P(),
            P(),
            P("dp", None),
        ),
        out_specs=(
            P("dp", None),
            P("dp", None),
            P(None, "dp", "mp"),
            P("dp", "mp"),
            P("dp", "mp"),
            P("mp", "dp"),
            P(),
            P(),
            P(),
            P("dp", "mp"),
            P("mp"),
            P("mp", "dp"),
            P(),
            P(),
            P(),
        ),
        check_vma=False,
    )
```

```python
import functools
import math
import operator
import types

import jax
import jax.numpy as jnp
from jax import lax
from jax.experimental import pallas as pl
from jax.experimental.pallas import tpu as pltpu
from jax.sharding import PartitionSpec as P

HD = 64
LINE = 4
TILE = 128
CHUNK = 32
VMEM_LIMIT = 67043328

norm_epsilon = 1e-05


def remote(src, dst, send_sem, recv_sem, **axes):
    return pltpu.make_async_remote_copy(
        src_ref=src,
        dst_ref=dst,
        send_sem=send_sem,
        recv_sem=recv_sem,
        device_id=axes,
        device_id_type=pl.DeviceIdType.MESH,
    )


class LineReduce:
    def __init__(self, part, carry, single, summed, out, send, recv):
        self.part, self.carry, self.single, self.summed, self.out = part, carry, single, summed, out
        me = lax.axis_index("mp")
        self.me = me
        left = me < 2
        self.is_mid = jnp.logical_or(me == 1, me == 2)
        self.is_end = jnp.logical_not(self.is_mid)
        self.mid = jnp.where(left, 1, 2)
        self.end = jnp.where(left, 0, 3)
        self.far_mid = 3 - self.mid
        self.far_end = 3 - self.end
        self.send, self.recv = send, recv

    def end_sends(self):
        return (
            remote(self.part.at[self.far_end], self.carry.at[0], self.send.at[0], self.recv.at[2], mp=self.mid),
            remote(self.part.at[self.far_mid], self.carry.at[1], self.send.at[1], self.recv.at[3], mp=self.mid),
            remote(self.part.at[self.mid], self.single, self.send.at[2], self.recv.at[0], mp=self.mid),
        )

    def mid_sends(self):
        return (
            remote(self.part.at[self.end], self.single, self.send.at[0], self.recv.at[0], mp=self.end),
            remote(self.carry.at[0], self.summed, self.send.at[1], self.recv.at[1], mp=self.far_end),
            remote(self.carry.at[1], self.summed, self.send.at[2], self.recv.at[1], mp=self.far_mid),
        )

    def gather(self, block, slot, target):
        return remote(self.out.at[block], self.out.at[block], self.send.at[slot], self.recv.at[4 + block], mp=target)

    def start(self):
        @pl.when(self.is_end)
        def _():
            for copy in self.end_sends():
                copy.start()

        @pl.when(self.is_mid)
        def _():
            self.mid_sends()[0].start()

    def forward(self):
        @pl.when(self.is_mid)
        def _():
            sends = self.mid_sends()
            for i, block in ((0, self.far_end), (1, self.far_mid)):
                remote(self.carry.at[i], self.carry.at[i], self.send.at[0], self.recv.at[2 + i], mp=self.end).wait_recv()
                total = self.carry[i].astype(jnp.float32) + self.part[block].astype(jnp.float32)
                self.carry[i] = total.astype(jnp.bfloat16)
                sends[1 + i].start()

    def total(self):
        remote(self.single, self.single, self.send.at[0], self.recv.at[0], mp=self.mid).wait_recv()
        remote(self.summed, self.summed, self.send.at[0], self.recv.at[1], mp=self.mid).wait_recv()
        return (
            self.part[self.me].astype(jnp.float32)
            + self.single[...].astype(jnp.float32)
            + self.summed[...].astype(jnp.float32)
        )

    def spread(self):
        @pl.when(self.is_end)
        def _():
            self.gather(self.me, 3, self.mid).start()

        @pl.when(self.is_mid)
        def _():
            self.gather(self.me, 3, self.end).start()
            self.gather(self.me, 4, self.far_mid).start()

    def wait_block(self, block):
        self.gather(block, 3, self.mid).wait_recv()

    def relay(self):
        @pl.when(self.is_mid)
        def _():
            self.wait_block(self.end)
            self.gather(self.end, 5, self.far_mid).start()
            self.wait_block(self.far_mid)
            self.gather(self.far_mid, 6, self.end).start()
            self.wait_block(self.far_end)
            self.gather(self.far_end, 7, self.end).start()

    def arrive(self):
        @pl.when(self.is_end)
        def _():
            self.wait_block(self.mid)
            self.wait_block(self.far_mid)
            self.wait_block(self.far_end)

    def drain(self):
        @pl.when(self.is_end)
        def _():
            for copy in self.end_sends():
                copy.wait_send()
            self.gather(self.me, 3, self.mid).wait_send()

        @pl.when(self.is_mid)
        def _():
            for copy in self.mid_sends():
                copy.wait_send()
            for slot in range(3, 8):
                self.gather(self.me, slot, self.end).wait_send()


def line_scratch(tiles, rows, width):
    block = pltpu.VMEM((tiles, rows, width), jnp.bfloat16)
    return [
        pltpu.VMEM((tiles, LINE, rows, width), jnp.bfloat16),
        pltpu.VMEM((tiles, 2, rows, width), jnp.bfloat16),
        block,
        block,
        pltpu.SemaphoreType.DMA((tiles, 8)),
        pltpu.SemaphoreType.DMA((tiles, 8)),
    ]


class LineGather:
    def __init__(self, place, send, recv, out):
        self.place, self.send, self.recv, self.out = place, send, recv, out

    def copy(self, block, slot, target):
        return remote(self.out(block), self.out(block), self.send.at[slot], self.recv.at[block], mp=target)

    def spread(self):
        at = self.place

        @pl.when(at.is_end)
        def _():
            self.copy(at.me, 0, at.mid).start()

        @pl.when(at.is_mid)
        def _():
            self.copy(at.me, 0, at.end).start()
            self.copy(at.me, 1, at.far_mid).start()

    def relay(self):
        at = self.place

        @pl.when(at.is_mid)
        def _():
            self.copy(at.end, 2, at.far_mid).wait_recv()
            self.copy(at.end, 2, at.far_mid).start()
            self.copy(at.far_mid, 3, at.end).wait_recv()
            self.copy(at.far_mid, 3, at.end).start()
            self.copy(at.far_end, 4, at.end).wait_recv()
            self.copy(at.far_end, 4, at.end).start()

    def arrive(self):
        at = self.place

        @pl.when(at.is_end)
        def _():
            self.copy(at.mid, 0, at.mid).wait_recv()
            self.copy(at.far_mid, 0, at.mid).wait_recv()
            self.copy(at.far_end, 0, at.mid).wait_recv()

    def drain(self):
        at = self.place

        @pl.when(at.is_end)
        def _():
            self.copy(at.me, 0, at.mid).wait_send()

        @pl.when(at.is_mid)
        def _():
            for slot in range(5):
                self.copy(at.me, slot, at.end).wait_send()


class Place:
    def __init__(self):
        me = lax.axis_index("mp")
        self.me = me
        self.is_mid = jnp.logical_or(me == 1, me == 2)
        self.is_end = jnp.logical_not(self.is_mid)
        left = me < 2
        self.mid = jnp.where(left, 1, 2)
        self.end = jnp.where(left, 0, 3)
        self.far_mid = 3 - self.mid
        self.far_end = 3 - self.end


class PlaneReduce:
    def __init__(self, grads, r1, sums, mid2, r2a, r2b, s3a, s3b, r3a, r3b, send, recv):
        self.grads, self.r1, self.sums, self.mid2 = grads, r1, sums, mid2
        self.r2a, self.r2b, self.s3a, self.s3b, self.r3a, self.r3b = r2a, r2b, s3a, s3b, r3a, r3b
        dp = lax.axis_index("dp")
        self.core, self.x, self.y = lax.rem(dp, 2), lax.rem(dp // 2, 2), dp // 4
        across = dp + 1 - 2 * self.core
        over_x = dp + 2 - 4 * self.x
        over_y = dp + 4 - 8 * self.y
        half = r2a.shape[2]
        self.low, self.high = pl.ds(0, half), pl.ds(half, grads.shape[2] - half)
        self.first = [
            remote(grads.at[2 * k + 1 - self.core], r1.at[k], send.at[k], recv.at[k], dp=across) for k in range(4)
        ]
        self.second = [
            remote(mid2.at[2 * j + 1 - self.x, :, self.low], r2a.at[j], send.at[4 + j], recv.at[4 + j], dp=over_x)
            for j in range(2)
        ] + [
            remote(mid2.at[2 * (1 - self.y) + j, :, self.high], r2b.at[j], send.at[6 + j], recv.at[6 + j], dp=over_y)
            for j in range(2)
        ]
        self.third = [
            remote(s3a, r3a, send.at[8], recv.at[8], dp=over_y),
            remote(s3b, r3b, send.at[9], recv.at[9], dp=over_x),
        ]

    def start(self):
        for copy in self.first:
            copy.start()

    def step_one(self):
        for copy in self.first:
            copy.wait_recv()

        def body(k, carry):
            total = self.grads[2 * k + self.core].astype(jnp.float32) + self.r1[k].astype(jnp.float32)
            self.sums[k] = total
            self.mid2[k] = total.astype(jnp.bfloat16)
            return carry

        lax.fori_loop(0, 4, body, 0)
        for copy in self.second:
            copy.start()

    def step_two(self):
        for copy in self.second:
            copy.wait_recv()
        x, y = self.x, self.y
        self.s3a[...] = (
            self.sums[2 * (1 - y) + x, :, self.low] + self.r2a[1 - y].astype(jnp.float32)
        ).astype(jnp.bfloat16)
        self.third[0].start()
        self.s3b[...] = (
            self.sums[2 * y + 1 - x, :, self.high] + self.r2b[1 - x].astype(jnp.float32)
        ).astype(jnp.bfloat16)
        self.third[1].start()

    def finish(self):
        x, y = self.x, self.y
        for copy in self.third:
            copy.wait_recv()
        own = self.sums.at[2 * y + x]
        own[:, self.low] = own[:, self.low] + self.r2a[y].astype(jnp.float32) + self.r3a[...].astype(jnp.float32)
        own[:, self.high] = own[:, self.high] + self.r2b[x].astype(jnp.float32) + self.r3b[...].astype(jnp.float32)
        for copy in self.first + self.second + self.third:
            copy.wait_send()
        return own


def plane_scratch(rows, width):
    half = (width // 128 + 1) // 2 * 128
    rest = width - half
    low = jnp.bfloat16
    return [
        pltpu.VMEM((4, rows, width), low),
        pltpu.VMEM((4, rows, width), jnp.float32),
        pltpu.VMEM((4, rows, width), low),
        pltpu.VMEM((2, rows, half), low),
        pltpu.VMEM((2, rows, rest), low),
        pltpu.VMEM((rows, half), low),
        pltpu.VMEM((rows, rest), low),
        pltpu.VMEM((rows, half), low),
        pltpu.VMEM((rows, rest), low),
        pltpu.SemaphoreType.DMA((10,)),
        pltpu.SemaphoreType.DMA((10,)),
    ]


def dot(left, right, left_dim=1, right_dim=0):
    return lax.dot_general(
        left, right, (((left_dim,), (right_dim,)), ((), ())), preferred_element_type=jnp.float32
    )


def rows_loop(start, count, body):
    def step(i, carry):
        inside = pl.ds(pl.multiple_of(i * CHUNK, CHUNK), CHUNK)
        body(pl.ds(pl.multiple_of(start + i * CHUNK, CHUNK), CHUNK), inside)
        return carry

    lax.fori_loop(0, count // CHUNK, step, 0)


def fold(value):
    return jnp.sum(value.reshape(value.shape[0] // 8, 8, value.shape[1]), axis=0)


def row_mean(value):
    return jnp.mean(value, axis=-1, keepdims=True)


def layer_kernel(planar, layout, *refs):
    r = types.SimpleNamespace(**functools.reduce(operator.or_, jax.tree.unflatten(layout, refs)))
    tokens, rows, width = r.tokens, r.tokens.shape[0], r.tokens.shape[1]
    local_width = r.k_weight.shape[0]
    heads = local_width // HD
    pair = 2 * HD
    hidden_width = r.in_weight.shape[1]
    tiles = rows // TILE
    block_rows = TILE // LINE
    low, wide = jnp.bfloat16, jnp.float32
    at = Place()
    me = at.me
    dp = lax.axis_index("dp")
    core = lax.rem(dp, 2)
    across = dp + 1 - 2 * core

    barrier = pltpu.get_barrier_semaphore()
    peers = [{"mp": lax.rem(me + step, LINE)} for step in range(1, LINE)] + [{"dp": across}]
    if planar:
        x, y = lax.rem(dp // 2, 2), dp // 4
        over_x, over_y = dp + 2 - 4 * x, dp + 4 - 8 * y
        peers += [{"dp": over_x}, {"dp": over_y}]
    for peer in peers:
        pl.semaphore_signal(barrier, inc=1, device_id=peer, device_id_type=pl.DeviceIdType.MESH)
    pl.semaphore_wait(barrier, len(peers))

    ow, ow_send, ow_recv = r.ow, r.ow_send, r.ow_recv
    share = local_width // 2
    mine = pl.ds(core * share, share)
    ow_line = [
        remote(
            r.o_weight.at[mine],
            ow.at[me, mine],
            ow_send.at[step - 1],
            ow_recv.at[step - 1],
            mp=lax.rem(me + step, LINE),
        )
        for step in range(1, LINE)
    ]
    for copy in ow_line:
        copy.start()
    ow_swap = []
    for step in range(1, LINE):
        source = lax.rem(me + LINE - step, LINE)
        ow_swap.append(
            remote(ow.at[source, mine], ow.at[source, mine], ow_send.at[2 + step], ow_recv.at[2 + step], dp=across)
        )

    vec = r.vec
    o_bias, gain1, shift1, in_bias, out_bias, gain2, shift2 = (vec[i : i + 1, :] for i in range(7))
    wa, wb, wk = r.wa, r.wb, r.wk
    for h in range(heads):
        cols = slice(h * HD, (h + 1) * HD)
        both = slice(h * pair, (h + 1) * pair)
        wa[both, :] = jnp.concatenate([r.q_weight[0, cols, :], r.q_weight[1, cols, :]], axis=0)
        wb[both, :] = jnp.concatenate([r.q_weight[2, cols, :], r.q_weight[3, cols, :]], axis=0)
        key_part = r.k_weight[cols, :]
        wk[both, :] = jnp.concatenate([key_part, key_part], axis=0)
    kind_wide, seg_wide = r.kind_wide, r.seg_wide
    kind_wide[...] = jnp.broadcast_to(r.kind_row[...], (pair, rows)).T
    seg_wide[...] = jnp.broadcast_to(r.seg_row[...], (pair, rows)).T
    qcat, kcat, vt = r.qcat, r.kcat, r.vt
    tok = tokens[...]
    entity = kind_wide[...] == 1
    upper = lax.broadcasted_iota(jnp.int32, (rows, pair), 1) >= HD
    keys = dot(tok, wk[...], 1, 1)
    for h in range(heads):
        both = slice(h * pair, (h + 1) * pair)
        kcat[:, both] = jnp.where(entity == upper, keys[:, both], 0.0).astype(low)
    vt[...] = dot(r.v_weight[...], tok, 1, 1).astype(low)
    q_plain = dot(tok, wa[...], 1, 1)
    q_entity = dot(tok, wb[...], 1, 1)
    for h in range(heads):
        both = slice(h * pair, (h + 1) * pair)
        qcat[:, both] = jnp.where(entity, q_entity[:, both], q_plain[:, both]).astype(low)

    pt, mx, mloc = r.pt, r.mx, r.mloc
    scale = HD ** (-0.5)
    gathers = [
        LineGather(at, r.mx_send.at[q], r.mx_recv.at[q], lambda block, q=q: mx.at[block, q]) for q in range(tiles)
    ]

    def pair_of(h):
        return pl.ds(pl.multiple_of(h * pair, pair), pair)

    def head_of(h):
        return pl.ds(pl.multiple_of(h * HD, HD), HD)

    def attend(q):
        span = slice(q * TILE, (q + 1) * TILE)

        def head_step(h, carry):
            raw = dot(kcat[:, pair_of(h)], qcat[span, pair_of(h)], 1, 1)
            scores = jnp.where(seg_wide[...] == r.seg_row[:, span], raw * scale, -1000000000.0)
            shifted = jnp.exp(scores - jnp.max(scores, axis=0, keepdims=True))
            total = jnp.sum(shifted, axis=0, keepdims=True)
            prob = (shifted * (1.0 / total)).astype(low)
            pt[h, :, span] = prob
            mixed = dot(vt[head_of(h), :], prob).astype(low)
            mx[me, q, head_of(h), :] = mixed
            mloc[head_of(h), span] = mixed
            return carry

        lax.fori_loop(0, heads, head_step, 0)
        gathers[q].spread()

    def swap_weights():
        for copy in ow_line:
            copy.wait_recv()
        for copy in ow_swap:
            copy.start()
        ow[me] = r.o_weight[...]

    tok_t, kct, vn = r.tok_t, r.kct, r.vn

    def turn():
        tok_t[...] = tokens[...].T
        kct[...] = kcat[...].T
        for h in range(heads):
            vn[h] = vt[h * HD : (h + 1) * HD, :].T

    xh1, rstd1, hl = r.xh1, r.rstd1, r.hl
    act, gp, dr2, gf, il, gb, tmp, acc = r.act, r.gp, r.dr2, r.gf, r.il, r.gb, r.tmp, r.acc
    acc[...] = jnp.zeros_like(acc)

    def make_lines(parts, out):
        part, carry, single, summed, send, recv = parts
        return [
            LineReduce(part.at[q], carry.at[q], single.at[q], summed.at[q], out.at[q], send.at[q], recv.at[q])
            for q in range(tiles)
        ]

    ffn = make_lines(r.ffn, r.ffn_out)
    back = make_lines(r.back, r.back_out)
    grad = make_lines(r.grad, r.tokens_grad)

    def put_part(line, value):
        line.part[...] = value.astype(low).reshape(line.part.shape)

    def settle(line):
        line.forward()
        line.out[me] = line.total().astype(low)
        line.spread()

    root_half = math.sqrt(0.5)
    density = 1.0 / math.sqrt(2.0 * math.pi)

    def forward(q):
        gathers[q].arrive()
        start = q * TILE
        here = pl.ds(start, TILE)
        tmp[...] = dot(mx[:, q].reshape(LINE * local_width, TILE), ow[...].reshape(LINE * local_width, width), 0, 0)

        def first_norm(at_rows, inside):
            value = tmp[inside, :] + tokens[at_rows, :].astype(wide) + o_bias
            centred = value - row_mean(value)
            scaled = lax.rsqrt(row_mean(centred * centred) + norm_epsilon)
            normal = centred * scaled
            xh1[at_rows, :] = normal
            rstd1[at_rows, :] = jnp.broadcast_to(scaled, (CHUNK, 128))
            hl[at_rows, :] = (normal * gain1 + shift1).astype(low)

        rows_loop(start, TILE, first_norm)
        tmp[...] = dot(hl[here, :], r.in_weight[...])

        def activate(at_rows, inside):
            inner = tmp[inside, :] + in_bias
            gate = 0.5 + 0.5 * lax.erf(inner * root_half)
            act[at_rows, :] = (inner * gate).astype(low)
            gp[at_rows, :] = gate + inner * (density * jnp.exp(-0.5 * inner * inner))

        rows_loop(start, TILE, activate)
        put_part(ffn[q], dot(act[here, :], r.out_weight[...]))
        ffn[q].start()

    def backward(q):
        ffn[q].arrive()
        start = q * TILE
        here = pl.ds(start, TILE)
        tmp[...] = ffn[q].out[...].reshape(TILE, width).astype(wide)

        def second_norm(at_rows, inside):
            value = xh1[at_rows, :] * gain1 + shift1
            value = value + tmp[inside, :] + out_bias
            centred = value - row_mean(value)
            scaled = lax.rsqrt(row_mean(centred * centred) + norm_epsilon)
            normal = centred * scaled
            r.layer_out[at_rows, :] = (normal * gain2 + shift2).astype(low)
            cot = r.cotangent[at_rows, :].astype(wide)
            acc[6] += fold(cot)
            acc[5] += fold(cot * normal)
            grown = cot * gain2
            grad_in = scaled * (grown - row_mean(grown) - normal * row_mean(grown * normal))
            acc[4] += fold(grad_in)
            dr2[at_rows, :] = grad_in
            gf[at_rows, :] = grad_in.astype(low)

        rows_loop(start, TILE, second_norm)
        tmp[...] = dot(gf[here, :], r.out_weight[...], 1, 1)

        def inner_step(at_rows, inside):
            d_inner = tmp[inside, :] * gp[at_rows, :]
            acc[3] += fold(d_inner)
            il[at_rows, :] = d_inner.astype(low)

        rows_loop(start, TILE, inner_step)
        put_part(back[q], dot(il[here, :], r.in_weight[...], 1, 1))
        back[q].start()

    dqa, dqb, dkv, dk_sum, dv_sum = r.dqa, r.dqb, r.dkv, r.dk_sum, r.dv_sum
    dmt = r.dmt

    def finish_rows(q):
        back[q].arrive()
        start = q * TILE
        here = pl.ds(start, TILE)
        span = slice(start, start + TILE)
        tmp[...] = back[q].out[...].reshape(TILE, width).astype(wide)

        def last_norm(at_rows, inside):
            d_hidden = dr2[at_rows, :] + tmp[inside, :]
            normal = xh1[at_rows, :]
            acc[2] += fold(d_hidden)
            acc[1] += fold(d_hidden * normal)
            grown = d_hidden * gain1
            grad_in = rstd1[at_rows, 0:1] * (grown - row_mean(grown) - normal * row_mean(grown * normal))
            acc[0] += fold(grad_in)
            dr2[at_rows, :] = grad_in
            gb[at_rows, :] = grad_in.astype(low)

        rows_loop(start, TILE, last_norm)
        dmt[...] = dot(r.o_weight[...], gb[here, :], 1, 1).astype(low)
        row_entity = kind_wide[span, :] == 1

        def head_step(h, carry):
            d_mixed = dmt[head_of(h), :]
            d_prob = dot(vn[h], d_mixed)
            prob_low = pt[h, :, span]
            prob = prob_low.astype(wide)
            delta = jnp.sum(prob * d_prob, axis=0, keepdims=True)
            d_score = (prob * (d_prob - delta) * scale).astype(low)
            d_value = dot(prob_low, d_mixed, 1, 1)
            d_key = dot(d_score, qcat[span, pair_of(h)])
            if q == 0:
                dv_sum[h] = d_value
                dk_sum[h] = d_key
            else:
                dv_sum[h] += d_value
                dk_sum[h] += d_key
            d_query = dot(kct[pair_of(h), :], d_score).T
            dqa[span, pair_of(h)] = jnp.where(row_entity, 0.0, d_query).astype(low)
            dqb[span, pair_of(h)] = jnp.where(row_entity, d_query, 0.0).astype(low)
            return carry

        lax.fori_loop(0, heads, head_step, 0)

    gfeed, gattn = r.gfeed, r.gattn
    blocks, per_block = gfeed.shape[0], gfeed.shape[1]

    def put_grad(packed, start, value):
        packed[:, :, start : start + value.shape[1]] = value.astype(low).reshape(blocks, per_block, value.shape[1])

    if planar:
        feed = PlaneReduce(gfeed, *r.feed)
        attn = PlaneReduce(gattn, *r.attn)

    def feed_grads():
        put_grad(gfeed, hidden_width, dot(gf[...], act[...], 0, 0))
        put_grad(gfeed, 0, dot(hl[...], il[...], 0, 0))
        if planar:
            feed.start()

    stages = (
        attend,
        lambda q: gathers[q].relay(),
        forward,
        lambda q: settle(ffn[q]),
        lambda q: ffn[q].relay(),
        backward,
        lambda q: settle(back[q]),
        lambda q: back[q].relay(),
        finish_rows,
    )
    lag = (0, 2, 3, 4, 5, 6, 7, 8, 9)
    for tick in range(tiles + lag[-1]):
        if tick == 3:
            swap_weights()
            for copy in ow_swap:
                copy.wait_recv()
        for stage, late in reversed(tuple(zip(stages, lag))):
            q = tick - late
            if 0 <= q < tiles:
                stage(q)
        if tick == lag[-1] - 1:
            turn()
        if tick == tiles - 1 + lag[6]:
            feed_grads()

    small = r.small
    for i in range(8):
        small[i : i + 1, :] = jnp.sum(acc[i], axis=0, keepdims=True)
    if planar:
        small_in, partners = r.small_in, (across, over_x, over_y)
        small_sum = r.small_sum
        tiny = [
            remote(
                small if s == 0 else small_sum.at[s - 1],
                small_in.at[s],
                r.small_send.at[s],
                r.small_recv.at[s],
                dp=partners[s],
            )
            for s in range(3)
        ]
        tiny[0].start()

    d_keys = [
        jnp.where(kind_wide[:, :HD] == 1, dk_sum[h, :, HD:], dk_sum[h, :, :HD]).astype(low) for h in range(heads)
    ]
    d_values = [dv_sum[h].astype(low) for h in range(heads)]
    dkv[...] = jnp.concatenate(d_keys + d_values, axis=1)
    wkv = jnp.concatenate([r.k_weight[...], r.v_weight[...]], axis=0)
    for q in range(tiles):
        span = slice(q * TILE, (q + 1) * TILE)
        put_part(grad[q], dot(dqa[span, :], wa[...]) + dot(dqb[span, :], wb[...]) + dot(dkv[span, :], wkv))
        grad[q].start()

    def settle_grad(q):
        line = grad[q]
        line.forward()
        own = pl.ds(pl.multiple_of(q * TILE + me * block_rows, block_rows), block_rows)
        line.out[me] = (line.total() + dr2[own, :]).astype(low)
        line.spread()

    if planar:
        feed.step_one()
    put_grad(gattn, 0, dot(tok_t[...], dqa[...]))
    put_grad(gattn, 2 * local_width, dot(tok_t[...], dqb[...]))
    settle_grad(0)
    put_grad(gattn, 4 * local_width, dot(tok_t[...], dkv[...]))
    o_grad = dot(gb[...], mloc[...], 0, 1)
    pad = gattn.shape[2] - 7 * local_width
    put_grad(gattn, 6 * local_width, jnp.concatenate([o_grad, jnp.zeros((width, pad), wide)], axis=1))
    if planar:
        attn.start()
    settle_grad(1)
    grad[0].relay()
    if planar:
        tiny[0].wait_recv()
        small_sum[0] = small[...] + small_in[0]
        tiny[1].start()
        feed.step_two()
        attn.step_one()
    for q in range(2, tiles):
        settle_grad(q)
        grad[q - 1].relay()
        if planar and q == 2:
            tiny[1].wait_recv()
            small_sum[1] = small_sum[0] + small_in[1]
            tiny[2].start()
            feed_sum = feed.finish()
            r.in_grad[...] = feed_sum[:, :hidden_width]
            r.out_grad[...] = feed_sum[:, hidden_width:]
        if planar and q == 3:
            attn.step_two()
    if planar:
        tiny[2].wait_recv()
        r.small_out[...] = small_sum[1] + small_in[2]
    grad[tiles - 1].relay()
    if planar:
        attn_sum = attn.finish()
        for part in range(4):
            base = (part // 2) * 2 * local_width + (part % 2) * HD
            r.q_grad[part] = jnp.concatenate(
                [attn_sum[:, base + h * pair : base + h * pair + HD] for h in range(heads)], axis=1
            )
        both_grads = attn_sum[:, 4 * local_width : 6 * local_width]
        r.k_grad[...] = both_grads[:, :local_width]
        r.v_grad[...] = both_grads[:, local_width:]
        r.o_grad[...] = attn_sum[:, 6 * local_width : 7 * local_width].T
    else:
        r.small_out[...] = small[...]
        r.feed_out[...] = gfeed[...]
        r.attn_out[...] = gattn[...]
    for line in grad:
        line.arrive()
    for line in ffn + back + grad:
        line.drain()
    for gather in gathers:
        gather.drain()
    for copy in ow_line + ow_swap:
        copy.wait_send()
    if planar:
        for copy in tiny:
            copy.wait_send()


def hand_on(*refs):
    count = len(refs) // 2
    for source, target in zip(refs[:count], refs[count:]):
        target[...] = source[...]


def local(
    tokens,
    segment_ids,
    token_types,
    q_weight,
    k_weight,
    v_weight,
    o_weight,
    o_bias,
    norm1_gain,
    norm1_shift,
    in_weight,
    in_bias,
    out_weight,
    out_bias,
    norm2_gain,
    norm2_shift,
    cotangent,
):
    rows, width = tokens.shape
    local_width = k_weight.shape[1]
    heads = local_width // HD
    hidden_width = in_weight.shape[1]
    n_dp = lax.axis_size("dp")
    planar = n_dp == 8
    blocks = 8
    per_block = width // blocks
    tiles = rows // TILE
    block_rows = TILE // LINE
    low, wide = jnp.bfloat16, jnp.float32
    attn_width = -(-7 * local_width // 128) * 128
    args = dict(
        tokens=tokens,
        seg_row=segment_ids,
        kind_row=token_types,
        q_weight=q_weight.swapaxes(1, 2),
        k_weight=k_weight.T,
        v_weight=v_weight.T,
        o_weight=o_weight,
        vec=jnp.stack([o_bias, norm1_gain, norm1_shift, in_bias, out_bias, norm2_gain, norm2_shift, o_bias]),
        in_weight=in_weight,
        out_weight=out_weight,
        cotangent=cotangent,
    )
    shaped = jax.ShapeDtypeStruct
    outs = dict(
        layer_out=shaped((rows, width), low),
        tokens_grad=shaped((tiles, LINE, block_rows, width), low),
        small_out=shaped((8, width), wide),
    )
    if planar:
        outs |= dict(
            q_grad=shaped((4, per_block, local_width), wide),
            k_grad=shaped((per_block, local_width), wide),
            v_grad=shaped((per_block, local_width), wide),
            o_grad=shaped((local_width, per_block), wide),
            in_grad=shaped((per_block, hidden_width), wide),
            out_grad=shaped((per_block, hidden_width), wide),
        )
    else:
        outs |= dict(
            feed_out=shaped((blocks, per_block, 2 * hidden_width), low),
            attn_out=shaped((blocks, per_block, attn_width), low),
        )
    dma = pltpu.SemaphoreType.DMA
    scratch = dict(
        ow=pltpu.VMEM((LINE, local_width, width), low),
        ow_send=dma((6,)),
        ow_recv=dma((6,)),
        wa=pltpu.VMEM((2 * local_width, width), low),
        wb=pltpu.VMEM((2 * local_width, width), low),
        wk=pltpu.VMEM((2 * local_width, width), low),
        kind_wide=pltpu.VMEM((rows, 2 * HD), jnp.int32),
        seg_wide=pltpu.VMEM((rows, 2 * HD), jnp.int32),
        qcat=pltpu.VMEM((rows, 2 * local_width), low),
        kcat=pltpu.VMEM((rows, 2 * local_width), low),
        vt=pltpu.VMEM((local_width, rows), low),
        pt=pltpu.VMEM((heads, rows, rows), low),
        mx=pltpu.VMEM((LINE, tiles, local_width, TILE), low),
        mloc=pltpu.VMEM((local_width, rows), low),
        mx_send=dma((tiles, 5)),
        mx_recv=dma((tiles, LINE)),
        tok_t=pltpu.VMEM((width, rows), low),
        xh1=pltpu.VMEM((rows, width), wide),
        rstd1=pltpu.VMEM((rows, 128), wide),
        hl=pltpu.VMEM((rows, width), low),
        act=pltpu.VMEM((rows, hidden_width), low),
        gp=pltpu.VMEM((rows, hidden_width), wide),
        dr2=pltpu.VMEM((rows, width), wide),
        gf=pltpu.VMEM((rows, width), low),
        il=pltpu.VMEM((rows, hidden_width), low),
        tmp=pltpu.VMEM((TILE, width), wide),
        acc=pltpu.VMEM((8, 8, width), wide),
        gb=pltpu.VMEM((rows, width), low),
        ffn_out=pltpu.VMEM((tiles, LINE, block_rows, width), low),
        back_out=pltpu.VMEM((tiles, LINE, block_rows, width), low),
        gfeed=pltpu.VMEM((blocks, per_block, 2 * hidden_width), low),
        gattn=pltpu.VMEM((blocks, per_block, attn_width), low),
        small=pltpu.VMEM((8, width), wide),
        kct=pltpu.VMEM((2 * local_width, rows), low),
        vn=pltpu.VMEM((heads, rows, HD), low),
        dmt=pltpu.VMEM((local_width, TILE), low),
        dk_sum=pltpu.VMEM((heads, rows, 2 * HD), wide),
        dv_sum=pltpu.VMEM((heads, rows, HD), wide),
        dqa=pltpu.VMEM((rows, 2 * local_width), low),
        dqb=pltpu.VMEM((rows, 2 * local_width), low),
        dkv=pltpu.VMEM((rows, 2 * local_width), low),
    )
    for name in ("ffn", "back", "grad"):
        scratch[name] = line_scratch(tiles, block_rows, width)
    if planar:
        scratch |= dict(
            feed=plane_scratch(per_block, 2 * hidden_width),
            attn=plane_scratch(per_block, attn_width),
            small_in=pltpu.VMEM((3, 8, width), wide),
            small_sum=pltpu.VMEM((2, 8, width), wide),
            small_send=dma((3,)),
            small_recv=dma((3,)),
        )
    layout = jax.tree.structure((args, outs, scratch))
    vm = pl.BlockSpec(memory_space=pltpu.VMEM)
    results = pl.pallas_call(
        functools.partial(layer_kernel, planar, layout),
        out_shape=jax.tree.leaves(outs),
        in_specs=[vm] * len(args),
        out_specs=[vm] * len(outs),
        scratch_shapes=jax.tree.leaves(scratch),
        compiler_params=pltpu.CompilerParams(
            collective_id=0, has_side_effects=True, vmem_limit_bytes=VMEM_LIMIT
        ),
    )(*jax.tree.leaves(args))
    results = dict(zip(sorted(outs), results))
    if planar:
        small = results.pop("small_out")
        results["tokens_grad"] = results["tokens_grad"].reshape(rows, width)
        flat, tree = jax.tree.flatten(results)
        flat = pl.pallas_call(
            hand_on,
            out_shape=[shaped(a.shape, a.dtype) for a in flat],
            in_specs=[vm] * len(flat),
            out_specs=[vm] * len(flat),
            compiler_params=pltpu.CompilerParams(vmem_limit_bytes=VMEM_LIMIT),
        )(*flat)
        results = jax.tree.unflatten(tree, flat) | {"small_out": small}
    res = types.SimpleNamespace(**results)
    small = res.small_out
    if planar:
        grads = (res.q_grad, res.k_grad, res.v_grad, res.o_grad, res.in_grad, res.out_grad.T)
    else:
        feed = res.feed_out.astype(wide).reshape(width, 2 * hidden_width)
        attn = res.attn_out.astype(wide).reshape(width, attn_width)
        feed = lax.psum_scatter(feed, "dp", scatter_dimension=0, tiled=True)
        attn = lax.psum_scatter(attn, "dp", scatter_dimension=0, tiled=True)
        small = lax.psum(small, "dp")
        per = feed.shape[0]
        queries = attn[:, : 4 * local_width].reshape(per, 2, heads, 2, HD)
        queries = queries.transpose(1, 3, 0, 2, 4).reshape(4, per, local_width)
        grads = (
            queries,
            attn[:, 4 * local_width : 5 * local_width],
            attn[:, 5 * local_width : 6 * local_width],
            attn[:, 6 * local_width : 7 * local_width].T,
            feed[:, :hidden_width],
            feed[:, hidden_width:].T,
        )
    d_q, d_k, d_v, d_o, d_in, d_out = grads
    return (
        res.layer_out,
        res.tokens_grad.reshape(rows, width),
        d_q,
        d_k,
        d_v,
        d_o,
        small[0],
        small[1],
        small[2],
        d_in,
        small[3],
        d_out,
        small[4],
        small[5],
        small[6],
    )


def solution(mesh):
    return jax.shard_map(
        local,
        mesh=mesh,
        in_specs=(
            P("dp", None),
            P("dp", None),
            P("dp", None),
            P(None, None, "mp"),
            P(None, "mp"),
            P(None, "mp"),
            P("mp", None),
            P(),
            P(),
            P(),
            P(None, "mp"),
            P("mp"),
            P("mp", None),
            P(),
            P(),
            P(),
            P("dp", None),
        ),
        out_specs=(
            P("dp", None),
            P("dp", None),
            P(None, "dp", "mp"),
            P("dp", "mp"),
            P("dp", "mp"),
            P("mp", "dp"),
            P(),
            P(),
            P(),
            P("dp", "mp"),
            P("mp"),
            P("mp", "dp"),
            P(),
            P(),
            P(),
        ),
        check_vma=False,
    )
```

```python
import functools
import math
import operator
import types

import jax
import jax.numpy as jnp
from jax import lax
from jax.experimental import pallas as pl
from jax.experimental.pallas import tpu as pltpu
from jax.sharding import PartitionSpec as P

HD = 64
LINE = 4
PORTIONS = (2, 3)
LANES = 128
CHUNK = 32
VMEM_LIMIT = 67043328

norm_epsilon = 1e-05


def remote(src, dst, send_sem, recv_sem, **axes):
    return pltpu.make_async_remote_copy(
        src_ref=src,
        dst_ref=dst,
        send_sem=send_sem,
        recv_sem=recv_sem,
        device_id=axes,
        device_id_type=pl.DeviceIdType.MESH,
    )


class Place:
    def __init__(self):
        me = lax.axis_index("mp")
        self.me = me
        self.is_mid = jnp.logical_or(me == 1, me == 2)
        self.is_end = jnp.logical_not(self.is_mid)
        left = me < 2
        self.mid = jnp.where(left, 1, 2)
        self.end = jnp.where(left, 0, 3)
        self.far_mid = 3 - self.mid
        self.far_end = 3 - self.end


class LineGather:
    def __init__(self, place, send, recv, out):
        self.at, self.send, self.recv, self.out = place, send, recv, out

    def copy(self, block, slot, target):
        return remote(self.out(block), self.out(block), self.send.at[slot], self.recv.at[block], mp=target)

    def spread(self):
        at = self.at

        @pl.when(at.is_end)
        def _():
            self.copy(at.me, 0, at.mid).start()

        @pl.when(at.is_mid)
        def _():
            self.copy(at.me, 0, at.end).start()
            self.copy(at.me, 1, at.far_mid).start()

    def relay(self, step):
        at = self.at
        block = (at.end, at.far_mid, at.far_end)[step]
        target = (at.far_mid, at.end, at.end)[step]

        @pl.when(at.is_mid)
        def _():
            self.copy(block, 2 + step, target).wait_recv()
            self.copy(block, 2 + step, target).start()

    def arrive(self):
        at = self.at

        @pl.when(at.is_end)
        def _():
            self.copy(at.mid, 0, at.mid).wait_recv()
            self.copy(at.far_mid, 0, at.mid).wait_recv()
            self.copy(at.far_end, 0, at.mid).wait_recv()

    def drain(self):
        at = self.at

        @pl.when(at.is_end)
        def _():
            self.copy(at.me, 0, at.mid).wait_send()

        @pl.when(at.is_mid)
        def _():
            for slot in range(5):
                self.copy(at.me, slot, at.end).wait_send()


class LineReduce:
    def __init__(self, place, part, carry, single, summed, send, recv, start, block_rows, out):
        self.at, self.carry, self.single, self.summed = place, carry, single, summed
        self.send, self.recv = send, recv

        def rows_of(block):
            return pl.ds(pl.multiple_of(start + block * block_rows, 16), block_rows)

        self.rows_of, self.part_ref, self.out_ref = rows_of, part, out
        self.gather = LineGather(place, send.at[1], recv.at[1], lambda block: out.at[rows_of(block)])

    def part(self, block):
        return self.part_ref.at[self.rows_of(block)]

    def end_sends(self):
        at, send, recv = self.at, self.send, self.recv
        return (
            remote(self.part(at.far_end), self.carry.at[0], send.at[0, 0], recv.at[0, 2], mp=at.mid),
            remote(self.part(at.far_mid), self.carry.at[1], send.at[0, 1], recv.at[0, 3], mp=at.mid),
            remote(self.part(at.mid), self.single, send.at[0, 2], recv.at[0, 0], mp=at.mid),
        )

    def mid_sends(self):
        at, send, recv = self.at, self.send, self.recv
        return (
            remote(self.carry.at[0], self.summed, send.at[0, 1], recv.at[0, 1], mp=at.far_end),
            remote(self.carry.at[1], self.summed, send.at[0, 2], recv.at[0, 1], mp=at.far_mid),
            remote(self.part(at.end), self.single, send.at[0, 0], recv.at[0, 0], mp=at.end),
        )

    def start(self):
        @pl.when(self.at.is_end)
        def _():
            for copy in self.end_sends():
                copy.start()

        @pl.when(self.at.is_mid)
        def _():
            self.mid_sends()[2].start()

    def forward(self, step):
        at = self.at

        @pl.when(at.is_mid)
        def _():
            block = (at.far_end, at.far_mid)[step]
            self.end_sends()[step].wait_recv()
            total = self.carry[step].astype(jnp.float32) + self.part(block)[...].astype(jnp.float32)
            self.carry[step] = total.astype(jnp.bfloat16)
            self.mid_sends()[step].start()

    def settle(self, extra=None):
        at = self.at
        self.end_sends()[2].wait_recv()
        self.mid_sends()[0].wait_recv()
        total = (
            self.part(at.me)[...].astype(jnp.float32)
            + self.single[...].astype(jnp.float32)
            + self.summed[...].astype(jnp.float32)
        )
        if extra is not None:
            total = total + extra[self.rows_of(at.me), :]
        self.out_ref[self.rows_of(at.me), :] = total.astype(jnp.bfloat16)
        self.gather.spread()

    def relay(self, step):
        self.gather.relay(step)

    def arrive(self):
        self.gather.arrive()

    def drain(self):
        @pl.when(self.at.is_end)
        def _():
            for copy in self.end_sends():
                copy.wait_send()

        @pl.when(self.at.is_mid)
        def _():
            for copy in self.mid_sends():
                copy.wait_send()

        self.gather.drain()


def line_scratch(rows, width):
    return [
        pltpu.VMEM((2, rows, width), jnp.bfloat16),
        pltpu.VMEM((rows, width), jnp.bfloat16),
        pltpu.VMEM((rows, width), jnp.bfloat16),
        pltpu.SemaphoreType.DMA((2, 5)),
        pltpu.SemaphoreType.DMA((2, 4)),
    ]


class PlaneReduce:
    def __init__(self, grads, r1, sums, mid2, r2a, r2b, s3a, s3b, r3a, r3b, send, recv):
        self.grads, self.r1, self.sums, self.mid2 = grads, r1, sums, mid2
        self.r2a, self.r2b, self.s3a, self.s3b, self.r3a, self.r3b = r2a, r2b, s3a, s3b, r3a, r3b
        dp = lax.axis_index("dp")
        self.core, self.x, self.y = lax.rem(dp, 2), lax.rem(dp // 2, 2), dp // 4
        across = dp + 1 - 2 * self.core
        over_x = dp + 2 - 4 * self.x
        over_y = dp + 4 - 8 * self.y
        half = r2a.shape[2]
        self.low, self.high = pl.ds(0, half), pl.ds(half, grads.shape[2] - half)
        self.first = [
            remote(grads.at[2 * k + 1 - self.core], r1.at[k], send.at[k], recv.at[k], dp=across) for k in range(4)
        ]
        self.second = [
            remote(mid2.at[2 * j + 1 - self.x, :, self.low], r2a.at[j], send.at[4 + j], recv.at[4 + j], dp=over_x)
            for j in range(2)
        ] + [
            remote(mid2.at[2 * (1 - self.y) + j, :, self.high], r2b.at[j], send.at[6 + j], recv.at[6 + j], dp=over_y)
            for j in range(2)
        ]
        self.third = [
            remote(s3a, r3a, send.at[8], recv.at[8], dp=over_y),
            remote(s3b, r3b, send.at[9], recv.at[9], dp=over_x),
        ]

    def start(self):
        for copy in self.first:
            copy.start()

    def step_one(self):
        for copy in self.first:
            copy.wait_recv()

        def body(k, carry):
            total = self.grads[2 * k + self.core].astype(jnp.float32) + self.r1[k].astype(jnp.float32)
            self.sums[k] = total
            self.mid2[k] = total.astype(jnp.bfloat16)
            return carry

        lax.fori_loop(0, 4, body, 0)
        for copy in self.second:
            copy.start()

    def step_two(self):
        for copy in self.second:
            copy.wait_recv()
        x, y = self.x, self.y
        self.s3a[...] = (
            self.sums[2 * (1 - y) + x, :, self.low] + self.r2a[1 - y].astype(jnp.float32)
        ).astype(jnp.bfloat16)
        self.third[0].start()
        self.s3b[...] = (
            self.sums[2 * y + 1 - x, :, self.high] + self.r2b[1 - x].astype(jnp.float32)
        ).astype(jnp.bfloat16)
        self.third[1].start()

    def finish(self):
        x, y = self.x, self.y
        for copy in self.third:
            copy.wait_recv()
        own = self.sums.at[2 * y + x]
        own[:, self.low] = own[:, self.low] + self.r2a[y].astype(jnp.float32) + self.r3a[...].astype(jnp.float32)
        own[:, self.high] = own[:, self.high] + self.r2b[x].astype(jnp.float32) + self.r3b[...].astype(jnp.float32)
        for copy in self.first + self.second + self.third:
            copy.wait_send()
        return own


def plane_scratch(rows, width):
    half = (width // 128 + 1) // 2 * 128
    rest = width - half
    low = jnp.bfloat16
    return [
        pltpu.VMEM((4, rows, width), low),
        pltpu.VMEM((4, rows, width), jnp.float32),
        pltpu.VMEM((4, rows, width), low),
        pltpu.VMEM((2, rows, half), low),
        pltpu.VMEM((2, rows, rest), low),
        pltpu.VMEM((rows, half), low),
        pltpu.VMEM((rows, rest), low),
        pltpu.VMEM((rows, half), low),
        pltpu.VMEM((rows, rest), low),
        pltpu.SemaphoreType.DMA((10,)),
        pltpu.SemaphoreType.DMA((10,)),
    ]


def dot(left, right, left_dim=1, right_dim=0):
    return lax.dot_general(
        left, right, (((left_dim,), (right_dim,)), ((), ())), preferred_element_type=jnp.float32
    )


def rows_loop(start, count, body):
    def step(i, carry):
        inside = pl.ds(pl.multiple_of(i * CHUNK, CHUNK), CHUNK)
        body(pl.ds(pl.multiple_of(start + i * CHUNK, CHUNK), CHUNK), inside)
        return carry

    lax.fori_loop(0, count // CHUNK, step, 0)


def fold(value):
    return jnp.sum(value.reshape(value.shape[0] // 8, 8, value.shape[1]), axis=0)


def row_mean(value):
    return jnp.mean(value, axis=-1, keepdims=True)


def portions_of(rows):
    unit = rows // sum(PORTIONS)
    return [(unit * sum(PORTIONS[:i]), unit * size) for i, size in enumerate(PORTIONS)]


def layer_kernel(planar, layout, *refs):
    r = types.SimpleNamespace(**functools.reduce(operator.or_, jax.tree.unflatten(layout, refs)))
    tokens, rows, width = r.tokens, r.tokens.shape[0], r.tokens.shape[1]
    local_width = r.k_weight.shape[0]
    heads = local_width // HD
    pair = 2 * HD
    hidden_width = r.in_weight.shape[1]
    spans = portions_of(rows)
    low, wide = jnp.bfloat16, jnp.float32
    at = Place()
    me = at.me
    dp = lax.axis_index("dp")
    core = lax.rem(dp, 2)
    across = dp + 1 - 2 * core

    barrier = pltpu.get_barrier_semaphore()
    peers = [{"mp": lax.rem(me + step, LINE)} for step in range(1, LINE)] + [{"dp": across}]
    if planar:
        x, y = lax.rem(dp // 2, 2), dp // 4
        over_x, over_y = dp + 2 - 4 * x, dp + 4 - 8 * y
        peers += [{"dp": over_x}, {"dp": over_y}]
    for peer in peers:
        pl.semaphore_signal(barrier, inc=1, device_id=peer, device_id_type=pl.DeviceIdType.MESH)
    pl.semaphore_wait(barrier, len(peers))

    ow, ow_send, ow_recv = r.ow, r.ow_send, r.ow_recv
    share = local_width // 2
    mine = pl.ds(core * share, share)
    ow_line = [
        remote(
            r.o_weight.at[mine],
            ow.at[me, mine],
            ow_send.at[step - 1],
            ow_recv.at[step - 1],
            mp=lax.rem(me + step, LINE),
        )
        for step in range(1, LINE)
    ]
    for copy in ow_line:
        copy.start()
    ow_swap = []
    for step in range(1, LINE):
        source = lax.rem(me + LINE - step, LINE)
        ow_swap.append(
            remote(ow.at[source, mine], ow.at[source, mine], ow_send.at[2 + step], ow_recv.at[2 + step], dp=across)
        )

    vec = r.vec
    for i, name in enumerate((r.o_bias, r.gain1, r.shift1, r.in_bias, r.out_bias, r.gain2, r.shift2)):
        vec[i, :] = name[...]
    o_bias, gain1, shift1, in_bias, out_bias, gain2, shift2 = (vec[i : i + 1, :] for i in range(7))
    wa, wb, wk = r.wa, r.wb, r.wk
    for h in range(heads):
        cols = slice(h * HD, (h + 1) * HD)
        both = slice(h * pair, (h + 1) * pair)
        wa[both, :] = jnp.concatenate([r.q_weight[0, cols, :], r.q_weight[1, cols, :]], axis=0)
        wb[both, :] = jnp.concatenate([r.q_weight[2, cols, :], r.q_weight[3, cols, :]], axis=0)
        key_part = r.k_weight[cols, :]
        wk[both, :] = jnp.concatenate([key_part, key_part], axis=0)
    kind_wide, seg_wide = r.kind_wide, r.seg_wide
    kind_wide[...] = jnp.broadcast_to(r.kind_row[...], (pair, rows)).T
    seg_wide[...] = jnp.broadcast_to(r.seg_row[...], (pair, rows)).T
    qcat, kcat, vt = r.qcat, r.kcat, r.vt
    tok = tokens[...]
    entity = kind_wide[...] == 1
    upper = lax.broadcasted_iota(jnp.int32, (rows, pair), 1) >= HD
    keys = dot(tok, wk[...], 1, 1)
    for h in range(heads):
        both = slice(h * pair, (h + 1) * pair)
        kcat[:, both] = jnp.where(entity == upper, keys[:, both], 0.0).astype(low)
    vt[...] = dot(r.v_weight[...], tok, 1, 1).astype(low)
    q_plain = dot(tok, wa[...], 1, 1)
    q_entity = dot(tok, wb[...], 1, 1)
    for h in range(heads):
        both = slice(h * pair, (h + 1) * pair)
        qcat[:, both] = jnp.where(entity, q_entity[:, both], q_plain[:, both]).astype(low)

    pt, mx, mloc, st = r.pt, r.mx, r.mloc, r.st
    scale = HD ** (-0.5)
    gathers = [
        LineGather(at, r.mx_send.at[q], r.mx_recv.at[q], lambda block, q=q: mx[q].at[block])
        for q in range(len(spans))
    ]

    def pair_of(h):
        return pl.ds(pl.multiple_of(h * pair, pair), pair)

    def head_of(h):
        return pl.ds(pl.multiple_of(h * HD, HD), HD)

    def attend(q):
        start, size = spans[q]
        here = pl.ds(start, size)

        def head_step(h, carry):
            st[:, :size] = dot(kcat[:, pair_of(h)], qcat[here, pair_of(h)], 1, 1)

            def soften(i, carry):
                cols = pl.ds(pl.multiple_of(i * LANES, LANES), LANES)
                span = pl.ds(pl.multiple_of(start + i * LANES, LANES), LANES)
                scores = jnp.where(seg_wide[...] == r.seg_row[:, span], st[:, cols] * scale, -1000000000.0)
                shifted = jnp.exp(scores - jnp.max(scores, axis=0, keepdims=True))
                total = jnp.sum(shifted, axis=0, keepdims=True)
                pt[h, :, span] = (shifted * (1.0 / total)).astype(low)
                return carry

            lax.fori_loop(0, size // LANES, soften, 0)
            mixed = dot(vt[head_of(h), :], pt[h, :, here]).astype(low)
            mx[q][me, head_of(h), :] = mixed
            mloc[head_of(h), here] = mixed
            return carry

        lax.fori_loop(0, heads, head_step, 0)
        gathers[q].spread()

    def swap_weights():
        for copy in ow_line:
            copy.wait_recv()
        for copy in ow_swap:
            copy.start()
        ow[me] = r.o_weight[...]

    tok_t, kct, vn = r.tok_t, r.kct, r.vn

    def turn():
        tok_t[...] = tokens[...].T
        kct[...] = kcat[...].T
        for h in range(heads):
            vn[h] = vt[h * HD : (h + 1) * HD, :].T

    xh1, rstd1, hl = r.xh1, r.rstd1, r.hl
    act, gp, dr2, gf, il, gb, tmp, acc = r.act, r.gp, r.dr2, r.gf, r.il, r.gb, r.tmp, r.acc
    acc[...] = jnp.zeros_like(acc)

    def make_lines(parts, part, out):
        return [
            LineReduce(at, part, *parts[q], start, size // LINE, out) for q, (start, size) in enumerate(spans)
        ]

    ffn = make_lines(r.ffn, r.ffn_part, r.ffn_out)
    back = make_lines(r.back, r.back_part, r.back_out)
    grad = make_lines(r.grad, r.grad_part, r.tokens_grad)

    root_half = math.sqrt(0.5)
    density = 1.0 / math.sqrt(2.0 * math.pi)

    def forward(q):
        gathers[q].arrive()
        start, size = spans[q]
        here = pl.ds(start, size)
        mixed = mx[q][...].reshape(LINE * local_width, size)
        tmp[:size, :] = dot(mixed, ow[...].reshape(LINE * local_width, width), 0, 0)

        def first_norm(at_rows, inside):
            value = tmp[inside, :] + tokens[at_rows, :].astype(wide) + o_bias
            centred = value - row_mean(value)
            scaled = lax.rsqrt(row_mean(centred * centred) + norm_epsilon)
            normal = centred * scaled
            xh1[at_rows, :] = normal
            rstd1[at_rows, :] = jnp.broadcast_to(scaled, (CHUNK, 128))
            hl[at_rows, :] = (normal * gain1 + shift1).astype(low)

        rows_loop(start, size, first_norm)
        tmp[:size, :] = dot(hl[here, :], r.in_weight[...])

        def activate(at_rows, inside):
            inner = tmp[inside, :] + in_bias
            gate = 0.5 + 0.5 * lax.erf(inner * root_half)
            act[at_rows, :] = (inner * gate).astype(low)
            gp[at_rows, :] = gate + inner * (density * jnp.exp(-0.5 * inner * inner))

        rows_loop(start, size, activate)
        r.ffn_part[here, :] = dot(act[here, :], r.out_weight[...]).astype(low)
        ffn[q].start()

    def backward(q):
        ffn[q].arrive()
        start, size = spans[q]
        here = pl.ds(start, size)

        def second_norm(at_rows, inside):
            value = xh1[at_rows, :] * gain1 + shift1
            value = value + r.ffn_out[at_rows, :].astype(wide) + out_bias
            centred = value - row_mean(value)
            scaled = lax.rsqrt(row_mean(centred * centred) + norm_epsilon)
            normal = centred * scaled
            r.layer_out[at_rows, :] = (normal * gain2 + shift2).astype(low)
            cot = r.cotangent[at_rows, :].astype(wide)
            acc[6] += fold(cot)
            acc[5] += fold(cot * normal)
            grown = cot * gain2
            grad_in = scaled * (grown - row_mean(grown) - normal * row_mean(grown * normal))
            acc[4] += fold(grad_in)
            dr2[at_rows, :] = grad_in
            gf[at_rows, :] = grad_in.astype(low)

        rows_loop(start, size, second_norm)
        tmp[:size, :] = dot(gf[here, :], r.out_weight[...], 1, 1)

        def inner_step(at_rows, inside):
            d_inner = tmp[inside, :] * gp[at_rows, :]
            acc[3] += fold(d_inner)
            il[at_rows, :] = d_inner.astype(low)

        rows_loop(start, size, inner_step)
        r.back_part[here, :] = dot(il[here, :], r.in_weight[...], 1, 1).astype(low)
        back[q].start()

    dqa, dqb, dkv, dk_sum, dv_sum = r.dqa, r.dqb, r.dkv, r.dk_sum, r.dv_sum
    dmt, ds = r.dmt, r.ds

    def finish_rows(q):
        back[q].arrive()
        start, size = spans[q]
        here = pl.ds(start, size)

        def last_norm(at_rows, inside):
            d_hidden = dr2[at_rows, :] + r.back_out[at_rows, :].astype(wide)
            normal = xh1[at_rows, :]
            acc[2] += fold(d_hidden)
            acc[1] += fold(d_hidden * normal)
            grown = d_hidden * gain1
            grad_in = rstd1[at_rows, 0:1] * (grown - row_mean(grown) - normal * row_mean(grown * normal))
            acc[0] += fold(grad_in)
            dr2[at_rows, :] = grad_in
            gb[at_rows, :] = grad_in.astype(low)

        rows_loop(start, size, last_norm)
        dmt[:, here] = dot(r.o_weight[...], gb[here, :], 1, 1).astype(low)

        def head_step(h, carry):
            d_mixed = dmt[head_of(h), here]
            st[:, :size] = dot(vn[h], d_mixed)

            def harden(i, carry):
                cols = pl.ds(pl.multiple_of(i * LANES, LANES), LANES)
                span = pl.ds(pl.multiple_of(start + i * LANES, LANES), LANES)
                prob = pt[h, :, span].astype(wide)
                d_prob = st[:, cols]
                delta = jnp.sum(prob * d_prob, axis=0, keepdims=True)
                ds[:, cols] = (prob * (d_prob - delta) * scale).astype(low)
                return carry

            lax.fori_loop(0, size // LANES, harden, 0)
            d_score = ds[:, :size]
            d_value = dot(pt[h, :, here], d_mixed, 1, 1)
            d_key = dot(d_score, qcat[here, pair_of(h)])
            if q == 0:
                dv_sum[h] = d_value
                dk_sum[h] = d_key
            else:
                dv_sum[h] += d_value
                dk_sum[h] += d_key
            d_query = dot(kct[pair_of(h), :], d_score).T
            row_entity = kind_wide[here, :] == 1
            dqa[here, pair_of(h)] = jnp.where(row_entity, 0.0, d_query).astype(low)
            dqb[here, pair_of(h)] = jnp.where(row_entity, d_query, 0.0).astype(low)
            return carry

        lax.fori_loop(0, heads, head_step, 0)

    gfeed, gattn = r.gfeed, r.gattn
    blocks, per_block = gfeed.shape[0], gfeed.shape[1]

    def put_grad(packed, start, value):
        packed[:, :, start : start + value.shape[1]] = value.astype(low).reshape(blocks, per_block, value.shape[1])

    if planar:
        feed = PlaneReduce(gfeed, *r.feed)
        attn = PlaneReduce(gattn, *r.attn)

    attend(0)
    attend(1)
    turn()
    for step in range(3):
        gathers[0].relay(step)
    swap_weights()
    gathers[1].relay(0)
    for copy in ow_swap:
        copy.wait_recv()
    forward(0)
    gathers[1].relay(1)
    gathers[1].relay(2)
    ffn[0].forward(0)
    forward(1)
    ffn[0].forward(1)
    ffn[0].settle()
    ffn[1].forward(0)
    ffn[0].relay(0)
    ffn[0].relay(1)
    ffn[1].forward(1)
    ffn[0].relay(2)
    ffn[1].settle()
    backward(0)
    ffn[1].relay(0)
    ffn[1].relay(1)
    back[0].forward(0)
    ffn[1].relay(2)
    back[0].forward(1)
    back[0].settle()
    backward(1)
    back[0].relay(0)
    back[0].relay(1)
    back[0].relay(2)
    back[1].forward(0)
    put_grad(gfeed, hidden_width, dot(gf[...], act[...], 0, 0))
    back[1].forward(1)
    finish_rows(0)
    back[1].settle()
    put_grad(gfeed, 0, dot(hl[...], il[...], 0, 0))
    if planar:
        feed.start()
    for step in range(3):
        back[1].relay(step)
    if planar:
        feed.step_one()
    finish_rows(1)

    small = r.small
    for i in range(8):
        small[i : i + 1, :] = jnp.sum(acc[i], axis=0, keepdims=True)
    if planar:
        small_in, partners = r.small_in, (across, over_x, over_y)
        small_sum = r.small_sum
        tiny = [
            remote(
                small if s == 0 else small_sum.at[s - 1],
                small_in.at[s],
                r.small_send.at[s],
                r.small_recv.at[s],
                dp=partners[s],
            )
            for s in range(3)
        ]
        tiny[0].start()

    d_keys = [
        jnp.where(kind_wide[:, :HD] == 1, dk_sum[h, :, HD:], dk_sum[h, :, :HD]).astype(low) for h in range(heads)
    ]
    d_values = [dv_sum[h].astype(low) for h in range(heads)]
    dkv[...] = jnp.concatenate(d_keys + d_values, axis=1)
    wkv = jnp.concatenate([r.k_weight[...], r.v_weight[...]], axis=0)
    for q, (start, size) in enumerate(spans):
        here = pl.ds(start, size)
        share = dot(dqa[here, :], wa[...]) + dot(dqb[here, :], wb[...]) + dot(dkv[here, :], wkv)
        r.grad_part[here, :] = share.astype(low)
        grad[q].start()
    put_grad(gattn, 0, dot(tok_t[...], dqa[...]))
    put_grad(gattn, 2 * local_width, dot(tok_t[...], dqb[...]))
    grad[0].forward(0)
    put_grad(gattn, 4 * local_width, dot(tok_t[...], dkv[...]))
    o_grad = dot(gb[...], mloc[...], 0, 1)
    pad = gattn.shape[2] - 7 * local_width
    put_grad(gattn, 6 * local_width, jnp.concatenate([o_grad, jnp.zeros((width, pad), wide)], axis=1))
    grad[0].forward(1)
    if planar:
        attn.start()
        tiny[0].wait_recv()
        small_sum[0] = small[...] + small_in[0]
        tiny[1].start()
        feed.step_two()
    grad[0].settle(dr2)
    grad[1].forward(0)
    grad[0].relay(0)
    grad[0].relay(1)
    grad[1].forward(1)
    if planar:
        attn.step_one()
        tiny[1].wait_recv()
        small_sum[1] = small_sum[0] + small_in[1]
        tiny[2].start()
    grad[0].relay(2)
    grad[1].settle(dr2)
    if planar:
        feed_sum = feed.finish()
        r.in_grad[...] = feed_sum[:, :hidden_width]
        r.out_grad[...] = feed_sum[:, hidden_width:]
        attn.step_two()
    grad[1].relay(0)
    grad[1].relay(1)
    if planar:
        tiny[2].wait_recv()
        r.small_out[...] = small_sum[1] + small_in[2]
    grad[1].relay(2)
    if planar:
        attn_sum = attn.finish()
        for part in range(4):
            base = (part // 2) * 2 * local_width + (part % 2) * HD
            r.q_grad[part] = jnp.concatenate(
                [attn_sum[:, base + h * pair : base + h * pair + HD] for h in range(heads)], axis=1
            )
        both_grads = attn_sum[:, 4 * local_width : 6 * local_width]
        r.k_grad[...] = both_grads[:, :local_width]
        r.v_grad[...] = both_grads[:, local_width:]
        r.o_grad[...] = attn_sum[:, 6 * local_width : 7 * local_width].T
    else:
        r.small_out[...] = small[...]
        r.feed_out[...] = gfeed[...]
        r.attn_out[...] = gattn[...]
    for line in grad:
        line.arrive()
    for line in ffn + back + grad:
        line.drain()
    for gather in gathers:
        gather.drain()
    for copy in ow_line + ow_swap:
        copy.wait_send()
    if planar:
        for copy in tiny:
            copy.wait_send()


def hand_on(*refs):
    count = len(refs) // 2
    for source, target in zip(refs[:count], refs[count:]):
        target[...] = source[...]


def local(
    tokens,
    segment_ids,
    token_types,
    q_weight,
    k_weight,
    v_weight,
    o_weight,
    o_bias,
    norm1_gain,
    norm1_shift,
    in_weight,
    in_bias,
    out_weight,
    out_bias,
    norm2_gain,
    norm2_shift,
    cotangent,
):
    rows, width = tokens.shape
    local_width = k_weight.shape[1]
    heads = local_width // HD
    hidden_width = in_weight.shape[1]
    n_dp = lax.axis_size("dp")
    planar = n_dp == 8
    blocks = 8
    per_block = width // blocks
    spans = portions_of(rows)
    largest = max(size for _, size in spans)
    low, wide = jnp.bfloat16, jnp.float32
    attn_width = -(-7 * local_width // 128) * 128
    args = dict(
        tokens=tokens,
        seg_row=segment_ids,
        kind_row=token_types,
        q_weight=q_weight.swapaxes(1, 2),
        k_weight=k_weight.T,
        v_weight=v_weight.T,
        o_weight=o_weight,
        o_bias=o_bias,
        gain1=norm1_gain,
        shift1=norm1_shift,
        in_bias=in_bias,
        out_bias=out_bias,
        gain2=norm2_gain,
        shift2=norm2_shift,
        in_weight=in_weight,
        out_weight=out_weight,
        cotangent=cotangent,
    )
    shaped = jax.ShapeDtypeStruct
    outs = dict(
        layer_out=shaped((rows, width), low),
        tokens_grad=shaped((rows, width), low),
        small_out=shaped((8, width), wide),
    )
    if planar:
        outs |= dict(
            q_grad=shaped((4, per_block, local_width), wide),
            k_grad=shaped((per_block, local_width), wide),
            v_grad=shaped((per_block, local_width), wide),
            o_grad=shaped((local_width, per_block), wide),
            in_grad=shaped((per_block, hidden_width), wide),
            out_grad=shaped((per_block, hidden_width), wide),
        )
    else:
        outs |= dict(
            feed_out=shaped((blocks, per_block, 2 * hidden_width), low),
            attn_out=shaped((blocks, per_block, attn_width), low),
        )
    dma = pltpu.SemaphoreType.DMA
    scratch = dict(
        ow=pltpu.VMEM((LINE, local_width, width), low),
        ow_send=dma((6,)),
        ow_recv=dma((6,)),
        wa=pltpu.VMEM((2 * local_width, width), low),
        wb=pltpu.VMEM((2 * local_width, width), low),
        wk=pltpu.VMEM((2 * local_width, width), low),
        kind_wide=pltpu.VMEM((rows, 2 * HD), jnp.int32),
        seg_wide=pltpu.VMEM((rows, 2 * HD), jnp.int32),
        qcat=pltpu.VMEM((rows, 2 * local_width), low),
        kcat=pltpu.VMEM((rows, 2 * local_width), low),
        vt=pltpu.VMEM((local_width, rows), low),
        pt=pltpu.VMEM((heads, rows, rows), low),
        mx=[pltpu.VMEM((LINE, local_width, size), low) for _, size in spans],
        st=pltpu.VMEM((rows, largest), wide),
        ds=pltpu.VMEM((rows, largest), low),
        mloc=pltpu.VMEM((local_width, rows), low),
        mx_send=dma((len(spans), 5)),
        mx_recv=dma((len(spans), LINE)),
        tok_t=pltpu.VMEM((width, rows), low),
        xh1=pltpu.VMEM((rows, width), wide),
        rstd1=pltpu.VMEM((rows, 128), wide),
        hl=pltpu.VMEM((rows, width), low),
        act=pltpu.VMEM((rows, hidden_width), low),
        gp=pltpu.VMEM((rows, hidden_width), wide),
        dr2=pltpu.VMEM((rows, width), wide),
        gf=pltpu.VMEM((rows, width), low),
        il=pltpu.VMEM((rows, hidden_width), low),
        tmp=pltpu.VMEM((largest, width), wide),
        vec=pltpu.VMEM((8, width), wide),
        acc=pltpu.VMEM((8, 8, width), wide),
        gb=pltpu.VMEM((rows, width), low),
        ffn_part=pltpu.VMEM((rows, width), low),
        back_part=pltpu.VMEM((rows, width), low),
        grad_part=pltpu.VMEM((rows, width), low),
        ffn_out=pltpu.VMEM((rows, width), low),
        back_out=pltpu.VMEM((rows, width), low),
        gfeed=pltpu.VMEM((blocks, per_block, 2 * hidden_width), low),
        gattn=pltpu.VMEM((blocks, per_block, attn_width), low),
        small=pltpu.VMEM((8, width), wide),
        kct=pltpu.VMEM((2 * local_width, rows), low),
        vn=pltpu.VMEM((heads, rows, HD), low),
        dmt=pltpu.VMEM((local_width, rows), low),
        dk_sum=pltpu.VMEM((heads, rows, 2 * HD), wide),
        dv_sum=pltpu.VMEM((heads, rows, HD), wide),
        dqa=pltpu.VMEM((rows, 2 * local_width), low),
        dqb=pltpu.VMEM((rows, 2 * local_width), low),
        dkv=pltpu.VMEM((rows, 2 * local_width), low),
    )
    for name in ("ffn", "back", "grad"):
        scratch[name] = [line_scratch(size // LINE, width) for _, size in spans]
    if planar:
        scratch |= dict(
            feed=plane_scratch(per_block, 2 * hidden_width),
            attn=plane_scratch(per_block, attn_width),
            small_in=pltpu.VMEM((3, 8, width), wide),
            small_sum=pltpu.VMEM((2, 8, width), wide),
            small_send=dma((3,)),
            small_recv=dma((3,)),
        )
    layout = jax.tree.structure((args, outs, scratch))
    vm = pl.BlockSpec(memory_space=pltpu.VMEM)
    results = pl.pallas_call(
        functools.partial(layer_kernel, planar, layout),
        out_shape=jax.tree.leaves(outs),
        in_specs=[vm] * len(args),
        out_specs=[vm] * len(outs),
        scratch_shapes=jax.tree.leaves(scratch),
        compiler_params=pltpu.CompilerParams(
            collective_id=0, has_side_effects=True, vmem_limit_bytes=VMEM_LIMIT
        ),
    )(*jax.tree.leaves(args))
    results = dict(zip(sorted(outs), results))
    if planar:
        small = results.pop("small_out")
        flat, tree = jax.tree.flatten(results)
        flat = pl.pallas_call(
            hand_on,
            out_shape=[shaped(a.shape, a.dtype) for a in flat],
            in_specs=[vm] * len(flat),
            out_specs=[vm] * len(flat),
            compiler_params=pltpu.CompilerParams(vmem_limit_bytes=VMEM_LIMIT),
        )(*flat)
        results = jax.tree.unflatten(tree, flat) | {"small_out": small}
    res = types.SimpleNamespace(**results)
    small = res.small_out
    if planar:
        grads = (res.q_grad, res.k_grad, res.v_grad, res.o_grad, res.in_grad, res.out_grad.T)
    else:
        feed = res.feed_out.astype(wide).reshape(width, 2 * hidden_width)
        attn = res.attn_out.astype(wide).reshape(width, attn_width)
        feed = lax.psum_scatter(feed, "dp", scatter_dimension=0, tiled=True)
        attn = lax.psum_scatter(attn, "dp", scatter_dimension=0, tiled=True)
        small = lax.psum(small, "dp")
        per = feed.shape[0]
        queries = attn[:, : 4 * local_width].reshape(per, 2, heads, 2, HD)
        queries = queries.transpose(1, 3, 0, 2, 4).reshape(4, per, local_width)
        grads = (
            queries,
            attn[:, 4 * local_width : 5 * local_width],
            attn[:, 5 * local_width : 6 * local_width],
            attn[:, 6 * local_width : 7 * local_width].T,
            feed[:, :hidden_width],
            feed[:, hidden_width:].T,
        )
    d_q, d_k, d_v, d_o, d_in, d_out = grads
    return (
        res.layer_out,
        res.tokens_grad,
        d_q,
        d_k,
        d_v,
        d_o,
        small[0],
        small[1],
        small[2],
        d_in,
        small[3],
        d_out,
        small[4],
        small[5],
        small[6],
    )


def solution(mesh):
    return jax.shard_map(
        local,
        mesh=mesh,
        in_specs=(
            P("dp", None),
            P("dp", None),
            P("dp", None),
            P(None, None, "mp"),
            P(None, "mp"),
            P(None, "mp"),
            P("mp", None),
            P(),
            P(),
            P(),
            P(None, "mp"),
            P("mp"),
            P("mp", None),
            P(),
            P(),
            P(),
            P("dp", None),
        ),
        out_specs=(
            P("dp", None),
            P("dp", None),
            P(None, "dp", "mp"),
            P("dp", "mp"),
            P("dp", "mp"),
            P("mp", "dp"),
            P(),
            P(),
            P(),
            P("dp", "mp"),
            P("mp"),
            P("mp", "dp"),
            P(),
            P(),
            P(),
        ),
        check_vma=False,
    )
```

```python
import functools
import math
import operator
import types

import jax
import jax.numpy as jnp
from jax import lax
from jax.experimental import pallas as pl
from jax.experimental.pallas import tpu as pltpu
from jax.sharding import PartitionSpec as P

HD = 64
LINE = 4
PORTIONS = (1, 1, 1, 1, 1)
LANES = 128
CHUNK = 32
VMEM_LIMIT = 67043328

norm_epsilon = 1e-05


def remote(src, dst, send_sem, recv_sem, **axes):
    return pltpu.make_async_remote_copy(
        src_ref=src,
        dst_ref=dst,
        send_sem=send_sem,
        recv_sem=recv_sem,
        device_id=axes,
        device_id_type=pl.DeviceIdType.MESH,
    )


class Place:
    def __init__(self):
        me = lax.axis_index("mp")
        self.me = me
        self.is_mid = jnp.logical_or(me == 1, me == 2)
        self.is_end = jnp.logical_not(self.is_mid)
        left = me < 2
        self.mid = jnp.where(left, 1, 2)
        self.end = jnp.where(left, 0, 3)
        self.far_mid = 3 - self.mid
        self.far_end = 3 - self.end


class LineGather:
    def __init__(self, place, send, recv, out):
        self.at, self.send, self.recv, self.out = place, send, recv, out

    def copy(self, block, slot, target):
        return remote(self.out(block), self.out(block), self.send.at[slot], self.recv.at[block], mp=target)

    def spread(self):
        at = self.at

        @pl.when(at.is_end)
        def _():
            self.copy(at.me, 0, at.mid).start()

        @pl.when(at.is_mid)
        def _():
            self.copy(at.me, 0, at.end).start()
            self.copy(at.me, 1, at.far_mid).start()

    def relay(self, step):
        at = self.at
        block = (at.end, at.far_mid, at.far_end)[step]
        target = (at.far_mid, at.end, at.end)[step]

        @pl.when(at.is_mid)
        def _():
            self.copy(block, 2 + step, target).wait_recv()
            self.copy(block, 2 + step, target).start()

    def arrive(self):
        at = self.at

        @pl.when(at.is_end)
        def _():
            self.copy(at.mid, 0, at.mid).wait_recv()
            self.copy(at.far_mid, 0, at.mid).wait_recv()
            self.copy(at.far_end, 0, at.mid).wait_recv()

    def drain(self):
        at = self.at

        @pl.when(at.is_end)
        def _():
            self.copy(at.me, 0, at.mid).wait_send()

        @pl.when(at.is_mid)
        def _():
            for slot in range(5):
                self.copy(at.me, slot, at.end).wait_send()


class LineReduce:
    def __init__(self, place, part, carry, single, summed, send, recv, start, block_rows, out):
        self.at, self.carry, self.single, self.summed = place, carry, single, summed
        self.send, self.recv = send, recv

        def rows_of(block):
            return pl.ds(pl.multiple_of(start + block * block_rows, 16), block_rows)

        self.rows_of, self.part_ref, self.out_ref = rows_of, part, out
        self.gather = LineGather(place, send.at[1], recv.at[1], lambda block: out.at[rows_of(block)])

    def part(self, block):
        return self.part_ref.at[self.rows_of(block)]

    def end_sends(self):
        at, send, recv = self.at, self.send, self.recv
        return (
            remote(self.part(at.far_end), self.carry.at[0], send.at[0, 0], recv.at[0, 2], mp=at.mid),
            remote(self.part(at.far_mid), self.carry.at[1], send.at[0, 1], recv.at[0, 3], mp=at.mid),
            remote(self.part(at.mid), self.single, send.at[0, 2], recv.at[0, 0], mp=at.mid),
        )

    def mid_sends(self):
        at, send, recv = self.at, self.send, self.recv
        return (
            remote(self.carry.at[0], self.summed, send.at[0, 1], recv.at[0, 1], mp=at.far_end),
            remote(self.carry.at[1], self.summed, send.at[0, 2], recv.at[0, 1], mp=at.far_mid),
            remote(self.part(at.end), self.single, send.at[0, 0], recv.at[0, 0], mp=at.end),
        )

    def start(self):
        @pl.when(self.at.is_end)
        def _():
            for copy in self.end_sends():
                copy.start()

        @pl.when(self.at.is_mid)
        def _():
            self.mid_sends()[2].start()

    def forward(self, step):
        at = self.at

        @pl.when(at.is_mid)
        def _():
            block = (at.far_end, at.far_mid)[step]
            self.end_sends()[step].wait_recv()
            total = self.carry[step].astype(jnp.float32) + self.part(block)[...].astype(jnp.float32)
            self.carry[step] = total.astype(jnp.bfloat16)
            self.mid_sends()[step].start()

    def settle(self, extra=None):
        at = self.at
        self.end_sends()[2].wait_recv()
        self.mid_sends()[0].wait_recv()
        total = (
            self.part(at.me)[...].astype(jnp.float32)
            + self.single[...].astype(jnp.float32)
            + self.summed[...].astype(jnp.float32)
        )
        if extra is not None:
            total = total + extra[self.rows_of(at.me), :]
        self.out_ref[self.rows_of(at.me), :] = total.astype(jnp.bfloat16)
        self.gather.spread()

    def relay(self, step):
        self.gather.relay(step)

    def arrive(self):
        self.gather.arrive()

    def drain(self):
        @pl.when(self.at.is_end)
        def _():
            for copy in self.end_sends():
                copy.wait_send()

        @pl.when(self.at.is_mid)
        def _():
            for copy in self.mid_sends():
                copy.wait_send()

        self.gather.drain()


def line_scratch(rows, width):
    return [
        pltpu.VMEM((2, rows, width), jnp.bfloat16),
        pltpu.VMEM((rows, width), jnp.bfloat16),
        pltpu.VMEM((rows, width), jnp.bfloat16),
        pltpu.SemaphoreType.DMA((2, 5)),
        pltpu.SemaphoreType.DMA((2, 4)),
    ]


class PlaneReduce:
    def __init__(self, grads, r1, sums, mid2, r2a, r2b, s3a, s3b, r3a, r3b, send, recv):
        self.grads, self.r1, self.sums, self.mid2 = grads, r1, sums, mid2
        self.r2a, self.r2b, self.s3a, self.s3b, self.r3a, self.r3b = r2a, r2b, s3a, s3b, r3a, r3b
        dp = lax.axis_index("dp")
        self.core, self.x, self.y = lax.rem(dp, 2), lax.rem(dp // 2, 2), dp // 4
        across = dp + 1 - 2 * self.core
        over_x = dp + 2 - 4 * self.x
        over_y = dp + 4 - 8 * self.y
        half = r2a.shape[2]
        self.low, self.high = pl.ds(0, half), pl.ds(half, grads.shape[2] - half)
        self.first = [
            remote(grads.at[2 * k + 1 - self.core], r1.at[k], send.at[k], recv.at[k], dp=across) for k in range(4)
        ]
        self.second = [
            remote(mid2.at[2 * j + 1 - self.x, :, self.low], r2a.at[j], send.at[4 + j], recv.at[4 + j], dp=over_x)
            for j in range(2)
        ] + [
            remote(mid2.at[2 * (1 - self.y) + j, :, self.high], r2b.at[j], send.at[6 + j], recv.at[6 + j], dp=over_y)
            for j in range(2)
        ]
        self.third = [
            remote(s3a, r3a, send.at[8], recv.at[8], dp=over_y),
            remote(s3b, r3b, send.at[9], recv.at[9], dp=over_x),
        ]

    def start(self):
        for copy in self.first:
            copy.start()

    def step_one(self):
        for copy in self.first:
            copy.wait_recv()

        def body(k, carry):
            total = self.grads[2 * k + self.core].astype(jnp.float32) + self.r1[k].astype(jnp.float32)
            self.sums[k] = total
            self.mid2[k] = total.astype(jnp.bfloat16)
            return carry

        lax.fori_loop(0, 4, body, 0)
        for copy in self.second:
            copy.start()

    def step_two(self):
        for copy in self.second:
            copy.wait_recv()
        x, y = self.x, self.y
        self.s3a[...] = (
            self.sums[2 * (1 - y) + x, :, self.low] + self.r2a[1 - y].astype(jnp.float32)
        ).astype(jnp.bfloat16)
        self.third[0].start()
        self.s3b[...] = (
            self.sums[2 * y + 1 - x, :, self.high] + self.r2b[1 - x].astype(jnp.float32)
        ).astype(jnp.bfloat16)
        self.third[1].start()

    def finish(self):
        x, y = self.x, self.y
        for copy in self.third:
            copy.wait_recv()
        own = self.sums.at[2 * y + x]
        own[:, self.low] = own[:, self.low] + self.r2a[y].astype(jnp.float32) + self.r3a[...].astype(jnp.float32)
        own[:, self.high] = own[:, self.high] + self.r2b[x].astype(jnp.float32) + self.r3b[...].astype(jnp.float32)
        for copy in self.first + self.second + self.third:
            copy.wait_send()
        return own


def plane_scratch(rows, width):
    half = (width // 128 + 1) // 2 * 128
    rest = width - half
    low = jnp.bfloat16
    return [
        pltpu.VMEM((4, rows, width), low),
        pltpu.VMEM((4, rows, width), jnp.float32),
        pltpu.VMEM((4, rows, width), low),
        pltpu.VMEM((2, rows, half), low),
        pltpu.VMEM((2, rows, rest), low),
        pltpu.VMEM((rows, half), low),
        pltpu.VMEM((rows, rest), low),
        pltpu.VMEM((rows, half), low),
        pltpu.VMEM((rows, rest), low),
        pltpu.SemaphoreType.DMA((10,)),
        pltpu.SemaphoreType.DMA((10,)),
    ]


def dot(left, right, left_dim=1, right_dim=0):
    return lax.dot_general(
        left, right, (((left_dim,), (right_dim,)), ((), ())), preferred_element_type=jnp.float32
    )


def rows_loop(start, count, body):
    def step(i, carry):
        inside = pl.ds(pl.multiple_of(i * CHUNK, CHUNK), CHUNK)
        body(pl.ds(pl.multiple_of(start + i * CHUNK, CHUNK), CHUNK), inside)
        return carry

    lax.fori_loop(0, count // CHUNK, step, 0)


def fold(value):
    return jnp.sum(value.reshape(value.shape[0] // 8, 8, value.shape[1]), axis=0)


def row_mean(value):
    return jnp.mean(value, axis=-1, keepdims=True)


def portions_of(rows):
    unit = rows // sum(PORTIONS)
    return [(unit * sum(PORTIONS[:i]), unit * size) for i, size in enumerate(PORTIONS)]


def layer_kernel(planar, layout, *refs):
    r = types.SimpleNamespace(**functools.reduce(operator.or_, jax.tree.unflatten(layout, refs)))
    tokens, rows, width = r.tokens, r.tokens.shape[0], r.tokens.shape[1]
    local_width = r.k_weight.shape[0]
    heads = local_width // HD
    pair = 2 * HD
    hidden_width = r.in_weight.shape[1]
    spans = portions_of(rows)
    low, wide = jnp.bfloat16, jnp.float32
    at = Place()
    me = at.me
    dp = lax.axis_index("dp")
    core = lax.rem(dp, 2)
    across = dp + 1 - 2 * core

    barrier = pltpu.get_barrier_semaphore()
    near = lax.rem(dp // 2, 2)
    over_x = dp + 2 - 4 * near
    peers = [{"mp": lax.rem(me + step, LINE)} for step in range(1, LINE)] + [{"dp": across}, {"dp": over_x}]
    if planar:
        over_y = dp + 4 - 8 * (dp // 4)
        peers += [{"dp": over_y}]
    for peer in peers:
        pl.semaphore_signal(barrier, inc=1, device_id=peer, device_id_type=pl.DeviceIdType.MESH)

    late = [
        pltpu.make_async_copy(source, target, r.late_sem.at[i])
        for i, (source, target) in enumerate(
            ((r.in_weight, r.in_w), (r.out_weight, r.out_w), (r.cotangent, r.cot_in))
        )
    ]
    for copy in late:
        copy.start()

    vec = r.vec
    for i, name in enumerate((r.o_bias, r.gain1, r.shift1, r.in_bias, r.out_bias, r.gain2, r.shift2)):
        vec[i, :] = name[...]
    o_bias, gain1, shift1, in_bias, out_bias, gain2, shift2 = (vec[i : i + 1, :] for i in range(7))
    wa, wb, wk = r.wa, r.wb, r.wk
    for h in range(heads):
        cols = slice(h * HD, (h + 1) * HD)
        both = slice(h * pair, (h + 1) * pair)
        wa[both, :] = jnp.concatenate([r.q_weight[0, cols, :], r.q_weight[1, cols, :]], axis=0)
        wb[both, :] = jnp.concatenate([r.q_weight[2, cols, :], r.q_weight[3, cols, :]], axis=0)
        key_part = r.k_weight[cols, :]
        wk[both, :] = jnp.concatenate([key_part, key_part], axis=0)
    pl.semaphore_wait(barrier, len(peers))

    ow, ow_send, ow_recv = r.ow, r.ow_send, r.ow_recv
    share = local_width // 4
    quarter = pl.ds(pl.multiple_of((2 * core + near) * share, 16), share)
    pairs = pl.ds(pl.multiple_of(2 * core * share, 16), 2 * share)
    ow_line, ow_plane, ow_chip = [], [], []
    for step in range(1, LINE):
        source, i = lax.rem(me + LINE - step, LINE), step - 1
        ow_line.append(
            remote(
                r.o_weight.at[quarter], ow.at[me, quarter], ow_send.at[i], ow_recv.at[i], mp=lax.rem(me + step, LINE)
            )
        )
        held = ow.at[source, quarter]
        ow_plane.append(remote(held, held, ow_send.at[3 + i], ow_recv.at[3 + i], dp=over_x))
        held = ow.at[source, pairs]
        ow_chip.append(remote(held, held, ow_send.at[6 + i], ow_recv.at[6 + i], dp=across))
    for copy in ow_line:
        copy.start()

    kind_wide, seg_wide = r.kind_wide, r.seg_wide
    kind_wide[...] = jnp.broadcast_to(r.kind_row[...], (pair, rows)).T
    seg_wide[...] = jnp.broadcast_to(r.seg_row[...], (pair, rows)).T
    qcat, kcat, vt = r.qcat, r.kcat, r.vt
    tok = tokens[...]
    entity = kind_wide[...] == 1
    upper = lax.broadcasted_iota(jnp.int32, (rows, pair), 1) >= HD
    keys = dot(tok, wk[...], 1, 1)
    for h in range(heads):
        both = slice(h * pair, (h + 1) * pair)
        kcat[:, both] = jnp.where(entity == upper, keys[:, both], 0.0).astype(low)
    vt[...] = dot(r.v_weight[...], tok, 1, 1).astype(low)
    q_plain = dot(tok, wa[...], 1, 1)
    q_entity = dot(tok, wb[...], 1, 1)
    for h in range(heads):
        both = slice(h * pair, (h + 1) * pair)
        qcat[:, both] = jnp.where(entity, q_entity[:, both], q_plain[:, both]).astype(low)

    pt, mx, mloc, st = r.pt, r.mx, r.mloc, r.st
    scale = HD ** (-0.5)
    gathers = [
        LineGather(at, r.mx_send.at[q], r.mx_recv.at[q], lambda block, q=q: mx[q].at[block])
        for q in range(len(spans))
    ]

    def pair_of(h):
        return pl.ds(pl.multiple_of(h * pair, pair), pair)

    def head_of(h):
        return pl.ds(pl.multiple_of(h * HD, HD), HD)

    def attend(q):
        start, size = spans[q]
        here = pl.ds(start, size)

        def head_step(h, carry):
            st[:, :size] = dot(kcat[:, pair_of(h)], qcat[here, pair_of(h)], 1, 1)

            def soften(i, carry):
                cols = pl.ds(pl.multiple_of(i * LANES, LANES), LANES)
                span = pl.ds(pl.multiple_of(start + i * LANES, LANES), LANES)
                scores = jnp.where(seg_wide[...] == r.seg_row[:, span], st[:, cols] * scale, -1000000000.0)
                shifted = jnp.exp(scores - jnp.max(scores, axis=0, keepdims=True))
                total = jnp.sum(shifted, axis=0, keepdims=True)
                pt[h, :, span] = (shifted * (1.0 / total)).astype(low)
                return carry

            lax.fori_loop(0, size // LANES, soften, 0)
            mixed = dot(vt[head_of(h), :], pt[h, :, here]).astype(low)
            mx[q][me, head_of(h), :] = mixed
            mloc[head_of(h), here] = mixed
            return carry

        lax.fori_loop(0, heads, head_step, 0)
        gathers[q].spread()

    def swap_plane():
        ow[me] = r.o_weight[...]
        for copy in ow_line:
            copy.wait_recv()
        for copy in ow_plane:
            copy.start()

    def swap_chip():
        for copy in ow_plane:
            copy.wait_recv()
        for copy in ow_chip:
            copy.start()

    def own_weights():
        for copy in ow_chip:
            copy.wait_recv()
        late[0].wait()
        late[1].wait()

    tok_t, kct, vn = r.tok_t, r.kct, r.vn

    def turn():
        tok_t[...] = tokens[...].T
        kct[...] = kcat[...].T
        for h in range(heads):
            vn[h] = vt[h * HD : (h + 1) * HD, :].T

    xh1, rstd1, hl = r.xh1, r.rstd1, r.hl
    act, gp, dr2, gf, il, gb, tmp, acc = r.act, r.gp, r.dr2, r.gf, r.il, r.gb, r.tmp, r.acc
    acc[...] = jnp.zeros_like(acc)

    def make_lines(parts, part, out):
        return [
            LineReduce(at, part, *parts[q], start, size // LINE, out) for q, (start, size) in enumerate(spans)
        ]

    ffn = make_lines(r.ffn, r.ffn_part, r.ffn_out)
    back = make_lines(r.back, r.back_part, r.back_out)
    grad = make_lines(r.grad, r.grad_part, r.tokens_grad)

    root_half = math.sqrt(0.5)
    density = 1.0 / math.sqrt(2.0 * math.pi)

    def forward(q):
        gathers[q].arrive()
        start, size = spans[q]
        here = pl.ds(start, size)
        mixed = mx[q][...].reshape(LINE * local_width, size)
        tmp[:size, :] = dot(mixed, ow[...].reshape(LINE * local_width, width), 0, 0)

        def first_norm(at_rows, inside):
            value = tmp[inside, :] + tokens[at_rows, :].astype(wide) + o_bias
            centred = value - row_mean(value)
            scaled = lax.rsqrt(row_mean(centred * centred) + norm_epsilon)
            normal = centred * scaled
            xh1[at_rows, :] = normal
            rstd1[at_rows, :] = jnp.broadcast_to(scaled, (CHUNK, 128))
            hl[at_rows, :] = (normal * gain1 + shift1).astype(low)

        rows_loop(start, size, first_norm)
        tmp[:size, :] = dot(hl[here, :], r.in_w[...])

        def activate(at_rows, inside):
            inner = tmp[inside, :] + in_bias
            gate = 0.5 + 0.5 * lax.erf(inner * root_half)
            act[at_rows, :] = (inner * gate).astype(low)
            gp[at_rows, :] = gate + inner * (density * jnp.exp(-0.5 * inner * inner))

        rows_loop(start, size, activate)
        r.ffn_part[here, :] = dot(act[here, :], r.out_w[...]).astype(low)
        ffn[q].start()

    def backward(q):
        ffn[q].arrive()
        start, size = spans[q]
        here = pl.ds(start, size)

        def second_norm(at_rows, inside):
            value = xh1[at_rows, :] * gain1 + shift1
            value = value + r.ffn_out[at_rows, :].astype(wide) + out_bias
            centred = value - row_mean(value)
            scaled = lax.rsqrt(row_mean(centred * centred) + norm_epsilon)
            normal = centred * scaled
            r.layer_out[at_rows, :] = (normal * gain2 + shift2).astype(low)
            cot = r.cot_in[at_rows, :].astype(wide)
            acc[6] += fold(cot)
            acc[5] += fold(cot * normal)
            grown = cot * gain2
            grad_in = scaled * (grown - row_mean(grown) - normal * row_mean(grown * normal))
            acc[4] += fold(grad_in)
            dr2[at_rows, :] = grad_in
            gf[at_rows, :] = grad_in.astype(low)

        rows_loop(start, size, second_norm)
        tmp[:size, :] = dot(gf[here, :], r.out_w[...], 1, 1)

        def inner_step(at_rows, inside):
            d_inner = tmp[inside, :] * gp[at_rows, :]
            acc[3] += fold(d_inner)
            il[at_rows, :] = d_inner.astype(low)

        rows_loop(start, size, inner_step)
        r.back_part[here, :] = dot(il[here, :], r.in_w[...], 1, 1).astype(low)
        back[q].start()

    dqa, dqb, dkv, dk_sum, dv_sum = r.dqa, r.dqb, r.dkv, r.dk_sum, r.dv_sum
    dmt, ds = r.dmt, r.ds

    def finish_rows(q):
        back[q].arrive()
        start, size = spans[q]
        here = pl.ds(start, size)

        def last_norm(at_rows, inside):
            d_hidden = dr2[at_rows, :] + r.back_out[at_rows, :].astype(wide)
            normal = xh1[at_rows, :]
            acc[2] += fold(d_hidden)
            acc[1] += fold(d_hidden * normal)
            grown = d_hidden * gain1
            grad_in = rstd1[at_rows, 0:1] * (grown - row_mean(grown) - normal * row_mean(grown * normal))
            acc[0] += fold(grad_in)
            dr2[at_rows, :] = grad_in
            gb[at_rows, :] = grad_in.astype(low)

        rows_loop(start, size, last_norm)
        dmt[:, here] = dot(r.o_weight[...], gb[here, :], 1, 1).astype(low)

        def head_step(h, carry):
            d_mixed = dmt[head_of(h), here]
            st[:, :size] = dot(vn[h], d_mixed)

            def harden(i, carry):
                cols = pl.ds(pl.multiple_of(i * LANES, LANES), LANES)
                span = pl.ds(pl.multiple_of(start + i * LANES, LANES), LANES)
                prob = pt[h, :, span].astype(wide)
                d_prob = st[:, cols]
                delta = jnp.sum(prob * d_prob, axis=0, keepdims=True)
                ds[:, cols] = (prob * (d_prob - delta) * scale).astype(low)
                return carry

            lax.fori_loop(0, size // LANES, harden, 0)
            d_score = ds[:, :size]
            d_value = dot(pt[h, :, here], d_mixed, 1, 1)
            d_key = dot(d_score, qcat[here, pair_of(h)])
            if q == 0:
                dv_sum[h] = d_value
                dk_sum[h] = d_key
            else:
                dv_sum[h] += d_value
                dk_sum[h] += d_key
            d_query = dot(kct[pair_of(h), :], d_score).T
            row_entity = kind_wide[here, :] == 1
            dqa[here, pair_of(h)] = jnp.where(row_entity, 0.0, d_query).astype(low)
            dqb[here, pair_of(h)] = jnp.where(row_entity, d_query, 0.0).astype(low)
            return carry

        lax.fori_loop(0, heads, head_step, 0)

    gfeed, gattn = r.gfeed, r.gattn
    blocks, per_block = gfeed.shape[0], gfeed.shape[1]

    def put_grad(packed, start, value):
        packed[:, :, start : start + value.shape[1]] = value.astype(low).reshape(blocks, per_block, value.shape[1])

    if planar:
        feed = PlaneReduce(gfeed, *r.feed)
        attn = PlaneReduce(gattn, *r.attn)

    small = r.small
    if planar:
        small_sum = r.small_sum
        tiny = [
            remote(
                small if s == 0 else small_sum.at[s - 1],
                r.small_in.at[s],
                r.small_send.at[s],
                r.small_recv.at[s],
                dp=(across, over_x, over_y)[s],
            )
            for s in range(3)
        ]

    def tiny_step(s):
        if planar:
            tiny[s].wait_recv()
            small_sum[s] = (small if s == 0 else small_sum.at[s - 1])[...] + r.small_in[s]
            if s < 2:
                tiny[s + 1].start()

    def feed_step(i):
        if i == 0:
            put_grad(gfeed, hidden_width, dot(gf[...], act[...], 0, 0))
        elif i == 1:
            put_grad(gfeed, 0, dot(hl[...], il[...], 0, 0))
        elif planar and i == 2:
            feed.start()
        elif planar and i == 3:
            feed.step_one()
        elif planar and i == 4:
            feed.step_two()
        elif planar and i == 5:
            feed_sum = feed.finish()
            r.in_grad[...] = feed_sum[:, :hidden_width]
            r.out_grad[...] = feed_sum[:, hidden_width:]

    def key_grads():
        for i in range(8):
            small[i : i + 1, :] = jnp.sum(acc[i], axis=0, keepdims=True)
        if planar:
            tiny[0].start()
        d_keys = [
            jnp.where(kind_wide[:, :HD] == 1, dk_sum[h, :, HD:], dk_sum[h, :, :HD]).astype(low)
            for h in range(heads)
        ]
        d_values = [dv_sum[h].astype(low) for h in range(heads)]
        dkv[...] = jnp.concatenate(d_keys + d_values, axis=1)

    def input_share(q):
        start, size = spans[q]
        here = pl.ds(start, size)
        share = dot(dqa[here, :], wa[...]) + dot(dqb[here, :], wb[...])
        share = share + dot(dkv[here, :local_width], r.k_weight[...]) + dot(dkv[here, local_width:], r.v_weight[...])
        r.grad_part[here, :] = share.astype(low)
        grad[q].start()

    def attn_step(i):
        if i == 0:
            put_grad(gattn, 0, dot(tok_t[...], dqa[...]))
            put_grad(gattn, 2 * local_width, dot(tok_t[...], dqb[...]))
        elif i == 1:
            put_grad(gattn, 4 * local_width, dot(tok_t[...], dkv[...]))
            o_grad = dot(gb[...], mloc[...], 0, 1)
            pad = gattn.shape[2] - 7 * local_width
            put_grad(gattn, 6 * local_width, jnp.concatenate([o_grad, jnp.zeros((width, pad), wide)], axis=1))
        elif planar and i == 2:
            attn.start()
            tiny_step(0)
        elif planar and i == 3:
            attn.step_one()
            tiny_step(1)
        elif planar and i == 4:
            attn.step_two()
            tiny_step(2)

    attend(0)
    attend(1)
    gathers[0].relay(0)
    gathers[0].relay(1)
    swap_plane()
    attend(2)
    gathers[1].relay(0)
    gathers[0].relay(2)
    attend(3)
    gathers[3].relay(0)
    gathers[1].relay(1)
    gathers[1].relay(2)
    attend(4)
    gathers[4].relay(0)
    swap_chip()
    gathers[3].relay(1)
    gathers[3].relay(2)
    gathers[2].relay(0)
    gathers[4].relay(1)
    gathers[4].relay(2)
    gathers[2].relay(1)
    own_weights()
    forward(0)
    ffn[0].forward(0)
    ffn[0].forward(1)
    gathers[2].relay(2)
    forward(1)
    ffn[1].forward(0)
    forward(3)
    ffn[3].forward(0)
    ffn[1].forward(1)
    forward(4)
    ffn[0].settle()
    ffn[3].forward(1)
    ffn[4].forward(0)
    forward(2)
    ffn[0].relay(0)
    ffn[1].settle()
    ffn[2].forward(0)
    ffn[2].forward(1)
    ffn[0].relay(1)
    ffn[0].relay(2)
    ffn[1].relay(0)
    ffn[3].settle()
    ffn[1].relay(1)
    ffn[4].forward(1)
    ffn[3].relay(0)
    ffn[1].relay(2)
    ffn[2].settle()
    ffn[2].relay(0)
    ffn[3].relay(1)
    ffn[3].relay(2)
    ffn[4].settle()
    ffn[4].relay(0)
    ffn[2].relay(1)
    late[2].wait()
    backward(0)
    back[0].forward(0)
    ffn[2].relay(2)
    back[0].forward(1)
    backward(1)
    ffn[4].relay(1)
    back[1].forward(0)
    backward(3)
    back[1].forward(1)
    ffn[4].relay(2)
    back[3].forward(0)
    back[0].settle()
    backward(2)
    back[0].relay(0)
    back[3].forward(1)
    back[1].settle()
    back[2].forward(0)
    back[2].forward(1)
    back[0].relay(1)
    backward(4)
    back[1].relay(0)
    back[3].settle()
    feed_step(0)
    back[4].forward(0)
    back[1].relay(1)
    back[4].forward(1)
    back[0].relay(2)
    back[2].settle()
    turn()
    back[1].relay(2)
    back[3].relay(0)
    back[2].relay(0)
    back[4].settle()
    back[2].relay(1)
    feed_step(1)
    back[2].relay(2)
    back[3].relay(1)
    back[3].relay(2)
    feed_step(2)
    back[4].relay(0)
    finish_rows(0)
    back[4].relay(1)
    finish_rows(1)
    back[4].relay(2)
    finish_rows(2)
    finish_rows(3)
    finish_rows(4)
    key_grads()
    input_share(0)
    input_share(1)
    input_share(2)
    input_share(3)
    grad[0].forward(0)
    feed_step(3)
    grad[0].forward(1)
    input_share(4)
    attn_step(0)
    grad[1].forward(0)
    grad[1].forward(1)
    attn_step(1)
    grad[2].forward(0)
    grad[2].forward(1)
    grad[0].settle(dr2)
    attn_step(2)
    grad[3].forward(0)
    grad[3].forward(1)
    grad[2].settle(dr2)
    grad[4].forward(0)
    attn_step(3)
    grad[4].forward(1)
    grad[1].settle(dr2)
    feed_step(4)
    grad[3].settle(dr2)
    grad[0].relay(0)
    grad[0].relay(1)
    grad[4].settle(dr2)
    grad[2].relay(0)
    grad[1].relay(0)
    grad[2].relay(1)
    grad[1].relay(1)
    grad[3].relay(0)
    grad[4].relay(0)
    grad[0].relay(2)
    grad[3].relay(1)
    grad[2].relay(2)
    attn_step(4)
    grad[4].relay(1)
    grad[1].relay(2)
    grad[3].relay(2)
    grad[4].relay(2)
    feed_step(5)
    if planar:
        attn_sum = attn.finish()
        for part in range(4):
            base = (part // 2) * 2 * local_width + (part % 2) * HD
            r.q_grad[part] = jnp.concatenate(
                [attn_sum[:, base + h * pair : base + h * pair + HD] for h in range(heads)], axis=1
            )
        both_grads = attn_sum[:, 4 * local_width : 6 * local_width]
        r.k_grad[...] = both_grads[:, :local_width]
        r.v_grad[...] = both_grads[:, local_width:]
        r.o_grad[...] = attn_sum[:, 6 * local_width : 7 * local_width].T
        r.small_out[...] = small_sum[2]
    else:
        r.small_out[...] = small[...]
        r.feed_out[...] = gfeed[...]
        r.attn_out[...] = gattn[...]
    for line in grad:
        line.arrive()
    for line in ffn + back + grad:
        line.drain()
    for gather in gathers:
        gather.drain()
    for copy in ow_line + ow_plane + ow_chip:
        copy.wait_send()
    if planar:
        for copy in tiny:
            copy.wait_send()


def hand_on(count, vectors, small, *refs):
    sources, targets, rows_out, sems = refs[:count], refs[count : 2 * count], refs[2 * count : -1], refs[-1]
    copies = [pltpu.make_async_copy(sources[i], targets[i], sems.at[i]) for i in range(count)]
    for copy in copies:
        copy.start()
    for i in range(vectors):
        rows_out[i][...] = small[i, :]
    for copy in copies:
        copy.wait()


def local(
    tokens,
    segment_ids,
    token_types,
    q_weight,
    k_weight,
    v_weight,
    o_weight,
    o_bias,
    norm1_gain,
    norm1_shift,
    in_weight,
    in_bias,
    out_weight,
    out_bias,
    norm2_gain,
    norm2_shift,
    cotangent,
):
    rows, width = tokens.shape
    local_width = k_weight.shape[1]
    heads = local_width // HD
    hidden_width = in_weight.shape[1]
    n_dp = lax.axis_size("dp")
    planar = n_dp == 8
    blocks = 8
    per_block = width // blocks
    spans = portions_of(rows)
    largest = max(size for _, size in spans)
    low, wide = jnp.bfloat16, jnp.float32
    attn_width = -(-7 * local_width // 128) * 128
    args = dict(
        tokens=tokens,
        seg_row=segment_ids,
        kind_row=token_types,
        q_weight=q_weight.swapaxes(1, 2),
        k_weight=k_weight.T,
        v_weight=v_weight.T,
        o_weight=o_weight,
        o_bias=o_bias,
        gain1=norm1_gain,
        shift1=norm1_shift,
        in_bias=in_bias,
        out_bias=out_bias,
        gain2=norm2_gain,
        shift2=norm2_shift,
        in_weight=in_weight,
        out_weight=out_weight,
        cotangent=cotangent,
    )
    shaped = jax.ShapeDtypeStruct
    outs = dict(
        layer_out=shaped((rows, width), low),
        tokens_grad=shaped((rows, width), low),
        small_out=shaped((8, width), wide),
    )
    if planar:
        outs |= dict(
            q_grad=shaped((4, per_block, local_width), wide),
            k_grad=shaped((per_block, local_width), wide),
            v_grad=shaped((per_block, local_width), wide),
            o_grad=shaped((local_width, per_block), wide),
            in_grad=shaped((per_block, hidden_width), wide),
            out_grad=shaped((per_block, hidden_width), wide),
        )
    else:
        outs |= dict(
            feed_out=shaped((blocks, per_block, 2 * hidden_width), low),
            attn_out=shaped((blocks, per_block, attn_width), low),
        )
    dma = pltpu.SemaphoreType.DMA
    scratch = dict(
        ow=pltpu.VMEM((LINE, local_width, width), low),
        ow_send=dma((9,)),
        ow_recv=dma((9,)),
        wa=pltpu.VMEM((2 * local_width, width), low),
        wb=pltpu.VMEM((2 * local_width, width), low),
        wk=pltpu.VMEM((2 * local_width, width), low),
        kind_wide=pltpu.VMEM((rows, 2 * HD), jnp.int32),
        seg_wide=pltpu.VMEM((rows, 2 * HD), jnp.int32),
        qcat=pltpu.VMEM((rows, 2 * local_width), low),
        kcat=pltpu.VMEM((rows, 2 * local_width), low),
        vt=pltpu.VMEM((local_width, rows), low),
        pt=pltpu.VMEM((heads, rows, rows), low),
        mx=[pltpu.VMEM((LINE, local_width, size), low) for _, size in spans],
        st=pltpu.VMEM((rows, largest), wide),
        ds=pltpu.VMEM((rows, largest), low),
        mloc=pltpu.VMEM((local_width, rows), low),
        mx_send=dma((len(spans), 5)),
        mx_recv=dma((len(spans), LINE)),
        tok_t=pltpu.VMEM((width, rows), low),
        xh1=pltpu.VMEM((rows, width), wide),
        rstd1=pltpu.VMEM((rows, 128), wide),
        hl=pltpu.VMEM((rows, width), low),
        act=pltpu.VMEM((rows, hidden_width), low),
        gp=pltpu.VMEM((rows, hidden_width), wide),
        dr2=pltpu.VMEM((rows, width), wide),
        gf=pltpu.VMEM((rows, width), low),
        il=pltpu.VMEM((rows, hidden_width), low),
        in_w=pltpu.VMEM((width, hidden_width), low),
        out_w=pltpu.VMEM((hidden_width, width), low),
        cot_in=pltpu.VMEM((rows, width), low),
        late_sem=dma((3,)),
        tmp=pltpu.VMEM((largest, width), wide),
        vec=pltpu.VMEM((8, width), wide),
        acc=pltpu.VMEM((8, 8, width), wide),
        gb=pltpu.VMEM((rows, width), low),
        ffn_part=pltpu.VMEM((rows, width), low),
        back_part=pltpu.VMEM((rows, width), low),
        grad_part=pltpu.VMEM((rows, width), low),
        ffn_out=pltpu.VMEM((rows, width), low),
        back_out=pltpu.VMEM((rows, width), low),
        gfeed=pltpu.VMEM((blocks, per_block, 2 * hidden_width), low),
        gattn=pltpu.VMEM((blocks, per_block, attn_width), low),
        small=pltpu.VMEM((8, width), wide),
        kct=pltpu.VMEM((2 * local_width, rows), low),
        vn=pltpu.VMEM((heads, rows, HD), low),
        dmt=pltpu.VMEM((local_width, rows), low),
        dk_sum=pltpu.VMEM((heads, rows, 2 * HD), wide),
        dv_sum=pltpu.VMEM((heads, rows, HD), wide),
        dqa=pltpu.VMEM((rows, 2 * local_width), low),
        dqb=pltpu.VMEM((rows, 2 * local_width), low),
        dkv=pltpu.VMEM((rows, 2 * local_width), low),
    )
    for name in ("ffn", "back", "grad"):
        scratch[name] = [line_scratch(size // LINE, width) for _, size in spans]
    if planar:
        scratch |= dict(
            feed=plane_scratch(per_block, 2 * hidden_width),
            attn=plane_scratch(per_block, attn_width),
            small_in=pltpu.VMEM((3, 8, width), wide),
            small_sum=pltpu.VMEM((3, 8, width), wide),
            small_send=dma((3,)),
            small_recv=dma((3,)),
        )
    layout = jax.tree.structure((args, outs, scratch))
    vm, far = pl.BlockSpec(memory_space=pltpu.VMEM), pl.BlockSpec(memory_space=pl.ANY)
    results = pl.pallas_call(
        functools.partial(layer_kernel, planar, layout),
        out_shape=jax.tree.leaves(outs),
        in_specs=[far if name in ("in_weight", "out_weight", "cotangent") else vm for name in sorted(args)],
        out_specs=[vm] * len(outs),
        scratch_shapes=jax.tree.leaves(scratch),
        compiler_params=pltpu.CompilerParams(
            collective_id=0, has_side_effects=True, vmem_limit_bytes=VMEM_LIMIT
        ),
    )(*jax.tree.leaves(args))
    results = dict(zip(sorted(outs), results))
    if planar:
        small = results.pop("small_out")
        flat, tree = jax.tree.flatten(results)
        vectors = small.shape[0] - 1
        flat = pl.pallas_call(
            functools.partial(hand_on, len(flat), vectors),
            out_shape=[shaped(a.shape, a.dtype) for a in flat] + [shaped((width,), wide)] * vectors,
            in_specs=[vm] * (1 + len(flat)),
            out_specs=[far] * len(flat) + [vm] * vectors,
            scratch_shapes=[dma((len(flat),))],
            compiler_params=pltpu.CompilerParams(vmem_limit_bytes=16 * 1024 * 1024),
        )(small, *flat)
        small = flat[len(results) :]
        results = jax.tree.unflatten(tree, flat[: len(results)])
    res = types.SimpleNamespace(**results)
    if planar:
        grads = (res.q_grad, res.k_grad, res.v_grad, res.o_grad, res.in_grad, res.out_grad.T)
    else:
        feed = res.feed_out.astype(wide).reshape(width, 2 * hidden_width)
        attn = res.attn_out.astype(wide).reshape(width, attn_width)
        feed = lax.psum_scatter(feed, "dp", scatter_dimension=0, tiled=True)
        attn = lax.psum_scatter(attn, "dp", scatter_dimension=0, tiled=True)
        small = lax.psum(res.small_out, "dp")
        per = feed.shape[0]
        queries = attn[:, : 4 * local_width].reshape(per, 2, heads, 2, HD)
        queries = queries.transpose(1, 3, 0, 2, 4).reshape(4, per, local_width)
        grads = (
            queries,
            attn[:, 4 * local_width : 5 * local_width],
            attn[:, 5 * local_width : 6 * local_width],
            attn[:, 6 * local_width : 7 * local_width].T,
            feed[:, :hidden_width],
            feed[:, hidden_width:].T,
        )
    d_q, d_k, d_v, d_o, d_in, d_out = grads
    return (
        res.layer_out,
        res.tokens_grad,
        d_q,
        d_k,
        d_v,
        d_o,
        small[0],
        small[1],
        small[2],
        d_in,
        small[3],
        d_out,
        small[4],
        small[5],
        small[6],
    )


def solution(mesh):
    return jax.shard_map(
        local,
        mesh=mesh,
        in_specs=(
            P("dp", None),
            P("dp", None),
            P("dp", None),
            P(None, None, "mp"),
            P(None, "mp"),
            P(None, "mp"),
            P("mp", None),
            P(),
            P(),
            P(),
            P(None, "mp"),
            P("mp"),
            P("mp", None),
            P(),
            P(),
            P(),
            P("dp", None),
        ),
        out_specs=(
            P("dp", None),
            P("dp", None),
            P(None, "dp", "mp"),
            P("dp", "mp"),
            P("dp", "mp"),
            P("mp", "dp"),
            P(),
            P(),
            P(),
            P("dp", "mp"),
            P("mp"),
            P("mp", "dp"),
            P(),
            P(),
            P(),
        ),
        check_vma=False,
    )
```

```python
import functools
import math
import operator
import types

import jax
import jax.numpy as jnp
from jax import lax
from jax.experimental import pallas as pl
from jax.experimental.pallas import tpu as pltpu
from jax.sharding import PartitionSpec as P

HD = 64
LINE = 4
PORTIONS = (1, 1, 1, 1, 1)
LANES = 128
CHUNK = 32
VMEM_LIMIT = 67043328

norm_epsilon = 1e-05


def remote(src, dst, send_sem, recv_sem, **axes):
    return pltpu.make_async_remote_copy(
        src_ref=src,
        dst_ref=dst,
        send_sem=send_sem,
        recv_sem=recv_sem,
        device_id=axes,
        device_id_type=pl.DeviceIdType.MESH,
    )


class Place:
    def __init__(self):
        me = lax.axis_index("mp")
        self.me = me
        self.is_mid = jnp.logical_or(me == 1, me == 2)
        self.is_end = jnp.logical_not(self.is_mid)
        left = me < 2
        self.mid = jnp.where(left, 1, 2)
        self.end = jnp.where(left, 0, 3)
        self.far_mid = 3 - self.mid
        self.far_end = 3 - self.end


class LineGather:
    def __init__(self, place, send, recv, out):
        self.at, self.send, self.recv, self.out = place, send, recv, out

    def copy(self, block, slot, target):
        return remote(self.out(block), self.out(block), self.send.at[slot], self.recv.at[block], mp=target)

    def spread(self):
        at = self.at

        @pl.when(at.is_end)
        def _():
            self.copy(at.me, 0, at.mid).start()

        @pl.when(at.is_mid)
        def _():
            self.copy(at.me, 0, at.end).start()
            self.copy(at.me, 1, at.far_mid).start()

    def relay(self, step):
        at = self.at
        block = (at.end, at.far_mid, at.far_end)[step]
        target = (at.far_mid, at.end, at.end)[step]

        @pl.when(at.is_mid)
        def _():
            self.copy(block, 2 + step, target).wait_recv()
            self.copy(block, 2 + step, target).start()

    def arrive(self):
        at = self.at

        @pl.when(at.is_end)
        def _():
            self.copy(at.mid, 0, at.mid).wait_recv()
            self.copy(at.far_mid, 0, at.mid).wait_recv()
            self.copy(at.far_end, 0, at.mid).wait_recv()

    def drain(self):
        at = self.at

        @pl.when(at.is_end)
        def _():
            self.copy(at.me, 0, at.mid).wait_send()

        @pl.when(at.is_mid)
        def _():
            for slot in range(5):
                self.copy(at.me, slot, at.end).wait_send()


class LineReduce:
    def __init__(self, place, part, carry, single, summed, send, recv, start, block_rows, out):
        self.at, self.carry, self.single, self.summed = place, carry, single, summed
        self.send, self.recv = send, recv

        def rows_of(block):
            return pl.ds(pl.multiple_of(start + block * block_rows, 16), block_rows)

        self.rows_of, self.part_ref, self.out_ref = rows_of, part, out
        self.gather = LineGather(place, send.at[1], recv.at[1], lambda block: out.at[rows_of(block)])

    def part(self, block):
        return self.part_ref.at[self.rows_of(block)]

    def end_sends(self):
        at, send, recv = self.at, self.send, self.recv
        return (
            remote(self.part(at.far_end), self.carry.at[0], send.at[0, 0], recv.at[0, 2], mp=at.mid),
            remote(self.part(at.far_mid), self.carry.at[1], send.at[0, 1], recv.at[0, 3], mp=at.mid),
            remote(self.part(at.mid), self.single, send.at[0, 2], recv.at[0, 0], mp=at.mid),
        )

    def mid_sends(self):
        at, send, recv = self.at, self.send, self.recv
        return (
            remote(self.carry.at[0], self.summed, send.at[0, 1], recv.at[0, 1], mp=at.far_end),
            remote(self.carry.at[1], self.summed, send.at[0, 2], recv.at[0, 1], mp=at.far_mid),
            remote(self.part(at.end), self.single, send.at[0, 0], recv.at[0, 0], mp=at.end),
        )

    def start(self):
        @pl.when(self.at.is_end)
        def _():
            for copy in self.end_sends():
                copy.start()

        @pl.when(self.at.is_mid)
        def _():
            self.mid_sends()[2].start()

    def forward(self, step):
        at = self.at

        @pl.when(at.is_mid)
        def _():
            block = (at.far_end, at.far_mid)[step]
            self.end_sends()[step].wait_recv()
            total = self.carry[step].astype(jnp.float32) + self.part(block)[...].astype(jnp.float32)
            self.carry[step] = total.astype(jnp.bfloat16)
            self.mid_sends()[step].start()

    def settle(self, extra=None):
        at = self.at
        self.end_sends()[2].wait_recv()
        self.mid_sends()[0].wait_recv()
        total = (
            self.part(at.me)[...].astype(jnp.float32)
            + self.single[...].astype(jnp.float32)
            + self.summed[...].astype(jnp.float32)
        )
        if extra is not None:
            total = total + extra[self.rows_of(at.me), :]
        self.out_ref[self.rows_of(at.me), :] = total.astype(jnp.bfloat16)
        self.gather.spread()

    def relay(self, step):
        self.gather.relay(step)

    def arrive(self):
        self.gather.arrive()

    def drain(self):
        @pl.when(self.at.is_end)
        def _():
            for copy in self.end_sends():
                copy.wait_send()

        @pl.when(self.at.is_mid)
        def _():
            for copy in self.mid_sends():
                copy.wait_send()

        self.gather.drain()


def line_scratch(rows, width):
    return [
        pltpu.VMEM((2, rows, width), jnp.bfloat16),
        pltpu.VMEM((rows, width), jnp.bfloat16),
        pltpu.VMEM((rows, width), jnp.bfloat16),
        pltpu.SemaphoreType.DMA((2, 5)),
        pltpu.SemaphoreType.DMA((2, 4)),
    ]


class PlaneReduce:
    def __init__(self, grads, r1, sums, mid2, r2a, r2b, s3a, s3b, r3a, r3b, send, recv):
        self.grads, self.r1, self.sums, self.mid2 = grads, r1, sums, mid2
        self.r2a, self.r2b, self.s3a, self.s3b, self.r3a, self.r3b = r2a, r2b, s3a, s3b, r3a, r3b
        dp = lax.axis_index("dp")
        self.core, self.x, self.y = lax.rem(dp, 2), lax.rem(dp // 2, 2), dp // 4
        across = dp + 1 - 2 * self.core
        over_x = dp + 2 - 4 * self.x
        over_y = dp + 4 - 8 * self.y
        half = r2a.shape[2]
        self.low, self.high = pl.ds(0, half), pl.ds(half, grads.shape[2] - half)
        self.first = [
            remote(grads.at[2 * k + 1 - self.core], r1.at[k], send.at[k], recv.at[k], dp=across) for k in range(4)
        ]
        self.second = [
            remote(mid2.at[2 * j + 1 - self.x, :, self.low], r2a.at[j], send.at[4 + j], recv.at[4 + j], dp=over_x)
            for j in range(2)
        ] + [
            remote(mid2.at[2 * (1 - self.y) + j, :, self.high], r2b.at[j], send.at[6 + j], recv.at[6 + j], dp=over_y)
            for j in range(2)
        ]
        self.third = [
            remote(s3a, r3a, send.at[8], recv.at[8], dp=over_y),
            remote(s3b, r3b, send.at[9], recv.at[9], dp=over_x),
        ]

    def start(self):
        for copy in self.first:
            copy.start()

    def step_one(self):
        for copy in self.first:
            copy.wait_recv()

        def body(k, carry):
            total = self.grads[2 * k + self.core].astype(jnp.float32) + self.r1[k].astype(jnp.float32)
            self.sums[k] = total
            self.mid2[k] = total.astype(jnp.bfloat16)
            return carry

        lax.fori_loop(0, 4, body, 0)
        for copy in self.second:
            copy.start()

    def step_two(self):
        for copy in self.second:
            copy.wait_recv()
        x, y = self.x, self.y
        self.s3a[...] = (
            self.sums[2 * (1 - y) + x, :, self.low] + self.r2a[1 - y].astype(jnp.float32)
        ).astype(jnp.bfloat16)
        self.third[0].start()
        self.s3b[...] = (
            self.sums[2 * y + 1 - x, :, self.high] + self.r2b[1 - x].astype(jnp.float32)
        ).astype(jnp.bfloat16)
        self.third[1].start()

    def finish(self):
        x, y = self.x, self.y
        for copy in self.third:
            copy.wait_recv()
        own = self.sums.at[2 * y + x]
        own[:, self.low] = own[:, self.low] + self.r2a[y].astype(jnp.float32) + self.r3a[...].astype(jnp.float32)
        own[:, self.high] = own[:, self.high] + self.r2b[x].astype(jnp.float32) + self.r3b[...].astype(jnp.float32)
        for copy in self.first + self.second + self.third:
            copy.wait_send()
        return own


def plane_scratch(rows, width):
    half = (width // 128 + 1) // 2 * 128
    rest = width - half
    low = jnp.bfloat16
    return [
        pltpu.VMEM((4, rows, width), low),
        pltpu.VMEM((4, rows, width), jnp.float32),
        pltpu.VMEM((4, rows, width), low),
        pltpu.VMEM((2, rows, half), low),
        pltpu.VMEM((2, rows, rest), low),
        pltpu.VMEM((rows, half), low),
        pltpu.VMEM((rows, rest), low),
        pltpu.VMEM((rows, half), low),
        pltpu.VMEM((rows, rest), low),
        pltpu.SemaphoreType.DMA((10,)),
        pltpu.SemaphoreType.DMA((10,)),
    ]


def dot(left, right, left_dim=1, right_dim=0):
    return lax.dot_general(
        left, right, (((left_dim,), (right_dim,)), ((), ())), preferred_element_type=jnp.float32
    )


def rows_loop(start, count, body):
    def step(i, carry):
        inside = pl.ds(pl.multiple_of(i * CHUNK, CHUNK), CHUNK)
        body(pl.ds(pl.multiple_of(start + i * CHUNK, CHUNK), CHUNK), inside)
        return carry

    lax.fori_loop(0, count // CHUNK, step, 0)


def fold(value):
    return jnp.sum(value.reshape(value.shape[0] // 8, 8, value.shape[1]), axis=0)


def row_mean(value):
    return jnp.mean(value, axis=-1, keepdims=True)


def portions_of(rows):
    unit = rows // sum(PORTIONS)
    return [(unit * sum(PORTIONS[:i]), unit * size) for i, size in enumerate(PORTIONS)]


def layer_kernel(planar, layout, *refs):
    given, wanted, scratch = jax.tree.unflatten(layout, refs)
    r = types.SimpleNamespace(**scratch, **scratch["held"], **scratch["made"])
    loads = {
        name: pltpu.make_async_copy(given[name], r.held[name], r.load_sem.at[i]) for i, name in enumerate(given)
    }
    stores = {
        name: pltpu.make_async_copy(r.made[name], wanted[name], r.store_sem.at[i]) for i, name in enumerate(wanted)
    }

    def need(*names):
        for name in names:
            loads[name].wait()

    tokens, rows, width = r.tokens, r.tokens.shape[0], r.tokens.shape[1]
    local_width = r.k_weight.shape[0]
    heads = local_width // HD
    pair = 2 * HD
    hidden_width = r.in_weight.shape[1]
    spans = portions_of(rows)
    low, wide = jnp.bfloat16, jnp.float32
    at = Place()
    me = at.me
    dp = lax.axis_index("dp")
    core = lax.rem(dp, 2)
    across = dp + 1 - 2 * core

    barrier = pltpu.get_barrier_semaphore()
    near = lax.rem(dp // 2, 2)
    over_x = dp + 2 - 4 * near
    peers = [{"mp": lax.rem(me + step, LINE)} for step in range(1, LINE)] + [{"dp": across}, {"dp": over_x}]
    if planar:
        over_y = dp + 4 - 8 * (dp // 4)
        peers += [{"dp": over_y}]
    for peer in peers:
        pl.semaphore_signal(barrier, inc=1, device_id=peer, device_id_type=pl.DeviceIdType.MESH)

    first = ("k_weight", "tokens", "kind_row", "seg_row", "v_weight", "q_weight", "o_weight")
    for name in first + tuple(name for name in loads if name not in first):
        loads[name].start()

    wa, wb, wk = r.wa, r.wb, r.wk
    need("k_weight", "q_weight")
    for h in range(heads):
        cols = slice(h * HD, (h + 1) * HD)
        both = slice(h * pair, (h + 1) * pair)
        wa[both, :] = jnp.concatenate([r.q_weight[0, cols, :], r.q_weight[1, cols, :]], axis=0)
        wb[both, :] = jnp.concatenate([r.q_weight[2, cols, :], r.q_weight[3, cols, :]], axis=0)
        key_part = r.k_weight[cols, :]
        wk[both, :] = jnp.concatenate([key_part, key_part], axis=0)
    need("o_weight")
    pl.semaphore_wait(barrier, len(peers))

    ow, ow_send, ow_recv = r.ow, r.ow_send, r.ow_recv
    vec = r.vec
    o_bias, gain1, shift1, in_bias, out_bias, gain2, shift2 = (vec.at[i : i + 1] for i in range(7))
    share = local_width // 4
    quarter = pl.ds(pl.multiple_of((2 * core + near) * share, 16), share)
    pairs = pl.ds(pl.multiple_of(2 * core * share, 16), 2 * share)
    ow_line, ow_plane, ow_chip = [], [], []
    for step in range(1, LINE):
        source, i = lax.rem(me + LINE - step, LINE), step - 1
        ow_line.append(
            remote(
                r.o_weight.at[quarter], ow.at[me, quarter], ow_send.at[i], ow_recv.at[i], mp=lax.rem(me + step, LINE)
            )
        )
        held = ow.at[source, quarter]
        ow_plane.append(remote(held, held, ow_send.at[3 + i], ow_recv.at[3 + i], dp=over_x))
        held = ow.at[source, pairs]
        ow_chip.append(remote(held, held, ow_send.at[6 + i], ow_recv.at[6 + i], dp=across))
    for copy in ow_line:
        copy.start()

    need("kind_row", "seg_row")
    kind_wide, seg_wide = r.kind_wide, r.seg_wide
    kind_wide[...] = jnp.broadcast_to(r.kind_row[...], (pair, rows)).T
    seg_wide[...] = jnp.broadcast_to(r.seg_row[...], (pair, rows)).T
    qcat, kcat, vt = r.qcat, r.kcat, r.vt
    need("tokens", "v_weight")
    tok = tokens[...]
    entity = kind_wide[...] == 1
    upper = lax.broadcasted_iota(jnp.int32, (rows, pair), 1) >= HD
    keys = dot(tok, wk[...], 1, 1)
    for h in range(heads):
        both = slice(h * pair, (h + 1) * pair)
        kcat[:, both] = jnp.where(entity == upper, keys[:, both], 0.0).astype(low)
    vt[...] = dot(r.v_weight[...], tok, 1, 1).astype(low)
    q_plain = dot(tok, wa[...], 1, 1)
    q_entity = dot(tok, wb[...], 1, 1)
    for h in range(heads):
        both = slice(h * pair, (h + 1) * pair)
        qcat[:, both] = jnp.where(entity, q_entity[:, both], q_plain[:, both]).astype(low)

    pt, mx, mloc, st = r.pt, r.mx, r.mloc, r.st
    scale = HD ** (-0.5)
    gathers = [
        LineGather(at, r.mx_send.at[q], r.mx_recv.at[q], lambda block, q=q: mx[q].at[block])
        for q in range(len(spans))
    ]

    def pair_of(h):
        return pl.ds(pl.multiple_of(h * pair, pair), pair)

    def head_of(h):
        return pl.ds(pl.multiple_of(h * HD, HD), HD)

    def attend(q):
        start, size = spans[q]
        here = pl.ds(start, size)

        def head_step(h, carry):
            st[:, :size] = dot(kcat[:, pair_of(h)], qcat[here, pair_of(h)], 1, 1)

            def soften(i, carry):
                cols = pl.ds(pl.multiple_of(i * LANES, LANES), LANES)
                span = pl.ds(pl.multiple_of(start + i * LANES, LANES), LANES)
                scores = jnp.where(seg_wide[...] == r.seg_row[:, span], st[:, cols] * scale, -1000000000.0)
                shifted = jnp.exp(scores - jnp.max(scores, axis=0, keepdims=True))
                total = jnp.sum(shifted, axis=0, keepdims=True)
                pt[h, :, span] = (shifted * (1.0 / total)).astype(low)
                return carry

            lax.fori_loop(0, size // LANES, soften, 0)
            mixed = dot(vt[head_of(h), :], pt[h, :, here]).astype(low)
            mx[q][me, head_of(h), :] = mixed
            mloc[head_of(h), here] = mixed
            return carry

        lax.fori_loop(0, heads, head_step, 0)
        gathers[q].spread()

    def swap_plane():
        ow[me] = r.o_weight[...]
        for copy in ow_line:
            copy.wait_recv()
        for copy in ow_plane:
            copy.start()

    def swap_chip():
        for copy in ow_plane:
            copy.wait_recv()
        for copy in ow_chip:
            copy.start()

    def own_weights():
        for copy in ow_chip:
            copy.wait_recv()
        need("in_weight", "out_weight", "o_bias", "gain1", "shift1", "in_bias", "out_bias", "gain2", "shift2")
        for i, name in enumerate((r.o_bias, r.gain1, r.shift1, r.in_bias, r.out_bias, r.gain2, r.shift2)):
            vec[i, :] = name[...]

    tok_t, kct, vn = r.tok_t, r.kct, r.vn

    def turn():
        tok_t[...] = tokens[...].T
        kct[...] = kcat[...].T
        for h in range(heads):
            vn[h] = vt[h * HD : (h + 1) * HD, :].T

    xh1, rstd1, hl = r.xh1, r.rstd1, r.hl
    act, gp, dr2, gf, il, gb, tmp, acc = r.act, r.gp, r.dr2, r.gf, r.il, r.gb, r.tmp, r.acc
    acc[...] = jnp.zeros_like(acc)

    def make_lines(parts, part, out):
        return [
            LineReduce(at, part, *parts[q], start, size // LINE, out) for q, (start, size) in enumerate(spans)
        ]

    ffn = make_lines(r.ffn, r.ffn_part, r.ffn_out)
    back = make_lines(r.back, r.back_part, r.back_out)
    grad = make_lines(r.grad, r.grad_part, r.tokens_grad)

    root_half = math.sqrt(0.5)
    density = 1.0 / math.sqrt(2.0 * math.pi)

    def forward(q):
        gathers[q].arrive()
        start, size = spans[q]
        here = pl.ds(start, size)
        mixed = mx[q][...].reshape(LINE * local_width, size)
        tmp[:size, :] = dot(mixed, ow[...].reshape(LINE * local_width, width), 0, 0)

        def first_norm(at_rows, inside):
            value = tmp[inside, :] + tokens[at_rows, :].astype(wide) + o_bias[...]
            centred = value - row_mean(value)
            scaled = lax.rsqrt(row_mean(centred * centred) + norm_epsilon)
            normal = centred * scaled
            xh1[at_rows, :] = normal
            rstd1[at_rows, :] = jnp.broadcast_to(scaled, (CHUNK, 128))
            hl[at_rows, :] = (normal * gain1[...] + shift1[...]).astype(low)

        rows_loop(start, size, first_norm)
        tmp[:size, :] = dot(hl[here, :], r.in_weight[...])

        def activate(at_rows, inside):
            inner = tmp[inside, :] + in_bias[...]
            gate = 0.5 + 0.5 * lax.erf(inner * root_half)
            act[at_rows, :] = (inner * gate).astype(low)
            gp[at_rows, :] = gate + inner * (density * jnp.exp(-0.5 * inner * inner))

        rows_loop(start, size, activate)
        r.ffn_part[here, :] = dot(act[here, :], r.out_weight[...]).astype(low)
        ffn[q].start()

    def backward(q):
        ffn[q].arrive()
        start, size = spans[q]
        here = pl.ds(start, size)

        def second_norm(at_rows, inside):
            value = xh1[at_rows, :] * gain1[...] + shift1[...]
            value = value + r.ffn_out[at_rows, :].astype(wide) + out_bias[...]
            centred = value - row_mean(value)
            scaled = lax.rsqrt(row_mean(centred * centred) + norm_epsilon)
            normal = centred * scaled
            r.layer_out[at_rows, :] = (normal * gain2[...] + shift2[...]).astype(low)
            cot = r.cotangent[at_rows, :].astype(wide)
            acc[6] += fold(cot)
            acc[5] += fold(cot * normal)
            grown = cot * gain2[...]
            grad_in = scaled * (grown - row_mean(grown) - normal * row_mean(grown * normal))
            acc[4] += fold(grad_in)
            dr2[at_rows, :] = grad_in
            gf[at_rows, :] = grad_in.astype(low)

        rows_loop(start, size, second_norm)
        tmp[:size, :] = dot(gf[here, :], r.out_weight[...], 1, 1)

        def inner_step(at_rows, inside):
            d_inner = tmp[inside, :] * gp[at_rows, :]
            acc[3] += fold(d_inner)
            il[at_rows, :] = d_inner.astype(low)

        rows_loop(start, size, inner_step)
        r.back_part[here, :] = dot(il[here, :], r.in_weight[...], 1, 1).astype(low)
        back[q].start()

    dqa, dqb, dkv, dk_sum, dv_sum = r.dqa, r.dqb, r.dkv, r.dk_sum, r.dv_sum
    dmt, ds = r.dmt, r.ds

    def finish_rows(q):
        back[q].arrive()
        start, size = spans[q]
        here = pl.ds(start, size)

        def last_norm(at_rows, inside):
            d_hidden = dr2[at_rows, :] + r.back_out[at_rows, :].astype(wide)
            normal = xh1[at_rows, :]
            acc[2] += fold(d_hidden)
            acc[1] += fold(d_hidden * normal)
            grown = d_hidden * gain1[...]
            grad_in = rstd1[at_rows, 0:1] * (grown - row_mean(grown) - normal * row_mean(grown * normal))
            acc[0] += fold(grad_in)
            dr2[at_rows, :] = grad_in
            gb[at_rows, :] = grad_in.astype(low)

        rows_loop(start, size, last_norm)
        dmt[:, here] = dot(r.o_weight[...], gb[here, :], 1, 1).astype(low)

        def head_step(h, carry):
            d_mixed = dmt[head_of(h), here]
            st[:, :size] = dot(vn[h], d_mixed)

            def harden(i, carry):
                cols = pl.ds(pl.multiple_of(i * LANES, LANES), LANES)
                span = pl.ds(pl.multiple_of(start + i * LANES, LANES), LANES)
                prob = pt[h, :, span].astype(wide)
                d_prob = st[:, cols]
                delta = jnp.sum(prob * d_prob, axis=0, keepdims=True)
                ds[:, cols] = (prob * (d_prob - delta) * scale).astype(low)
                return carry

            lax.fori_loop(0, size // LANES, harden, 0)
            d_score = ds[:, :size]
            d_value = dot(pt[h, :, here], d_mixed, 1, 1)
            d_key = dot(d_score, qcat[here, pair_of(h)])
            if q == 0:
                dv_sum[h] = d_value
                dk_sum[h] = d_key
            else:
                dv_sum[h] += d_value
                dk_sum[h] += d_key
            d_query = dot(kct[pair_of(h), :], d_score).T
            row_entity = kind_wide[here, :] == 1
            dqa[here, pair_of(h)] = jnp.where(row_entity, 0.0, d_query).astype(low)
            dqb[here, pair_of(h)] = jnp.where(row_entity, d_query, 0.0).astype(low)
            return carry

        lax.fori_loop(0, heads, head_step, 0)

    gfeed, gattn = r.gfeed, r.gattn
    blocks, per_block = gfeed.shape[0], gfeed.shape[1]

    def put_grad(packed, start, value):
        packed[:, :, start : start + value.shape[1]] = value.astype(low).reshape(blocks, per_block, value.shape[1])

    if planar:
        feed = PlaneReduce(gfeed, *r.feed)
        attn = PlaneReduce(gattn, *r.attn)

    small = r.small
    if planar:
        small_sum = r.small_sum
        tiny = [
            remote(
                small if s == 0 else small_sum.at[s - 1],
                r.small_in.at[s],
                r.small_send.at[s],
                r.small_recv.at[s],
                dp=(across, over_x, over_y)[s],
            )
            for s in range(3)
        ]

    def tiny_step(s):
        if planar:
            tiny[s].wait_recv()
            small_sum[s] = (small if s == 0 else small_sum.at[s - 1])[...] + r.small_in[s]
            if s < 2:
                tiny[s + 1].start()

    def feed_step(i):
        if i == 0:
            put_grad(gfeed, hidden_width, dot(gf[...], act[...], 0, 0))
        elif i == 1:
            put_grad(gfeed, 0, dot(hl[...], il[...], 0, 0))
        elif planar and i == 2:
            feed.start()
        elif planar and i == 3:
            feed.step_one()
        elif planar and i == 4:
            feed.step_two()
        elif planar and i == 5:
            feed_sum = feed.finish()
            r.in_grad[...] = feed_sum[:, :hidden_width]
            r.out_grad[...] = feed_sum[:, hidden_width:]
            stores["in_grad"].start()
            stores["out_grad"].start()

    def key_grads():
        for i in range(8):
            small[i : i + 1, :] = jnp.sum(acc[i], axis=0, keepdims=True)
        if planar:
            tiny[0].start()
        d_keys = [
            jnp.where(kind_wide[:, :HD] == 1, dk_sum[h, :, HD:], dk_sum[h, :, :HD]).astype(low)
            for h in range(heads)
        ]
        d_values = [dv_sum[h].astype(low) for h in range(heads)]
        dkv[...] = jnp.concatenate(d_keys + d_values, axis=1)

    def input_share(q):
        start, size = spans[q]
        here = pl.ds(start, size)
        share = dot(dqa[here, :], wa[...]) + dot(dqb[here, :], wb[...])
        share = share + dot(dkv[here, :local_width], r.k_weight[...]) + dot(dkv[here, local_width:], r.v_weight[...])
        r.grad_part[here, :] = share.astype(low)
        grad[q].start()

    def attn_step(i):
        if i == 0:
            put_grad(gattn, 0, dot(tok_t[...], dqa[...]))
            put_grad(gattn, 2 * local_width, dot(tok_t[...], dqb[...]))
        elif i == 1:
            put_grad(gattn, 4 * local_width, dot(tok_t[...], dkv[...]))
            o_grad = dot(gb[...], mloc[...], 0, 1)
            pad = gattn.shape[2] - 7 * local_width
            put_grad(gattn, 6 * local_width, jnp.concatenate([o_grad, jnp.zeros((width, pad), wide)], axis=1))
        elif planar and i == 2:
            attn.start()
            tiny_step(0)
        elif planar and i == 3:
            attn.step_one()
            tiny_step(1)
        elif planar and i == 4:
            attn.step_two()
            tiny_step(2)

    attend(0)
    attend(1)
    gathers[0].relay(0)
    gathers[0].relay(1)
    swap_plane()
    attend(2)
    gathers[1].relay(0)
    gathers[0].relay(2)
    attend(3)
    gathers[3].relay(0)
    gathers[1].relay(1)
    gathers[1].relay(2)
    attend(4)
    gathers[4].relay(0)
    swap_chip()
    gathers[3].relay(1)
    gathers[3].relay(2)
    gathers[2].relay(0)
    gathers[4].relay(1)
    gathers[4].relay(2)
    gathers[2].relay(1)
    own_weights()
    forward(0)
    ffn[0].forward(0)
    ffn[0].forward(1)
    gathers[2].relay(2)
    forward(1)
    ffn[1].forward(0)
    forward(3)
    ffn[3].forward(0)
    ffn[1].forward(1)
    forward(4)
    ffn[0].settle()
    ffn[3].forward(1)
    ffn[4].forward(0)
    forward(2)
    ffn[0].relay(0)
    ffn[1].settle()
    ffn[2].forward(0)
    ffn[2].forward(1)
    ffn[0].relay(1)
    ffn[0].relay(2)
    ffn[1].relay(0)
    ffn[3].settle()
    ffn[1].relay(1)
    ffn[4].forward(1)
    ffn[3].relay(0)
    ffn[1].relay(2)
    ffn[2].settle()
    ffn[2].relay(0)
    ffn[3].relay(1)
    ffn[3].relay(2)
    ffn[4].settle()
    ffn[4].relay(0)
    ffn[2].relay(1)
    need("cotangent")
    backward(0)
    back[0].forward(0)
    ffn[2].relay(2)
    back[0].forward(1)
    backward(1)
    ffn[4].relay(1)
    back[1].forward(0)
    backward(3)
    back[1].forward(1)
    ffn[4].relay(2)
    back[3].forward(0)
    back[0].settle()
    backward(2)
    back[0].relay(0)
    back[3].forward(1)
    back[1].settle()
    back[2].forward(0)
    back[2].forward(1)
    back[0].relay(1)
    backward(4)
    stores["layer_out"].start()
    back[1].relay(0)
    back[3].settle()
    feed_step(0)
    back[4].forward(0)
    back[1].relay(1)
    back[4].forward(1)
    back[0].relay(2)
    back[2].settle()
    turn()
    back[1].relay(2)
    back[3].relay(0)
    back[2].relay(0)
    back[4].settle()
    back[2].relay(1)
    feed_step(1)
    back[2].relay(2)
    back[3].relay(1)
    back[3].relay(2)
    feed_step(2)
    back[4].relay(0)
    finish_rows(0)
    back[4].relay(1)
    finish_rows(1)
    back[4].relay(2)
    finish_rows(2)
    finish_rows(3)
    finish_rows(4)
    key_grads()
    input_share(0)
    input_share(1)
    input_share(2)
    input_share(3)
    grad[0].forward(0)
    feed_step(3)
    grad[0].forward(1)
    input_share(4)
    attn_step(0)
    grad[1].forward(0)
    grad[1].forward(1)
    attn_step(1)
    grad[2].forward(0)
    grad[2].forward(1)
    grad[0].settle(dr2)
    attn_step(2)
    grad[3].forward(0)
    grad[3].forward(1)
    grad[2].settle(dr2)
    grad[4].forward(0)
    attn_step(3)
    grad[4].forward(1)
    grad[1].settle(dr2)
    feed_step(4)
    grad[3].settle(dr2)
    grad[0].relay(0)
    grad[0].relay(1)
    grad[4].settle(dr2)
    grad[2].relay(0)
    grad[1].relay(0)
    grad[2].relay(1)
    grad[1].relay(1)
    grad[3].relay(0)
    grad[4].relay(0)
    grad[0].relay(2)
    grad[3].relay(1)
    grad[2].relay(2)
    attn_step(4)
    grad[4].relay(1)
    grad[1].relay(2)
    grad[3].relay(2)
    grad[4].relay(2)
    feed_step(5)
    if planar:
        attn_sum = attn.finish()
        for part in range(4):
            base = (part // 2) * 2 * local_width + (part % 2) * HD
            r.q_grad[part] = jnp.concatenate(
                [attn_sum[:, base + h * pair : base + h * pair + HD] for h in range(heads)], axis=1
            )
        both_grads = attn_sum[:, 4 * local_width : 6 * local_width]
        r.k_grad[...] = both_grads[:, :local_width]
        r.v_grad[...] = both_grads[:, local_width:]
        r.o_grad[...] = attn_sum[:, 6 * local_width : 7 * local_width].T
        r.small_out[...] = small_sum[2]
        for name in ("q_grad", "k_grad", "v_grad", "o_grad", "small_out"):
            stores[name].start()
    else:
        r.small_out[...] = small[...]
        r.feed_out[...] = gfeed[...]
        r.attn_out[...] = gattn[...]
        for name in ("small_out", "feed_out", "attn_out"):
            stores[name].start()
    for line in grad:
        line.arrive()
    stores["tokens_grad"].start()
    for line in ffn + back + grad:
        line.drain()
    for gather in gathers:
        gather.drain()
    for copy in ow_line + ow_plane + ow_chip:
        copy.wait_send()
    if planar:
        for copy in tiny:
            copy.wait_send()
    for copy in stores.values():
        copy.wait()


def hand_on(layout, *refs):
    sources, targets, held, lines, sems = jax.tree.unflatten(layout, refs)
    count = len(sources) - 1
    small = held[0]
    fetch = [pltpu.make_async_copy(source, kept, sems.at[0, i]) for i, (source, kept) in enumerate(zip(sources, held))]
    store = [
        pltpu.make_async_copy(kept, target, sems.at[1, i])
        for i, (kept, target) in enumerate(zip(list(held[1:]) + list(lines), targets))
    ]
    for copy in fetch:
        copy.start()
    fetch[0].wait()
    for i, line in enumerate(lines):
        line[...] = small[i, :]
        store[count + i].start()
    for i in range(count):
        fetch[1 + i].wait()
        store[i].start()
    for copy in store:
        copy.wait()


def local(
    tokens,
    segment_ids,
    token_types,
    q_weight,
    k_weight,
    v_weight,
    o_weight,
    o_bias,
    norm1_gain,
    norm1_shift,
    in_weight,
    in_bias,
    out_weight,
    out_bias,
    norm2_gain,
    norm2_shift,
    cotangent,
):
    rows, width = tokens.shape
    local_width = k_weight.shape[1]
    heads = local_width // HD
    hidden_width = in_weight.shape[1]
    n_dp = lax.axis_size("dp")
    planar = n_dp == 8
    blocks = 8
    per_block = width // blocks
    spans = portions_of(rows)
    largest = max(size for _, size in spans)
    low, wide = jnp.bfloat16, jnp.float32
    attn_width = -(-7 * local_width // 128) * 128
    args = dict(
        tokens=tokens,
        seg_row=segment_ids,
        kind_row=token_types,
        q_weight=q_weight.swapaxes(1, 2),
        k_weight=k_weight.T,
        v_weight=v_weight.T,
        o_weight=o_weight,
        o_bias=o_bias,
        gain1=norm1_gain,
        shift1=norm1_shift,
        in_bias=in_bias,
        out_bias=out_bias,
        gain2=norm2_gain,
        shift2=norm2_shift,
        in_weight=in_weight,
        out_weight=out_weight,
        cotangent=cotangent,
    )
    shaped = jax.ShapeDtypeStruct
    outs = dict(
        layer_out=shaped((rows, width), low),
        tokens_grad=shaped((rows, width), low),
        small_out=shaped((8, width), wide),
    )
    if planar:
        outs |= dict(
            q_grad=shaped((4, per_block, local_width), wide),
            k_grad=shaped((per_block, local_width), wide),
            v_grad=shaped((per_block, local_width), wide),
            o_grad=shaped((local_width, per_block), wide),
            in_grad=shaped((per_block, hidden_width), wide),
            out_grad=shaped((per_block, hidden_width), wide),
        )
    else:
        outs |= dict(
            feed_out=shaped((blocks, per_block, 2 * hidden_width), low),
            attn_out=shaped((blocks, per_block, attn_width), low),
        )
    dma = pltpu.SemaphoreType.DMA
    scratch = dict(
        ow=pltpu.VMEM((LINE, local_width, width), low),
        ow_send=dma((9,)),
        ow_recv=dma((9,)),
        wa=pltpu.VMEM((2 * local_width, width), low),
        wb=pltpu.VMEM((2 * local_width, width), low),
        wk=pltpu.VMEM((2 * local_width, width), low),
        kind_wide=pltpu.VMEM((rows, 2 * HD), jnp.int32),
        seg_wide=pltpu.VMEM((rows, 2 * HD), jnp.int32),
        qcat=pltpu.VMEM((rows, 2 * local_width), low),
        kcat=pltpu.VMEM((rows, 2 * local_width), low),
        vt=pltpu.VMEM((local_width, rows), low),
        pt=pltpu.VMEM((heads, rows, rows), low),
        mx=[pltpu.VMEM((LINE, local_width, size), low) for _, size in spans],
        st=pltpu.VMEM((rows, largest), wide),
        ds=pltpu.VMEM((rows, largest), low),
        mloc=pltpu.VMEM((local_width, rows), low),
        mx_send=dma((len(spans), 5)),
        mx_recv=dma((len(spans), LINE)),
        tok_t=pltpu.VMEM((width, rows), low),
        xh1=pltpu.VMEM((rows, width), wide),
        rstd1=pltpu.VMEM((rows, 128), wide),
        hl=pltpu.VMEM((rows, width), low),
        act=pltpu.VMEM((rows, hidden_width), low),
        gp=pltpu.VMEM((rows, hidden_width), wide),
        dr2=pltpu.VMEM((rows, width), wide),
        gf=pltpu.VMEM((rows, width), low),
        il=pltpu.VMEM((rows, hidden_width), low),
        tmp=pltpu.VMEM((largest, width), wide),
        vec=pltpu.VMEM((8, width), wide),
        acc=pltpu.VMEM((8, 8, width), wide),
        gb=pltpu.VMEM((rows, width), low),
        ffn_part=pltpu.VMEM((rows, width), low),
        back_part=pltpu.VMEM((rows, width), low),
        grad_part=pltpu.VMEM((rows, width), low),
        ffn_out=pltpu.VMEM((rows, width), low),
        back_out=pltpu.VMEM((rows, width), low),
        gfeed=pltpu.VMEM((blocks, per_block, 2 * hidden_width), low),
        gattn=pltpu.VMEM((blocks, per_block, attn_width), low),
        small=pltpu.VMEM((8, width), wide),
        kct=pltpu.VMEM((2 * local_width, rows), low),
        vn=pltpu.VMEM((heads, rows, HD), low),
        dmt=pltpu.VMEM((local_width, rows), low),
        dk_sum=pltpu.VMEM((heads, rows, 2 * HD), wide),
        dv_sum=pltpu.VMEM((heads, rows, HD), wide),
        dqa=pltpu.VMEM((rows, 2 * local_width), low),
        dqb=pltpu.VMEM((rows, 2 * local_width), low),
        dkv=pltpu.VMEM((rows, 2 * local_width), low),
    )
    for name in ("ffn", "back", "grad"):
        scratch[name] = [line_scratch(size // LINE, width) for _, size in spans]
    if planar:
        scratch |= dict(
            feed=plane_scratch(per_block, 2 * hidden_width),
            attn=plane_scratch(per_block, attn_width),
            small_in=pltpu.VMEM((3, 8, width), wide),
            small_sum=pltpu.VMEM((3, 8, width), wide),
            small_send=dma((3,)),
            small_recv=dma((3,)),
        )
    scratch |= dict(
        held={name: pltpu.VMEM(a.shape, a.dtype) for name, a in args.items()},
        made={name: pltpu.VMEM(a.shape, a.dtype) for name, a in outs.items()},
        load_sem=dma((len(args),)),
        store_sem=dma((len(outs),)),
    )
    layout = jax.tree.structure((args, outs, scratch))
    vm, far = pl.BlockSpec(memory_space=pltpu.VMEM), pl.BlockSpec(memory_space=pl.ANY)
    results = pl.pallas_call(
        functools.partial(layer_kernel, planar, layout),
        out_shape=jax.tree.leaves(outs),
        in_specs=[far] * len(args),
        out_specs=[far] * len(outs),
        scratch_shapes=jax.tree.leaves(scratch),
        compiler_params=pltpu.CompilerParams(
            collective_id=0, has_side_effects=True, vmem_limit_bytes=VMEM_LIMIT
        ),
    )(*jax.tree.leaves(args))
    results = dict(zip(sorted(outs), results))
    if planar:
        small = results.pop("small_out")
        flat, tree = jax.tree.flatten(results)
        vectors = small.shape[0] - 1
        line = (width,)
        targets = [shaped(a.shape, a.dtype) for a in flat] + [shaped(line, wide)] * vectors
        held = [pltpu.VMEM(a.shape, a.dtype) for a in [small] + flat]
        lines = [pltpu.VMEM(line, wide)] * vectors
        sems = dma((2, len(targets)))
        pieces = ([small] + flat, targets, held, lines, sems)
        flat = pl.pallas_call(
            functools.partial(hand_on, jax.tree.structure(pieces)),
            out_shape=targets,
            in_specs=[far] * (1 + len(flat)),
            out_specs=[far] * len(targets),
            scratch_shapes=held + lines + [sems],
            compiler_params=pltpu.CompilerParams(vmem_limit_bytes=VMEM_LIMIT),
        )(small, *flat)
        small = flat[len(results) :]
        results = jax.tree.unflatten(tree, flat[: len(results)])
    res = types.SimpleNamespace(**results)
    if planar:
        grads = (res.q_grad, res.k_grad, res.v_grad, res.o_grad, res.in_grad, res.out_grad.T)
    else:
        feed = res.feed_out.astype(wide).reshape(width, 2 * hidden_width)
        attn = res.attn_out.astype(wide).reshape(width, attn_width)
        feed = lax.psum_scatter(feed, "dp", scatter_dimension=0, tiled=True)
        attn = lax.psum_scatter(attn, "dp", scatter_dimension=0, tiled=True)
        small = lax.psum(res.small_out, "dp")
        per = feed.shape[0]
        queries = attn[:, : 4 * local_width].reshape(per, 2, heads, 2, HD)
        queries = queries.transpose(1, 3, 0, 2, 4).reshape(4, per, local_width)
        grads = (
            queries,
            attn[:, 4 * local_width : 5 * local_width],
            attn[:, 5 * local_width : 6 * local_width],
            attn[:, 6 * local_width : 7 * local_width].T,
            feed[:, :hidden_width],
            feed[:, hidden_width:].T,
        )
    d_q, d_k, d_v, d_o, d_in, d_out = grads
    return (
        res.layer_out,
        res.tokens_grad,
        d_q,
        d_k,
        d_v,
        d_o,
        small[0],
        small[1],
        small[2],
        d_in,
        small[3],
        d_out,
        small[4],
        small[5],
        small[6],
    )


def solution(mesh):
    return jax.shard_map(
        local,
        mesh=mesh,
        in_specs=(
            P("dp", None),
            P("dp", None),
            P("dp", None),
            P(None, None, "mp"),
            P(None, "mp"),
            P(None, "mp"),
            P("mp", None),
            P(),
            P(),
            P(),
            P(None, "mp"),
            P("mp"),
            P("mp", None),
            P(),
            P(),
            P(),
            P("dp", None),
        ),
        out_specs=(
            P("dp", None),
            P("dp", None),
            P(None, "dp", "mp"),
            P("dp", "mp"),
            P("dp", "mp"),
            P("mp", "dp"),
            P(),
            P(),
            P(),
            P("dp", "mp"),
            P("mp"),
            P("mp", "dp"),
            P(),
            P(),
            P(),
        ),
        check_vma=False,
    )
```

```python
import functools
import math
import operator
import types

import jax
import jax.numpy as jnp
from jax import lax
from jax.experimental import pallas as pl
from jax.experimental.pallas import tpu as pltpu
from jax.sharding import PartitionSpec as P

HD = 64
LINE = 4
PORTIONS = (1, 1, 1, 1, 1)
LANES = 128
CHUNK = 32
VMEM_LIMIT = 67043328

norm_epsilon = 1e-05


def remote(src, dst, send_sem, recv_sem, **axes):
    return pltpu.make_async_remote_copy(
        src_ref=src,
        dst_ref=dst,
        send_sem=send_sem,
        recv_sem=recv_sem,
        device_id=axes,
        device_id_type=pl.DeviceIdType.MESH,
    )


class Place:
    def __init__(self):
        me = lax.axis_index("mp")
        self.me = me
        self.is_mid = jnp.logical_or(me == 1, me == 2)
        self.is_end = jnp.logical_not(self.is_mid)
        left = me < 2
        self.mid = jnp.where(left, 1, 2)
        self.end = jnp.where(left, 0, 3)
        self.far_mid = 3 - self.mid
        self.far_end = 3 - self.end


class LineGather:
    def __init__(self, place, send, recv, out):
        self.at, self.send, self.recv, self.out = place, send, recv, out

    def copy(self, block, slot, target):
        return remote(self.out(block), self.out(block), self.send, self.recv.at[block], mp=target)

    def spread(self):
        at = self.at

        @pl.when(at.is_end)
        def _():
            self.copy(at.me, 0, at.mid).start()

        @pl.when(at.is_mid)
        def _():
            self.copy(at.me, 0, at.end).start()
            self.copy(at.me, 1, at.far_mid).start()

    def relay(self, step):
        at = self.at
        block = (at.end, at.far_mid, at.far_end)[step]
        target = (at.far_mid, at.end, at.end)[step]

        @pl.when(at.is_mid)
        def _():
            self.copy(block, 2 + step, target).wait_recv()
            self.copy(block, 2 + step, target).start()

    def arrive(self):
        at = self.at

        @pl.when(at.is_end)
        def _():
            self.copy(at.mid, 0, at.mid).wait_recv()
            self.copy(at.far_mid, 0, at.mid).wait_recv()
            self.copy(at.far_end, 0, at.mid).wait_recv()


class LineReduce:
    def __init__(self, place, part, carry, single, summed, send, recv, start, block_rows, out):
        self.at, self.carry, self.single, self.summed = place, carry, single, summed
        self.send, self.recv = send, recv

        def rows_of(block):
            return pl.ds(pl.multiple_of(start + block * block_rows, 16), block_rows)

        self.rows_of, self.part_ref, self.out_ref = rows_of, part, out
        self.gather = LineGather(place, send, recv.at[1], lambda block: out.at[rows_of(block)])

    def part(self, block):
        return self.part_ref.at[self.rows_of(block)]

    def end_sends(self):
        at, send, recv = self.at, self.send, self.recv
        return (
            remote(self.part(at.far_end), self.carry.at[0], send, recv.at[0, 2], mp=at.mid),
            remote(self.part(at.far_mid), self.carry.at[1], send, recv.at[0, 3], mp=at.mid),
            remote(self.part(at.mid), self.single, send, recv.at[0, 0], mp=at.mid),
        )

    def mid_sends(self):
        at, send, recv = self.at, self.send, self.recv
        return (
            remote(self.carry.at[0], self.summed, send, recv.at[0, 1], mp=at.far_end),
            remote(self.carry.at[1], self.summed, send, recv.at[0, 1], mp=at.far_mid),
            remote(self.part(at.end), self.single, send, recv.at[0, 0], mp=at.end),
        )

    def start(self):
        @pl.when(self.at.is_end)
        def _():
            for copy in self.end_sends():
                copy.start()

        @pl.when(self.at.is_mid)
        def _():
            self.mid_sends()[2].start()

    def forward(self, step):
        at = self.at

        @pl.when(at.is_mid)
        def _():
            block = (at.far_end, at.far_mid)[step]
            self.end_sends()[step].wait_recv()
            total = self.carry[step].astype(jnp.float32) + self.part(block)[...].astype(jnp.float32)
            self.carry[step] = total.astype(jnp.bfloat16)
            self.mid_sends()[step].start()

    def total(self):
        self.end_sends()[2].wait_recv()
        self.mid_sends()[0].wait_recv()
        return (
            self.part(self.at.me)[...].astype(jnp.float32)
            + self.single[...].astype(jnp.float32)
            + self.summed[...].astype(jnp.float32)
        )

    def settle(self, extra=None):
        at = self.at
        total = self.total()
        if extra is not None:
            total = total + extra[self.rows_of(at.me), :]
        self.out_ref[self.rows_of(at.me), :] = total.astype(jnp.bfloat16)
        self.gather.spread()

    def relay(self, step):
        self.gather.relay(step)

    def arrive(self):
        self.gather.arrive()


class LineSwap:
    def __init__(self, place, sent, got, send, recv):
        me = place.me
        self.me, self.sent, self.got = me, sent, got
        targets = [lax.rem(me + step, LINE) for step in range(1, LINE)]
        self.outward = [
            remote(sent.at[j], got.at[me], send.at[i], recv.at[me], mp=j) for i, j in enumerate(targets)
        ]
        self.inward = [remote(got.at[j], got.at[j], send.at[i], recv.at[j], mp=j) for i, j in enumerate(targets)]

    def start(self):
        for copy in self.outward:
            copy.start()
        self.got[self.me] = self.sent[self.me]

    def wait(self):
        for copy in self.inward:
            copy.wait_recv()

    def drain(self):
        for copy in self.outward:
            copy.wait_send()


def swap_scratch(rows, width, kind):
    return [
        pltpu.VMEM((LINE, rows, width), kind),
        pltpu.VMEM((LINE, rows, width), kind),
        pltpu.SemaphoreType.DMA((LINE - 1,)),
        pltpu.SemaphoreType.DMA((LINE,)),
    ]


def line_scratch(rows, width):
    return [
        pltpu.VMEM((2, rows, width), jnp.bfloat16),
        pltpu.VMEM((rows, width), jnp.bfloat16),
        pltpu.VMEM((rows, width), jnp.bfloat16),
        pltpu.SemaphoreType.DMA((2, 4)),
    ]


class PlaneReduce:
    def __init__(self, grads, r1, sums, mid2, r2a, r2b, s3a, s3b, r3a, r3b, send, recv):
        self.grads, self.r1, self.sums, self.mid2 = grads, r1, sums, mid2
        self.r2a, self.r2b, self.s3a, self.s3b, self.r3a, self.r3b = r2a, r2b, s3a, s3b, r3a, r3b
        dp = lax.axis_index("dp")
        self.core, self.x, self.y = lax.rem(dp, 2), lax.rem(dp // 2, 2), dp // 4
        across = dp + 1 - 2 * self.core
        over_x = dp + 2 - 4 * self.x
        over_y = dp + 4 - 8 * self.y
        half = r2a.shape[2]
        self.low, self.high = pl.ds(0, half), pl.ds(half, grads.shape[2] - half)
        self.first = [
            remote(grads.at[2 * k + 1 - self.core], r1.at[k], send.at[k], recv.at[k], dp=across) for k in range(4)
        ]
        self.second = [
            remote(mid2.at[2 * j + 1 - self.x, :, self.low], r2a.at[j], send.at[4 + j], recv.at[4 + j], dp=over_x)
            for j in range(2)
        ] + [
            remote(mid2.at[2 * (1 - self.y) + j, :, self.high], r2b.at[j], send.at[6 + j], recv.at[6 + j], dp=over_y)
            for j in range(2)
        ]
        self.third = [
            remote(s3a, r3a, send.at[8], recv.at[8], dp=over_y),
            remote(s3b, r3b, send.at[9], recv.at[9], dp=over_x),
        ]

    def start(self):
        for copy in self.first:
            copy.start()

    def step_one(self):
        for copy in self.first:
            copy.wait_recv()

        def body(k, carry):
            total = self.grads[2 * k + self.core].astype(jnp.float32) + self.r1[k].astype(jnp.float32)
            self.sums[k] = total
            self.mid2[k] = total.astype(jnp.bfloat16)
            return carry

        lax.fori_loop(0, 4, body, 0)
        for copy in self.second:
            copy.start()

    def step_two(self):
        for copy in self.second:
            copy.wait_recv()
        x, y = self.x, self.y
        self.s3a[...] = (
            self.sums[2 * (1 - y) + x, :, self.low] + self.r2a[1 - y].astype(jnp.float32)
        ).astype(jnp.bfloat16)
        self.third[0].start()
        self.s3b[...] = (
            self.sums[2 * y + 1 - x, :, self.high] + self.r2b[1 - x].astype(jnp.float32)
        ).astype(jnp.bfloat16)
        self.third[1].start()

    def finish(self):
        x, y = self.x, self.y
        for copy in self.third:
            copy.wait_recv()
        own = self.sums.at[2 * y + x]
        own[:, self.low] = own[:, self.low] + self.r2a[y].astype(jnp.float32) + self.r3a[...].astype(jnp.float32)
        own[:, self.high] = own[:, self.high] + self.r2b[x].astype(jnp.float32) + self.r3b[...].astype(jnp.float32)
        for copy in self.first + self.second + self.third:
            copy.wait_send()
        return own


def plane_scratch(rows, width):
    half = (width // 128 + 1) // 2 * 128
    rest = width - half
    low = jnp.bfloat16
    return [
        pltpu.VMEM((4, rows, width), low),
        pltpu.VMEM((4, rows, width), jnp.float32),
        pltpu.VMEM((4, rows, width), low),
        pltpu.VMEM((2, rows, half), low),
        pltpu.VMEM((2, rows, rest), low),
        pltpu.VMEM((rows, half), low),
        pltpu.VMEM((rows, rest), low),
        pltpu.VMEM((rows, half), low),
        pltpu.VMEM((rows, rest), low),
        pltpu.SemaphoreType.DMA((10,)),
        pltpu.SemaphoreType.DMA((10,)),
    ]


def dot(left, right, left_dim=1, right_dim=0):
    return lax.dot_general(
        left, right, (((left_dim,), (right_dim,)), ((), ())), preferred_element_type=jnp.float32
    )


def rows_loop(start, count, body):
    def step(i, carry):
        inside = pl.ds(pl.multiple_of(i * CHUNK, CHUNK), CHUNK)
        body(pl.ds(pl.multiple_of(start + i * CHUNK, CHUNK), CHUNK), inside)
        return carry

    lax.fori_loop(0, count // CHUNK, step, 0)


def fold(value):
    return jnp.sum(value.reshape(value.shape[0] // 8, 8, value.shape[1]), axis=0)


def row_mean(value):
    return jnp.mean(value, axis=-1, keepdims=True)


def portions_of(rows):
    unit = rows // sum(PORTIONS)
    return [(unit * sum(PORTIONS[:i]), unit * size) for i, size in enumerate(PORTIONS)]


def layer_kernel(planar, layout, *refs):
    given, wanted, scratch = jax.tree.unflatten(layout, refs)
    r = types.SimpleNamespace(**scratch, **scratch["held"], **scratch["made"])
    loads = {
        name: pltpu.make_async_copy(given[name], r.held[name], r.load_sem.at[i]) for i, name in enumerate(given)
    }
    stores = {
        name: pltpu.make_async_copy(r.made[name], wanted[name], r.store_sem.at[i]) for i, name in enumerate(wanted)
    }

    def need(*names):
        for name in names:
            loads[name].wait()

    tokens, rows, width = r.tokens, r.tokens.shape[0], r.tokens.shape[1]
    local_width = r.k_weight.shape[0]
    heads = local_width // HD
    pair = 2 * HD
    hidden_width = r.in_weight.shape[1]
    spans = portions_of(rows)
    low, wide = jnp.bfloat16, jnp.float32
    at = Place()
    me = at.me
    dp = lax.axis_index("dp")
    core = lax.rem(dp, 2)
    across = dp + 1 - 2 * core

    barrier = pltpu.get_barrier_semaphore()
    near = lax.rem(dp // 2, 2)
    over_x = dp + 2 - 4 * near
    peers = [{"mp": lax.rem(me + step, LINE)} for step in range(1, LINE)] + [{"dp": across}, {"dp": over_x}]
    if planar:
        over_y = dp + 4 - 8 * (dp // 4)
        peers += [{"dp": over_y}]
    for peer in peers:
        pl.semaphore_signal(barrier, inc=1, device_id=peer, device_id_type=pl.DeviceIdType.MESH)

    first = ("k_weight", "tokens", "kind_row", "seg_row", "v_weight", "q_weight", "o_weight")
    for name in first + tuple(name for name in loads if name not in first):
        loads[name].start()

    wa, wb, wk = r.wa, r.wb, r.wk
    need("k_weight", "q_weight")
    for h in range(heads):
        cols = slice(h * HD, (h + 1) * HD)
        both = slice(h * pair, (h + 1) * pair)
        wa[both, :] = jnp.concatenate([r.q_weight[0, cols, :], r.q_weight[1, cols, :]], axis=0)
        wb[both, :] = jnp.concatenate([r.q_weight[2, cols, :], r.q_weight[3, cols, :]], axis=0)
        key_part = r.k_weight[cols, :]
        wk[both, :] = jnp.concatenate([key_part, key_part], axis=0)
    need("o_weight")
    pl.semaphore_wait(barrier, len(peers))

    ow, ow_send, ow_recv = r.ow, r.ow_send, r.ow_recv
    vec = r.vec
    o_bias, gain1, shift1, in_bias, out_bias, gain2, shift2 = (vec.at[i : i + 1] for i in range(7))
    share = local_width // 4
    quarter = pl.ds(pl.multiple_of((2 * core + near) * share, 16), share)
    pairs = pl.ds(pl.multiple_of(2 * core * share, 16), 2 * share)
    ow_line, ow_plane, ow_chip = [], [], []
    for step in range(1, LINE):
        source, i = lax.rem(me + LINE - step, LINE), step - 1
        ow_line.append(
            remote(
                r.o_weight.at[quarter], ow.at[me, quarter], ow_send.at[i], ow_recv.at[i], mp=lax.rem(me + step, LINE)
            )
        )
        held = ow.at[source, quarter]
        ow_plane.append(remote(held, held, ow_send.at[3 + i], ow_recv.at[3 + i], dp=over_x))
        held = ow.at[source, pairs]
        ow_chip.append(remote(held, held, ow_send.at[6 + i], ow_recv.at[6 + i], dp=across))
    for copy in ow_line:
        copy.start()

    need("kind_row", "seg_row")
    kind_wide, seg_wide = r.kind_wide, r.seg_wide
    kind_wide[...] = jnp.broadcast_to(r.kind_row[...], (pair, rows)).T
    seg_wide[...] = jnp.broadcast_to(r.seg_row[...], (pair, rows)).T
    qcat, kcat, vt = r.qcat, r.kcat, r.vt
    need("tokens", "v_weight")
    tok = tokens[...]
    entity = kind_wide[...] == 1
    upper = lax.broadcasted_iota(jnp.int32, (rows, pair), 1) >= HD
    keys = dot(tok, wk[...], 1, 1)
    for h in range(heads):
        both = slice(h * pair, (h + 1) * pair)
        kcat[:, both] = jnp.where(entity == upper, keys[:, both], 0.0).astype(low)
    vt[...] = dot(r.v_weight[...], tok, 1, 1).astype(low)
    q_plain = dot(tok, wa[...], 1, 1)
    q_entity = dot(tok, wb[...], 1, 1)
    for h in range(heads):
        both = slice(h * pair, (h + 1) * pair)
        qcat[:, both] = jnp.where(entity, q_entity[:, both], q_plain[:, both]).astype(low)

    pt, mx, st = r.pt, r.mx, r.st
    scale = HD ** (-0.5)
    gathers = [
        LineGather(at, r.line_send.at[0], r.mx_recv.at[q], lambda block, q=q: mx[q].at[block])
        for q in range(len(spans))
    ]

    def pair_of(h):
        return pl.ds(pl.multiple_of(h * pair, pair), pair)

    def head_of(h):
        return pl.ds(pl.multiple_of(h * HD, HD), HD)

    def attend(q):
        start, size = spans[q]
        here = pl.ds(start, size)

        def head_step(h, carry):
            st[:, :size] = dot(kcat[:, pair_of(h)], qcat[here, pair_of(h)], 1, 1)

            def soften(i, carry):
                cols = pl.ds(pl.multiple_of(i * LANES, LANES), LANES)
                span = pl.ds(pl.multiple_of(start + i * LANES, LANES), LANES)
                scores = jnp.where(seg_wide[...] == r.seg_row[:, span], st[:, cols] * scale, -1000000000.0)
                shifted = jnp.exp(scores - jnp.max(scores, axis=0, keepdims=True))
                total = jnp.sum(shifted, axis=0, keepdims=True)
                pt[h, :, span] = (shifted * (1.0 / total)).astype(low)
                return carry

            lax.fori_loop(0, size // LANES, soften, 0)
            mixed = dot(vt[head_of(h), :], pt[h, :, here]).astype(low)
            mx[q][me, head_of(h), :] = mixed
            return carry

        lax.fori_loop(0, heads, head_step, 0)
        gathers[q].spread()

    def swap_plane():
        ow[me] = r.o_weight[...]
        for copy in ow_line:
            copy.wait_recv()
        for copy in ow_plane:
            copy.start()

    def swap_chip():
        for copy in ow_plane:
            copy.wait_recv()
        for copy in ow_chip:
            copy.start()

    def own_weights():
        for copy in ow_chip:
            copy.wait_recv()
        need("in_weight", "out_weight", "o_bias", "gain1", "shift1", "in_bias", "out_bias", "gain2", "shift2")
        for i, name in enumerate((r.o_bias, r.gain1, r.shift1, r.in_bias, r.out_bias, r.gain2, r.shift2)):
            vec[i, :] = name[...]

    tok_t, kct, vn = r.tok_t, r.kct, r.vn

    def turn():
        tok_t[...] = tokens[...].T
        kct[...] = kcat[...].T
        for h in range(heads):
            vn[h] = vt[h * HD : (h + 1) * HD, :].T

    xh1, rstd1, hl, mnat, mown, gbown = r.xh1, r.rstd1, r.hl, r.mnat, r.mown, r.gbown
    act, gp, dr2, gf, il, tmp, acc = r.act, r.gp, r.dr2, r.gf, r.il, r.tmp, r.acc
    acc[...] = jnp.zeros_like(acc)

    def make_lines(parts, send, part, out):
        lines = []
        for q, (start, size) in enumerate(spans):
            carry, single, summed, recv = parts[q]
            lines.append(LineReduce(at, part, carry, single, summed, send, recv, start, size // LINE, out))
        return lines

    ffn = make_lines(r.ffn, r.line_send.at[1], r.ffn_part, r.ffn_out)
    back = make_lines(r.back, r.line_send.at[2], r.back_part, r.back_part)
    swaps = [LineSwap(at, *parts) for parts in r.swap]
    grad = make_lines(r.grad, r.line_send.at[3], r.grad_part, r.tokens_grad)

    root_half = math.sqrt(0.5)
    density = 1.0 / math.sqrt(2.0 * math.pi)

    def forward(q):
        gathers[q].arrive()
        start, size = spans[q]
        here = pl.ds(start, size)
        mnat[:size, :] = mx[q][...].reshape(LINE * local_width, size).T
        tmp[:size, :] = dot(mnat[:size, :], ow[...].reshape(LINE * local_width, width))
        quarter_rows = size // LINE
        own = pl.ds(pl.multiple_of(me * quarter_rows, 16), quarter_rows)
        mown[start // LINE : (start + size) // LINE, :] = mnat[own, :]

        def first_norm(at_rows, inside):
            value = tmp[inside, :] + tokens[at_rows, :].astype(wide) + o_bias[...]
            centred = value - row_mean(value)
            scaled = lax.rsqrt(row_mean(centred * centred) + norm_epsilon)
            normal = centred * scaled
            xh1[at_rows, :] = normal
            rstd1[at_rows, :] = jnp.broadcast_to(scaled, (CHUNK, 128))
            hl[at_rows, :] = (normal * gain1[...] + shift1[...]).astype(low)

        rows_loop(start, size, first_norm)
        tmp[:size, :] = dot(hl[here, :], r.in_weight[...])

        def activate(at_rows, inside):
            inner = tmp[inside, :] + in_bias[...]
            gate = 0.5 + 0.5 * lax.erf(inner * root_half)
            act[at_rows, :] = (inner * gate).astype(low)
            gp[at_rows, :] = gate + inner * (density * jnp.exp(-0.5 * inner * inner))

        rows_loop(start, size, activate)
        r.ffn_part[here, :] = dot(act[here, :], r.out_weight[...]).astype(low)
        ffn[q].start()

    def backward(q):
        ffn[q].arrive()
        start, size = spans[q]
        here = pl.ds(start, size)

        def second_norm(at_rows, inside):
            value = xh1[at_rows, :] * gain1[...] + shift1[...]
            value = value + r.ffn_out[at_rows, :].astype(wide) + out_bias[...]
            centred = value - row_mean(value)
            scaled = lax.rsqrt(row_mean(centred * centred) + norm_epsilon)
            normal = centred * scaled
            r.layer_out[at_rows, :] = (normal * gain2[...] + shift2[...]).astype(low)
            cot = r.cotangent[at_rows, :].astype(wide)
            acc[6] += fold(cot)
            acc[5] += fold(cot * normal)
            grown = cot * gain2[...]
            grad_in = scaled * (grown - row_mean(grown) - normal * row_mean(grown * normal))
            acc[4] += fold(grad_in)
            dr2[at_rows, :] = grad_in
            gf[at_rows, :] = grad_in.astype(low)

        rows_loop(start, size, second_norm)
        tmp[:size, :] = dot(gf[here, :], r.out_weight[...], 1, 1)

        def inner_step(at_rows, inside):
            d_inner = tmp[inside, :] * gp[at_rows, :]
            acc[3] += fold(d_inner)
            il[at_rows, :] = d_inner.astype(low)

        rows_loop(start, size, inner_step)
        r.back_part[here, :] = dot(il[here, :], r.in_weight[...], 1, 1).astype(low)
        back[q].start()

    dqa, dqb, dkv, dk_sum, dv_sum = r.dqa, r.dqb, r.dkv, r.dk_sum, r.dv_sum
    dmt, ds = r.dmt, r.ds

    def settle_back(q):
        start, size = spans[q]
        own = back[q].rows_of(me)
        d_hidden = dr2[own, :] + back[q].total()
        normal = xh1[own, :]
        acc[2] += fold(d_hidden)
        acc[1] += fold(d_hidden * normal)
        grown = d_hidden * gain1[...]
        grad_in = rstd1[own, 0:1] * (grown - row_mean(grown) - normal * row_mean(grown * normal))
        acc[0] += fold(grad_in)
        dr2[own, :] = grad_in
        grad_low = grad_in.astype(low)
        gbown[start // LINE : (start + size) // LINE, :] = grad_low
        for j in range(LINE):
            swaps[q].sent[j] = dot(grad_low, ow[j], 1, 1).astype(low)
        swaps[q].start()

    def finish_rows(q):
        swaps[q].wait()
        start, size = spans[q]
        here = pl.ds(start, size)
        for h in range(heads):
            dmt[h, :size, :] = swaps[q].got[:, :, h * HD : (h + 1) * HD].reshape(size, HD)

        def head_step(h, carry):
            d_mixed = dmt[h, :size, :]
            st[:, :size] = dot(vn[h], d_mixed, 1, 1)

            def harden(i, carry):
                cols = pl.ds(pl.multiple_of(i * LANES, LANES), LANES)
                span = pl.ds(pl.multiple_of(start + i * LANES, LANES), LANES)
                prob = pt[h, :, span].astype(wide)
                d_prob = st[:, cols]
                delta = jnp.sum(prob * d_prob, axis=0, keepdims=True)
                ds[:, cols] = (prob * (d_prob - delta) * scale).astype(low)
                return carry

            lax.fori_loop(0, size // LANES, harden, 0)
            d_score = ds[:, :size]
            d_value = dot(pt[h, :, here], d_mixed)
            d_key = dot(d_score, qcat[here, pair_of(h)])
            if q == 0:
                dv_sum[h] = d_value
                dk_sum[h] = d_key
            else:
                dv_sum[h] += d_value
                dk_sum[h] += d_key
            d_query = dot(kct[pair_of(h), :], d_score).T
            row_entity = kind_wide[here, :] == 1
            dqa[here, pair_of(h)] = jnp.where(row_entity, 0.0, d_query).astype(low)
            dqb[here, pair_of(h)] = jnp.where(row_entity, d_query, 0.0).astype(low)
            return carry

        lax.fori_loop(0, heads, head_step, 0)

    gfeed, gattn = r.gfeed, r.gattn
    blocks, per_block = gfeed.shape[0], gfeed.shape[1]

    def put_grad(packed, start, value):
        packed[:, :, start : start + value.shape[1]] = value.astype(low).reshape(blocks, per_block, value.shape[1])

    if planar:
        feed = PlaneReduce(gfeed, *r.feed)
        attn = PlaneReduce(gattn, *r.attn)

    small = r.small
    if planar:
        small_sum = r.small_sum
        tiny = [
            remote(
                small if s == 0 else small_sum.at[s - 1],
                r.small_in.at[s],
                r.small_send.at[s],
                r.small_recv.at[s],
                dp=(across, over_x, over_y)[s],
            )
            for s in range(3)
        ]

    def tiny_step(s):
        if planar:
            tiny[s].wait_recv()
            small_sum[s] = (small if s == 0 else small_sum.at[s - 1])[...] + r.small_in[s]
            if s < 2:
                tiny[s + 1].start()

    norms = LineSwap(at, *r.norms)
    if planar:
        o_swap = LineSwap(at, *r.o_swap)

    def feed_step(i):
        if i == 0:
            put_grad(gfeed, hidden_width, dot(gf[...], act[...], 0, 0))
        elif i == 1:
            put_grad(gfeed, 0, dot(hl[...], il[...], 0, 0))
        elif planar and i == 2:
            feed.start()
        elif planar and i == 3:
            feed.step_one()
        elif planar and i == 4:
            feed.step_two()
        elif planar and i == 5:
            feed_sum = feed.finish()
            r.in_grad[...] = feed_sum[:, :hidden_width]
            r.out_grad[...] = feed_sum[:, hidden_width : 2 * hidden_width]
            for j in range(LINE):
                begin = 2 * hidden_width + j * local_width
                o_swap.sent[j] = feed_sum[:, begin : begin + local_width].astype(low)
            o_swap.start()
            stores["in_grad"].start()
            stores["out_grad"].start()

    def share_norms():
        for i in range(8):
            norms.sent[0, i : i + 1, :] = jnp.sum(acc[i], axis=0, keepdims=True)
        for j in range(1, LINE):
            norms.sent[j] = norms.sent[0]
        norms.start()
        put_grad(gfeed, 2 * hidden_width, dot(gbown[...], mown[...], 0, 0))

    def key_grads():
        norms.wait()
        small[...] = norms.sent[0]
        small[0:3, :] = norms.got[0, 0:3] + norms.got[1, 0:3] + norms.got[2, 0:3] + norms.got[3, 0:3]
        if planar:
            tiny[0].start()
        d_keys = [
            jnp.where(kind_wide[:, :HD] == 1, dk_sum[h, :, HD:], dk_sum[h, :, :HD]).astype(low)
            for h in range(heads)
        ]
        d_values = [dv_sum[h].astype(low) for h in range(heads)]
        dkv[...] = jnp.concatenate(d_keys + d_values, axis=1)

    def input_share(q):
        start, size = spans[q]
        here = pl.ds(start, size)
        share = dot(dqa[here, :], wa[...]) + dot(dqb[here, :], wb[...])
        share = share + dot(dkv[here, :local_width], r.k_weight[...]) + dot(dkv[here, local_width:], r.v_weight[...])
        r.grad_part[here, :] = share.astype(low)
        grad[q].start()

    def attn_step(i):
        if i == 0:
            put_grad(gattn, 0, dot(tok_t[...], dqa[...]))
            put_grad(gattn, 2 * local_width, dot(tok_t[...], dqb[...]))
        elif i == 1:
            put_grad(gattn, 4 * local_width, dot(tok_t[...], dkv[...]))
        elif planar and i == 2:
            attn.start()
            tiny_step(0)
        elif planar and i == 3:
            attn.step_one()
            tiny_step(1)
        elif planar and i == 4:
            attn.step_two()
            tiny_step(2)

    attend(0)
    attend(1)
    attend(2)
    attend(3)
    gathers[0].relay(0)
    swap_plane()
    gathers[0].relay(1)
    attend(4)
    gathers[3].relay(0)
    gathers[2].relay(0)
    gathers[3].relay(1)
    gathers[4].relay(0)
    gathers[0].relay(2)
    gathers[1].relay(0)
    gathers[3].relay(2)
    gathers[2].relay(1)
    gathers[1].relay(1)
    gathers[4].relay(1)
    turn()
    swap_chip()
    own_weights()
    gathers[1].relay(2)
    forward(0)
    ffn[0].forward(0)
    gathers[2].relay(2)
    forward(3)
    gathers[4].relay(2)
    ffn[0].forward(1)
    ffn[3].forward(0)
    forward(1)
    ffn[3].forward(1)
    ffn[0].settle()
    ffn[1].forward(0)
    forward(2)
    ffn[1].forward(1)
    ffn[0].relay(0)
    ffn[2].forward(0)
    ffn[3].settle()
    ffn[2].forward(1)
    ffn[0].relay(1)
    forward(4)
    ffn[3].relay(0)
    ffn[4].forward(0)
    ffn[0].relay(2)
    ffn[4].forward(1)
    ffn[1].settle()
    ffn[2].settle()
    ffn[3].relay(1)
    ffn[3].relay(2)
    ffn[1].relay(0)
    ffn[2].relay(0)
    ffn[1].relay(1)
    ffn[4].settle()
    ffn[4].relay(0)
    ffn[1].relay(2)
    ffn[2].relay(1)
    need("cotangent")
    backward(0)
    ffn[2].relay(2)
    ffn[4].relay(1)
    backward(3)
    back[0].forward(0)
    back[0].forward(1)
    ffn[4].relay(2)
    backward(1)
    back[3].forward(0)
    backward(2)
    back[1].forward(0)
    settle_back(0)
    back[2].forward(0)
    back[1].forward(1)
    back[3].forward(1)
    backward(4)
    stores["layer_out"].start()
    back[2].forward(1)
    feed_step(0)
    back[4].forward(0)
    settle_back(1)
    back[4].forward(1)
    feed_step(1)
    settle_back(2)
    settle_back(3)
    finish_rows(0)
    settle_back(4)
    share_norms()
    feed_step(2)
    finish_rows(1)
    finish_rows(2)
    finish_rows(3)
    finish_rows(4)
    key_grads()
    input_share(0)
    feed_step(3)
    input_share(1)
    input_share(2)
    grad[0].forward(0)
    input_share(3)
    input_share(4)
    grad[0].forward(1)
    attn_step(0)
    grad[1].forward(0)
    grad[1].forward(1)
    attn_step(1)
    grad[2].forward(0)
    grad[2].forward(1)
    attn_step(2)
    grad[3].forward(0)
    grad[3].forward(1)
    grad[2].settle(dr2)
    grad[4].forward(0)
    grad[0].settle(dr2)
    feed_step(4)
    grad[4].forward(1)
    attn_step(3)
    grad[3].settle(dr2)
    grad[2].relay(0)
    grad[2].relay(1)
    grad[1].settle(dr2)
    grad[0].relay(0)
    grad[0].relay(1)
    grad[4].settle(dr2)
    grad[1].relay(0)
    grad[3].relay(0)
    grad[3].relay(1)
    grad[2].relay(2)
    grad[4].relay(0)
    grad[1].relay(1)
    feed_step(5)
    grad[4].relay(1)
    attn_step(4)
    grad[1].relay(2)
    grad[3].relay(2)
    grad[4].relay(2)
    grad[0].relay(2)
    if planar:
        attn_sum = attn.finish()
        for part in range(4):
            base = (part // 2) * 2 * local_width + (part % 2) * HD
            r.q_grad[part] = jnp.concatenate(
                [attn_sum[:, base + h * pair : base + h * pair + HD] for h in range(heads)], axis=1
            )
        both_grads = attn_sum[:, 4 * local_width : 6 * local_width]
        r.k_grad[...] = both_grads[:, :local_width]
        r.v_grad[...] = both_grads[:, local_width:]
        o_swap.wait()
        o_sum = o_swap.got[0].astype(wide) + o_swap.got[1].astype(wide)
        r.o_grad[...] = (o_sum + o_swap.got[2].astype(wide) + o_swap.got[3].astype(wide)).T
        o_swap.drain()
        r.small_out[...] = small_sum[2]
        for name in ("q_grad", "k_grad", "v_grad", "o_grad", "small_out"):
            stores[name].start()
    else:
        r.small_out[...] = small[...]
        r.feed_out[...] = gfeed[...]
        r.attn_out[...] = gattn[...]
        for name in ("small_out", "feed_out", "attn_out"):
            stores[name].start()
    for line in grad:
        line.arrive()
    stores["tokens_grad"].start()

    def sent_all(i, held):
        remote(held, held, r.line_send.at[i], r.mx_recv.at[0, 0], mp=at.mid).wait_send()

    blocks_out = rows // LINE * 3

    @pl.when(at.is_end)
    def _():
        sent_all(0, vt)
        sent_all(1, hl)
        sent_all(2, hl.at[:blocks_out])
        sent_all(3, hl)

    @pl.when(at.is_mid)
    def _():
        sent_all(0, xh1.at[: 5 * rows * local_width // (2 * width)])
        sent_all(1, xh1)
        sent_all(2, hl.at[:blocks_out])
        sent_all(3, xh1)

    for swap in swaps + [norms]:
        swap.drain()
    for copy in ow_line + ow_plane + ow_chip:
        copy.wait_send()
    if planar:
        for copy in tiny:
            copy.wait_send()
    for copy in stores.values():
        copy.wait()


def hand_on(layout, *refs):
    sources, targets, held, lines, sems = jax.tree.unflatten(layout, refs)
    count = len(sources) - 1
    small = held[0]
    fetch = [pltpu.make_async_copy(source, kept, sems.at[0, i]) for i, (source, kept) in enumerate(zip(sources, held))]
    store = [
        pltpu.make_async_copy(kept, target, sems.at[1, i])
        for i, (kept, target) in enumerate(zip(list(held[1:]) + list(lines), targets))
    ]
    for copy in fetch:
        copy.start()
    fetch[0].wait()
    for i, line in enumerate(lines):
        line[...] = small[i, :]
        store[count + i].start()
    for i in range(count):
        fetch[1 + i].wait()
        store[i].start()
    for copy in store:
        copy.wait()


def local(
    tokens,
    segment_ids,
    token_types,
    q_weight,
    k_weight,
    v_weight,
    o_weight,
    o_bias,
    norm1_gain,
    norm1_shift,
    in_weight,
    in_bias,
    out_weight,
    out_bias,
    norm2_gain,
    norm2_shift,
    cotangent,
):
    rows, width = tokens.shape
    local_width = k_weight.shape[1]
    heads = local_width // HD
    hidden_width = in_weight.shape[1]
    n_dp = lax.axis_size("dp")
    planar = n_dp == 8
    blocks = 8
    per_block = width // blocks
    spans = portions_of(rows)
    largest = max(size for _, size in spans)
    low, wide = jnp.bfloat16, jnp.float32
    attn_width = 6 * local_width
    feed_width = 2 * hidden_width + LINE * local_width
    args = dict(
        tokens=tokens,
        seg_row=segment_ids,
        kind_row=token_types,
        q_weight=q_weight.swapaxes(1, 2),
        k_weight=k_weight.T,
        v_weight=v_weight.T,
        o_weight=o_weight,
        o_bias=o_bias,
        gain1=norm1_gain,
        shift1=norm1_shift,
        in_bias=in_bias,
        out_bias=out_bias,
        gain2=norm2_gain,
        shift2=norm2_shift,
        in_weight=in_weight,
        out_weight=out_weight,
        cotangent=cotangent,
    )
    shaped = jax.ShapeDtypeStruct
    outs = dict(
        layer_out=shaped((rows, width), low),
        tokens_grad=shaped((rows, width), low),
        small_out=shaped((8, width), wide),
    )
    if planar:
        outs |= dict(
            q_grad=shaped((4, per_block, local_width), wide),
            k_grad=shaped((per_block, local_width), wide),
            v_grad=shaped((per_block, local_width), wide),
            o_grad=shaped((local_width, per_block), wide),
            in_grad=shaped((per_block, hidden_width), wide),
            out_grad=shaped((per_block, hidden_width), wide),
        )
    else:
        outs |= dict(
            feed_out=shaped((blocks, per_block, feed_width), low),
            attn_out=shaped((blocks, per_block, attn_width), low),
        )
    dma = pltpu.SemaphoreType.DMA
    scratch = dict(
        ow=pltpu.VMEM((LINE, local_width, width), low),
        ow_send=dma((9,)),
        ow_recv=dma((9,)),
        wa=pltpu.VMEM((2 * local_width, width), low),
        wb=pltpu.VMEM((2 * local_width, width), low),
        wk=pltpu.VMEM((2 * local_width, width), low),
        kind_wide=pltpu.VMEM((rows, 2 * HD), jnp.int32),
        seg_wide=pltpu.VMEM((rows, 2 * HD), jnp.int32),
        qcat=pltpu.VMEM((rows, 2 * local_width), low),
        kcat=pltpu.VMEM((rows, 2 * local_width), low),
        vt=pltpu.VMEM((local_width, rows), low),
        pt=pltpu.VMEM((heads, rows, rows), low),
        mx=[pltpu.VMEM((LINE, local_width, size), low) for _, size in spans],
        st=pltpu.VMEM((rows, largest), wide),
        ds=pltpu.VMEM((rows, largest), low),
        line_send=dma((4,)),
        mx_recv=dma((len(spans), LINE)),
        tok_t=pltpu.VMEM((width, rows), low),
        xh1=pltpu.VMEM((rows, width), wide),
        rstd1=pltpu.VMEM((rows, 128), wide),
        hl=pltpu.VMEM((rows, width), low),
        act=pltpu.VMEM((rows, hidden_width), low),
        gp=pltpu.VMEM((rows, hidden_width), wide),
        dr2=pltpu.VMEM((rows, width), wide),
        gf=pltpu.VMEM((rows, width), low),
        il=pltpu.VMEM((rows, hidden_width), low),
        tmp=pltpu.VMEM((largest, width), wide),
        vec=pltpu.VMEM((8, width), wide),
        acc=pltpu.VMEM((8, 8, width), wide),
        mnat=pltpu.VMEM((largest, LINE * local_width), low),
        mown=pltpu.VMEM((rows // LINE, LINE * local_width), low),
        gbown=pltpu.VMEM((rows // LINE, width), low),
        swap=[swap_scratch(size // LINE, local_width, low) for _, size in spans],
        norms=swap_scratch(8, width, wide),
        ffn_part=pltpu.VMEM((rows, width), low),
        back_part=pltpu.VMEM((rows, width), low),
        grad_part=pltpu.VMEM((rows, width), low),
        ffn_out=pltpu.VMEM((rows, width), low),
        gfeed=pltpu.VMEM((blocks, per_block, feed_width), low),
        gattn=pltpu.VMEM((blocks, per_block, attn_width), low),
        small=pltpu.VMEM((8, width), wide),
        kct=pltpu.VMEM((2 * local_width, rows), low),
        vn=pltpu.VMEM((heads, rows, HD), low),
        dmt=pltpu.VMEM((heads, largest, HD), low),
        dk_sum=pltpu.VMEM((heads, rows, 2 * HD), wide),
        dv_sum=pltpu.VMEM((heads, rows, HD), wide),
        dqa=pltpu.VMEM((rows, 2 * local_width), low),
        dqb=pltpu.VMEM((rows, 2 * local_width), low),
        dkv=pltpu.VMEM((rows, 2 * local_width), low),
    )
    for name in ("ffn", "back", "grad"):
        scratch[name] = [line_scratch(size // LINE, width) for _, size in spans]
    if planar:
        scratch |= dict(
            feed=plane_scratch(per_block, feed_width),
            o_swap=swap_scratch(per_block, local_width, low),
            attn=plane_scratch(per_block, attn_width),
            small_in=pltpu.VMEM((3, 8, width), wide),
            small_sum=pltpu.VMEM((3, 8, width), wide),
            small_send=dma((3,)),
            small_recv=dma((3,)),
        )
    scratch |= dict(
        held={name: pltpu.VMEM(a.shape, a.dtype) for name, a in args.items()},
        made={name: pltpu.VMEM(a.shape, a.dtype) for name, a in outs.items()},
        load_sem=dma((len(args),)),
        store_sem=dma((len(outs),)),
    )
    layout = jax.tree.structure((args, outs, scratch))
    vm, far = pl.BlockSpec(memory_space=pltpu.VMEM), pl.BlockSpec(memory_space=pl.ANY)
    results = pl.pallas_call(
        functools.partial(layer_kernel, planar, layout),
        out_shape=jax.tree.leaves(outs),
        in_specs=[far] * len(args),
        out_specs=[far] * len(outs),
        scratch_shapes=jax.tree.leaves(scratch),
        compiler_params=pltpu.CompilerParams(
            collective_id=0, has_side_effects=True, vmem_limit_bytes=VMEM_LIMIT
        ),
    )(*jax.tree.leaves(args))
    results = dict(zip(sorted(outs), results))
    if planar:
        small = results.pop("small_out")
        flat, tree = jax.tree.flatten(results)
        vectors = small.shape[0] - 1
        line = (width,)
        targets = [shaped(a.shape, a.dtype) for a in flat] + [shaped(line, wide)] * vectors
        held = [pltpu.VMEM(a.shape, a.dtype) for a in [small] + flat]
        lines = [pltpu.VMEM(line, wide)] * vectors
        sems = dma((2, len(targets)))
        pieces = ([small] + flat, targets, held, lines, sems)
        flat = pl.pallas_call(
            functools.partial(hand_on, jax.tree.structure(pieces)),
            out_shape=targets,
            in_specs=[far] * (1 + len(flat)),
            out_specs=[far] * len(targets),
            scratch_shapes=held + lines + [sems],
            compiler_params=pltpu.CompilerParams(vmem_limit_bytes=VMEM_LIMIT),
        )(small, *flat)
        small = flat[len(results) :]
        results = jax.tree.unflatten(tree, flat[: len(results)])
    res = types.SimpleNamespace(**results)
    if planar:
        grads = (res.q_grad, res.k_grad, res.v_grad, res.o_grad, res.in_grad, res.out_grad.T)
    else:
        feed = res.feed_out.astype(wide).reshape(width, feed_width)
        attn = res.attn_out.astype(wide).reshape(width, attn_width)
        feed = lax.psum_scatter(feed, "dp", scatter_dimension=0, tiled=True)
        attn = lax.psum_scatter(attn, "dp", scatter_dimension=0, tiled=True)
        small = lax.psum(res.small_out, "dp")
        per = feed.shape[0]
        o_part = lax.psum_scatter(feed[:, 2 * hidden_width :], "mp", scatter_dimension=1, tiled=True)
        queries = attn[:, : 4 * local_width].reshape(per, 2, heads, 2, HD)
        queries = queries.transpose(1, 3, 0, 2, 4).reshape(4, per, local_width)
        grads = (
            queries,
            attn[:, 4 * local_width : 5 * local_width],
            attn[:, 5 * local_width : 6 * local_width],
            o_part.T,
            feed[:, :hidden_width],
            feed[:, hidden_width : 2 * hidden_width].T,
        )
    d_q, d_k, d_v, d_o, d_in, d_out = grads
    return (
        res.layer_out,
        res.tokens_grad,
        d_q,
        d_k,
        d_v,
        d_o,
        small[0],
        small[1],
        small[2],
        d_in,
        small[3],
        d_out,
        small[4],
        small[5],
        small[6],
    )


def solution(mesh):
    return jax.shard_map(
        local,
        mesh=mesh,
        in_specs=(
            P("dp", None),
            P("dp", None),
            P("dp", None),
            P(None, None, "mp"),
            P(None, "mp"),
            P(None, "mp"),
            P("mp", None),
            P(),
            P(),
            P(),
            P(None, "mp"),
            P("mp"),
            P("mp", None),
            P(),
            P(),
            P(),
            P("dp", None),
        ),
        out_specs=(
            P("dp", None),
            P("dp", None),
            P(None, "dp", "mp"),
            P("dp", "mp"),
            P("dp", "mp"),
            P("mp", "dp"),
            P(),
            P(),
            P(),
            P("dp", "mp"),
            P("mp"),
            P("mp", "dp"),
            P(),
            P(),
            P(),
        ),
        check_vma=False,
    )
```

```python
import functools
import math
import operator
import types

import jax
import jax.numpy as jnp
from jax import lax
from jax.experimental import pallas as pl
from jax.experimental.pallas import tpu as pltpu
from jax.sharding import PartitionSpec as P

HD = 64
LINE = 4
PORTIONS = (1, 1, 1, 1, 1)
LANES = 128
CHUNK = 32
VMEM_LIMIT = 67043328

norm_epsilon = 1e-05


def remote(src, dst, send_sem, recv_sem, **axes):
    return pltpu.make_async_remote_copy(
        src_ref=src,
        dst_ref=dst,
        send_sem=send_sem,
        recv_sem=recv_sem,
        device_id=axes,
        device_id_type=pl.DeviceIdType.MESH,
    )


class Place:
    def __init__(self):
        me = lax.axis_index("mp")
        self.me = me
        self.is_mid = jnp.logical_or(me == 1, me == 2)
        self.is_end = jnp.logical_not(self.is_mid)
        left = me < 2
        self.mid = jnp.where(left, 1, 2)
        self.end = jnp.where(left, 0, 3)
        self.far_mid = 3 - self.mid
        self.far_end = 3 - self.end


class LineGather:
    def __init__(self, place, send, recv, out):
        self.at, self.send, self.recv, self.out = place, send, recv, out

    def copy(self, block, slot, target):
        return remote(self.out(block), self.out(block), self.send, self.recv.at[block], mp=target)

    def spread(self):
        at = self.at

        @pl.when(at.is_end)
        def _():
            self.copy(at.me, 0, at.mid).start()

        @pl.when(at.is_mid)
        def _():
            self.copy(at.me, 0, at.end).start()
            self.copy(at.me, 1, at.far_mid).start()

    def relay(self, step):
        at = self.at
        block = (at.end, at.far_mid, at.far_end)[step]
        target = (at.far_mid, at.end, at.end)[step]

        @pl.when(at.is_mid)
        def _():
            self.copy(block, 2 + step, target).wait_recv()
            self.copy(block, 2 + step, target).start()

    def arrive(self):
        at = self.at

        @pl.when(at.is_end)
        def _():
            self.copy(at.mid, 0, at.mid).wait_recv()
            self.copy(at.far_mid, 0, at.mid).wait_recv()
            self.copy(at.far_end, 0, at.mid).wait_recv()


class LineReduce:
    def __init__(self, place, part, carry, single, summed, send, recv, start, block_rows, out):
        self.at, self.carry, self.single, self.summed = place, carry, single, summed
        self.send, self.recv = send, recv

        def rows_of(block):
            return pl.ds(pl.multiple_of(start + block * block_rows, 16), block_rows)

        self.rows_of, self.part_ref, self.out_ref = rows_of, part, out
        self.gather = LineGather(place, send, recv.at[1], lambda block: out.at[rows_of(block)])

    def part(self, block):
        return self.part_ref.at[self.rows_of(block)]

    def end_sends(self):
        at, send, recv = self.at, self.send, self.recv
        return (
            remote(self.part(at.far_end), self.carry.at[0], send, recv.at[0, 2], mp=at.mid),
            remote(self.part(at.far_mid), self.carry.at[1], send, recv.at[0, 3], mp=at.mid),
            remote(self.part(at.mid), self.single, send, recv.at[0, 0], mp=at.mid),
        )

    def mid_sends(self):
        at, send, recv = self.at, self.send, self.recv
        return (
            remote(self.carry.at[0], self.summed, send, recv.at[0, 1], mp=at.far_end),
            remote(self.carry.at[1], self.summed, send, recv.at[0, 1], mp=at.far_mid),
            remote(self.part(at.end), self.single, send, recv.at[0, 0], mp=at.end),
        )

    def start(self):
        @pl.when(self.at.is_end)
        def _():
            for copy in self.end_sends():
                copy.start()

        @pl.when(self.at.is_mid)
        def _():
            self.mid_sends()[2].start()

    def forward(self, step):
        at = self.at

        @pl.when(at.is_mid)
        def _():
            block = (at.far_end, at.far_mid)[step]
            self.end_sends()[step].wait_recv()
            total = self.carry[step].astype(jnp.float32) + self.part(block)[...].astype(jnp.float32)
            self.carry[step] = total.astype(jnp.bfloat16)
            self.mid_sends()[step].start()

    def total(self):
        self.end_sends()[2].wait_recv()
        self.mid_sends()[0].wait_recv()
        return (
            self.part(self.at.me)[...].astype(jnp.float32)
            + self.single[...].astype(jnp.float32)
            + self.summed[...].astype(jnp.float32)
        )

    def settle(self, extra=None):
        at = self.at
        total = self.total()
        if extra is not None:
            total = total + extra[self.rows_of(at.me), :]
        self.out_ref[self.rows_of(at.me), :] = total.astype(jnp.bfloat16)
        self.gather.spread()

    def relay(self, step):
        self.gather.relay(step)

    def arrive(self):
        self.gather.arrive()


class LineSwap:
    def __init__(self, place, sent, got, send, recv):
        me = place.me
        self.me, self.sent, self.got = me, sent, got
        targets = [lax.rem(me + step, LINE) for step in range(1, LINE)]
        self.outward = [
            remote(sent.at[j], got.at[me], send.at[i], recv.at[me], mp=j) for i, j in enumerate(targets)
        ]
        self.inward = [remote(got.at[j], got.at[j], send.at[i], recv.at[j], mp=j) for i, j in enumerate(targets)]

    def start(self):
        for copy in self.outward:
            copy.start()
        self.got[self.me] = self.sent[self.me]

    def wait(self):
        for copy in self.inward:
            copy.wait_recv()

    def drain(self):
        for copy in self.outward:
            copy.wait_send()


def swap_scratch(rows, width, kind):
    return [
        pltpu.VMEM((LINE, rows, width), kind),
        pltpu.VMEM((LINE, rows, width), kind),
        pltpu.SemaphoreType.DMA((LINE - 1,)),
        pltpu.SemaphoreType.DMA((LINE,)),
    ]


def line_scratch(rows, width):
    return [
        pltpu.VMEM((2, rows, width), jnp.bfloat16),
        pltpu.VMEM((rows, width), jnp.bfloat16),
        pltpu.VMEM((rows, width), jnp.bfloat16),
        pltpu.SemaphoreType.DMA((2, 4)),
    ]


class PlaneReduce:
    def __init__(self, grads, r1, sums, mid2, r2a, r2b, s3a, s3b, r3a, r3b, send, recv):
        self.grads, self.r1, self.sums, self.mid2 = grads, r1, sums, mid2
        self.r2a, self.r2b, self.s3a, self.s3b, self.r3a, self.r3b = r2a, r2b, s3a, s3b, r3a, r3b
        dp = lax.axis_index("dp")
        self.core, self.x, self.y = lax.rem(dp, 2), lax.rem(dp // 2, 2), dp // 4
        across = dp + 1 - 2 * self.core
        over_x = dp + 2 - 4 * self.x
        over_y = dp + 4 - 8 * self.y
        half = r2a.shape[2]
        self.low, self.high = pl.ds(0, half), pl.ds(half, grads.shape[2] - half)
        self.first = [
            remote(grads.at[2 * k + 1 - self.core], r1.at[k], send.at[k], recv.at[k], dp=across) for k in range(4)
        ]
        self.second = [
            remote(mid2.at[2 * j + 1 - self.x, :, self.low], r2a.at[j], send.at[4 + j], recv.at[4 + j], dp=over_x)
            for j in range(2)
        ] + [
            remote(mid2.at[2 * (1 - self.y) + j, :, self.high], r2b.at[j], send.at[6 + j], recv.at[6 + j], dp=over_y)
            for j in range(2)
        ]
        self.third = [
            remote(s3a, r3a, send.at[8], recv.at[8], dp=over_y),
            remote(s3b, r3b, send.at[9], recv.at[9], dp=over_x),
        ]

    def start(self):
        for copy in self.first:
            copy.start()

    def step_one(self):
        for copy in self.first:
            copy.wait_recv()

        def body(k, carry):
            total = self.grads[2 * k + self.core].astype(jnp.float32) + self.r1[k].astype(jnp.float32)
            self.sums[k] = total
            self.mid2[k] = total.astype(jnp.bfloat16)
            return carry

        lax.fori_loop(0, 4, body, 0)
        for copy in self.second:
            copy.start()

    def step_two(self):
        for copy in self.second:
            copy.wait_recv()
        x, y = self.x, self.y
        self.s3a[...] = (
            self.sums[2 * (1 - y) + x, :, self.low] + self.r2a[1 - y].astype(jnp.float32)
        ).astype(jnp.bfloat16)
        self.third[0].start()
        self.s3b[...] = (
            self.sums[2 * y + 1 - x, :, self.high] + self.r2b[1 - x].astype(jnp.float32)
        ).astype(jnp.bfloat16)
        self.third[1].start()

    def finish(self):
        x, y = self.x, self.y
        for copy in self.third:
            copy.wait_recv()
        own = self.sums.at[2 * y + x]
        own[:, self.low] = own[:, self.low] + self.r2a[y].astype(jnp.float32) + self.r3a[...].astype(jnp.float32)
        own[:, self.high] = own[:, self.high] + self.r2b[x].astype(jnp.float32) + self.r3b[...].astype(jnp.float32)
        for copy in self.first + self.second + self.third:
            copy.wait_send()
        return own


def plane_scratch(rows, width):
    half = (width // 128 + 1) // 2 * 128
    rest = width - half
    low = jnp.bfloat16
    return [
        pltpu.VMEM((4, rows, width), low),
        pltpu.VMEM((4, rows, width), jnp.float32),
        pltpu.VMEM((4, rows, width), low),
        pltpu.VMEM((2, rows, half), low),
        pltpu.VMEM((2, rows, rest), low),
        pltpu.VMEM((rows, half), low),
        pltpu.VMEM((rows, rest), low),
        pltpu.VMEM((rows, half), low),
        pltpu.VMEM((rows, rest), low),
        pltpu.SemaphoreType.DMA((10,)),
        pltpu.SemaphoreType.DMA((10,)),
    ]


def dot(left, right, left_dim=1, right_dim=0):
    return lax.dot_general(
        left, right, (((left_dim,), (right_dim,)), ((), ())), preferred_element_type=jnp.float32
    )


def rows_loop(start, count, body):
    def step(i, carry):
        inside = pl.ds(pl.multiple_of(i * CHUNK, CHUNK), CHUNK)
        body(pl.ds(pl.multiple_of(start + i * CHUNK, CHUNK), CHUNK), inside)
        return carry

    lax.fori_loop(0, count // CHUNK, step, 0, unroll=True)


def fold(value):
    return jnp.sum(value.reshape(value.shape[0] // 8, 8, value.shape[1]), axis=0)


def row_mean(value):
    return jnp.mean(value, axis=-1, keepdims=True)


def portions_of(rows):
    unit = rows // sum(PORTIONS)
    return [(unit * sum(PORTIONS[:i]), unit * size) for i, size in enumerate(PORTIONS)]


def layer_kernel(planar, layout, *refs):
    given, wanted, scratch = jax.tree.unflatten(layout, refs)
    r = types.SimpleNamespace(**scratch, **scratch["held"], **scratch["made"])
    loads = {
        name: pltpu.make_async_copy(given[name], r.held[name], r.load_sem.at[i]) for i, name in enumerate(given)
    }
    stores = {
        name: pltpu.make_async_copy(r.made[name], wanted[name], r.store_sem.at[i]) for i, name in enumerate(wanted)
    }

    def need(*names):
        for name in names:
            loads[name].wait()

    tokens, rows, width = r.tokens, r.tokens.shape[0], r.tokens.shape[1]
    local_width = r.k_weight.shape[0]
    heads = local_width // HD
    pair = 2 * HD
    hidden_width = r.in_weight.shape[1]
    spans = portions_of(rows)
    low, wide = jnp.bfloat16, jnp.float32
    at = Place()
    me = at.me
    dp = lax.axis_index("dp")
    core = lax.rem(dp, 2)
    across = dp + 1 - 2 * core

    barrier = pltpu.get_barrier_semaphore()
    near = lax.rem(dp // 2, 2)
    over_x = dp + 2 - 4 * near
    peers = [{"mp": lax.rem(me + step, LINE)} for step in range(1, LINE)] + [{"dp": across}, {"dp": over_x}]
    if planar:
        over_y = dp + 4 - 8 * (dp // 4)
        peers += [{"dp": over_y}]
    for peer in peers:
        pl.semaphore_signal(barrier, inc=1, device_id=peer, device_id_type=pl.DeviceIdType.MESH)

    first = ("k_weight", "tokens", "kind_row", "seg_row", "v_weight", "q_weight", "o_weight")
    for name in first + tuple(name for name in loads if name not in first):
        loads[name].start()

    wa, wb, wk = r.wa, r.wb, r.wk
    need("k_weight", "q_weight")
    for h in range(heads):
        cols = slice(h * HD, (h + 1) * HD)
        both = slice(h * pair, (h + 1) * pair)
        wa[both, :] = jnp.concatenate([r.q_weight[0, cols, :], r.q_weight[1, cols, :]], axis=0)
        wb[both, :] = jnp.concatenate([r.q_weight[2, cols, :], r.q_weight[3, cols, :]], axis=0)
        key_part = r.k_weight[cols, :]
        wk[both, :] = jnp.concatenate([key_part, key_part], axis=0)
    need("o_weight")
    pl.semaphore_wait(barrier, len(peers))

    ow, ow_send, ow_recv = r.ow, r.ow_send, r.ow_recv
    vec = r.vec
    o_bias, gain1, shift1, in_bias, out_bias, gain2, shift2 = (vec.at[i : i + 1] for i in range(7))
    share = local_width // 4
    quarter = pl.ds(pl.multiple_of((2 * core + near) * share, 16), share)
    pairs = pl.ds(pl.multiple_of(2 * core * share, 16), 2 * share)
    ow_line, ow_plane, ow_chip = [], [], []
    for step in range(1, LINE):
        source, i = lax.rem(me + LINE - step, LINE), step - 1
        ow_line.append(
            remote(
                r.o_weight.at[quarter], ow.at[me, quarter], ow_send.at[i], ow_recv.at[i], mp=lax.rem(me + step, LINE)
            )
        )
        held = ow.at[source, quarter]
        ow_plane.append(remote(held, held, ow_send.at[3 + i], ow_recv.at[3 + i], dp=over_x))
        held = ow.at[source, pairs]
        ow_chip.append(remote(held, held, ow_send.at[6 + i], ow_recv.at[6 + i], dp=across))
    for copy in ow_line:
        copy.start()

    need("kind_row", "seg_row")
    kind_wide, seg_wide = r.kind_wide, r.seg_wide
    kind_wide[...] = jnp.broadcast_to(r.kind_row[...], (pair, rows)).T
    seg_wide[...] = jnp.broadcast_to(r.seg_row[...], (pair, rows)).T
    qcat, kcat, vt = r.qcat, r.kcat, r.vt
    need("tokens", "v_weight")
    tok = tokens[...]
    entity = kind_wide[...] == 1
    upper = lax.broadcasted_iota(jnp.int32, (rows, pair), 1) >= HD
    keys = dot(tok, wk[...], 1, 1)
    for h in range(heads):
        both = slice(h * pair, (h + 1) * pair)
        kcat[:, both] = jnp.where(entity == upper, keys[:, both], 0.0).astype(low)
    vt[...] = dot(r.v_weight[...], tok, 1, 1).astype(low)
    q_plain = dot(tok, wa[...], 1, 1)
    q_entity = dot(tok, wb[...], 1, 1)
    for h in range(heads):
        both = slice(h * pair, (h + 1) * pair)
        qcat[:, both] = jnp.where(entity, q_entity[:, both], q_plain[:, both]).astype(low)

    pt, mx, st = r.pt, r.mx, r.st
    scale = HD ** (-0.5)
    gathers = [
        LineGather(at, r.line_send.at[0], r.mx_recv.at[q], lambda block, q=q: mx[q].at[block])
        for q in range(len(spans))
    ]

    def pair_of(h):
        return pl.ds(pl.multiple_of(h * pair, pair), pair)

    def head_of(h):
        return pl.ds(pl.multiple_of(h * HD, HD), HD)

    def attend(q):
        start, size = spans[q]
        here = pl.ds(start, size)

        def head_step(h, carry):
            st[:, :size] = dot(kcat[:, pair_of(h)], qcat[here, pair_of(h)], 1, 1)

            def soften(i, carry):
                cols = pl.ds(pl.multiple_of(i * LANES, LANES), LANES)
                span = pl.ds(pl.multiple_of(start + i * LANES, LANES), LANES)
                scores = jnp.where(seg_wide[...] == r.seg_row[:, span], st[:, cols] * scale, -1000000000.0)
                shifted = jnp.exp(scores - jnp.max(scores, axis=0, keepdims=True))
                total = jnp.sum(shifted, axis=0, keepdims=True)
                pt[h, :, span] = (shifted * (1.0 / total)).astype(low)
                return carry

            lax.fori_loop(0, size // LANES, soften, 0, unroll=True)
            mixed = dot(vt[head_of(h), :], pt[h, :, here]).astype(low)
            mx[q][me, head_of(h), :] = mixed
            return carry

        lax.fori_loop(0, heads, head_step, 0, unroll=True)
        gathers[q].spread()

    def swap_plane():
        ow[me] = r.o_weight[...]
        for copy in ow_line:
            copy.wait_recv()
        for copy in ow_plane:
            copy.start()

    def swap_chip():
        for copy in ow_plane:
            copy.wait_recv()
        for copy in ow_chip:
            copy.start()

    def own_weights():
        for copy in ow_chip:
            copy.wait_recv()
        need("in_weight", "out_weight", "o_bias", "gain1", "shift1", "in_bias", "out_bias", "gain2", "shift2")
        for i, name in enumerate((r.o_bias, r.gain1, r.shift1, r.in_bias, r.out_bias, r.gain2, r.shift2)):
            vec[i, :] = name[...]

    tok_t, kct, vn = r.tok_t, r.kct, r.vn

    def turn():
        tok_t[...] = tokens[...].T
        kct[...] = kcat[...].T
        for h in range(heads):
            vn[h] = vt[h * HD : (h + 1) * HD, :].T

    xh1, rstd1, hl, mnat, mown, gbown = r.xh1, r.rstd1, r.hl, r.mnat, r.mown, r.gbown
    act, gp, dr2, gf, il, tmp, acc = r.act, r.gp, r.dr2, r.gf, r.il, r.tmp, r.acc
    acc[...] = jnp.zeros_like(acc)

    def make_lines(parts, send, part, out):
        lines = []
        for q, (start, size) in enumerate(spans):
            carry, single, summed, recv = parts[q]
            lines.append(LineReduce(at, part, carry, single, summed, send, recv, start, size // LINE, out))
        return lines

    ffn = make_lines(r.ffn, r.line_send.at[1], r.ffn_part, r.ffn_out)
    back = make_lines(r.back, r.line_send.at[2], r.back_part, r.back_part)
    swaps = [LineSwap(at, *parts) for parts in r.swap]
    grad = make_lines(r.grad, r.line_send.at[3], r.grad_part, r.tokens_grad)

    root_half = math.sqrt(0.5)
    density = 1.0 / math.sqrt(2.0 * math.pi)

    def forward(q):
        gathers[q].arrive()
        start, size = spans[q]
        here = pl.ds(start, size)
        mnat[:size, :] = mx[q][...].reshape(LINE * local_width, size).T
        tmp[:size, :] = dot(mnat[:size, :], ow[...].reshape(LINE * local_width, width))
        quarter_rows = size // LINE
        own = pl.ds(pl.multiple_of(me * quarter_rows, 16), quarter_rows)
        mown[start // LINE : (start + size) // LINE, :] = mnat[own, :]

        def first_norm(at_rows, inside):
            value = tmp[inside, :] + tokens[at_rows, :].astype(wide) + o_bias[...]
            centred = value - row_mean(value)
            scaled = lax.rsqrt(row_mean(centred * centred) + norm_epsilon)
            normal = centred * scaled
            xh1[at_rows, :] = normal
            rstd1[at_rows, :] = jnp.broadcast_to(scaled, (CHUNK, 128))
            hl[at_rows, :] = (normal * gain1[...] + shift1[...]).astype(low)

        rows_loop(start, size, first_norm)
        tmp[:size, :] = dot(hl[here, :], r.in_weight[...])

        def activate(at_rows, inside):
            inner = tmp[inside, :] + in_bias[...]
            gate = 0.5 + 0.5 * lax.erf(inner * root_half)
            act[at_rows, :] = (inner * gate).astype(low)
            gp[at_rows, :] = gate + inner * (density * jnp.exp(-0.5 * inner * inner))

        rows_loop(start, size, activate)
        r.ffn_part[here, :] = dot(act[here, :], r.out_weight[...]).astype(low)
        ffn[q].start()

    def backward(q):
        ffn[q].arrive()
        start, size = spans[q]
        here = pl.ds(start, size)

        def second_norm(at_rows, inside):
            value = xh1[at_rows, :] * gain1[...] + shift1[...]
            value = value + r.ffn_out[at_rows, :].astype(wide) + out_bias[...]
            centred = value - row_mean(value)
            scaled = lax.rsqrt(row_mean(centred * centred) + norm_epsilon)
            normal = centred * scaled
            r.layer_out[at_rows, :] = (normal * gain2[...] + shift2[...]).astype(low)
            cot = r.cotangent[at_rows, :].astype(wide)
            acc[6] += fold(cot)
            acc[5] += fold(cot * normal)
            grown = cot * gain2[...]
            grad_in = scaled * (grown - row_mean(grown) - normal * row_mean(grown * normal))
            acc[4] += fold(grad_in)
            dr2[at_rows, :] = grad_in
            gf[at_rows, :] = grad_in.astype(low)

        rows_loop(start, size, second_norm)
        tmp[:size, :] = dot(gf[here, :], r.out_weight[...], 1, 1)

        def inner_step(at_rows, inside):
            d_inner = tmp[inside, :] * gp[at_rows, :]
            acc[3] += fold(d_inner)
            il[at_rows, :] = d_inner.astype(low)

        rows_loop(start, size, inner_step)
        r.back_part[here, :] = dot(il[here, :], r.in_weight[...], 1, 1).astype(low)
        back[q].start()

    dqa, dqb, dkv, dk_sum, dv_sum = r.dqa, r.dqb, r.dkv, r.dk_sum, r.dv_sum
    dmt, ds = r.dmt, r.ds

    def settle_back(q):
        start, size = spans[q]
        own = back[q].rows_of(me)
        d_hidden = dr2[own, :] + back[q].total()
        normal = xh1[own, :]
        acc[2] += fold(d_hidden)
        acc[1] += fold(d_hidden * normal)
        grown = d_hidden * gain1[...]
        grad_in = rstd1[own, 0:1] * (grown - row_mean(grown) - normal * row_mean(grown * normal))
        acc[0] += fold(grad_in)
        dr2[own, :] = grad_in
        grad_low = grad_in.astype(low)
        gbown[start // LINE : (start + size) // LINE, :] = grad_low
        for j in range(LINE):
            swaps[q].sent[j] = dot(grad_low, ow[j], 1, 1).astype(low)
        swaps[q].start()

    def finish_rows(q):
        swaps[q].wait()
        start, size = spans[q]
        here = pl.ds(start, size)
        for h in range(heads):
            dmt[h, :size, :] = swaps[q].got[:, :, h * HD : (h + 1) * HD].reshape(size, HD)

        def head_step(h, carry):
            d_mixed = dmt[h, :size, :]
            st[:, :size] = dot(vn[h], d_mixed, 1, 1)

            def harden(i, carry):
                cols = pl.ds(pl.multiple_of(i * LANES, LANES), LANES)
                span = pl.ds(pl.multiple_of(start + i * LANES, LANES), LANES)
                prob = pt[h, :, span].astype(wide)
                d_prob = st[:, cols]
                delta = jnp.sum(prob * d_prob, axis=0, keepdims=True)
                ds[:, cols] = (prob * (d_prob - delta) * scale).astype(low)
                return carry

            lax.fori_loop(0, size // LANES, harden, 0, unroll=True)
            d_score = ds[:, :size]
            d_value = dot(pt[h, :, here], d_mixed)
            d_key = dot(d_score, qcat[here, pair_of(h)])
            if q == 0:
                dv_sum[h] = d_value
                dk_sum[h] = d_key
            else:
                dv_sum[h] += d_value
                dk_sum[h] += d_key
            d_query = dot(kct[pair_of(h), :], d_score).T
            row_entity = kind_wide[here, :] == 1
            dqa[here, pair_of(h)] = jnp.where(row_entity, 0.0, d_query).astype(low)
            dqb[here, pair_of(h)] = jnp.where(row_entity, d_query, 0.0).astype(low)
            return carry

        lax.fori_loop(0, heads, head_step, 0, unroll=True)

    gfeed, gattn = r.gfeed, r.gattn
    blocks, per_block = gfeed.shape[0], gfeed.shape[1]

    def put_grad(packed, start, value):
        packed[:, :, start : start + value.shape[1]] = value.astype(low).reshape(blocks, per_block, value.shape[1])

    if planar:
        feed = PlaneReduce(gfeed, *r.feed)
        attn = PlaneReduce(gattn, *r.attn)

    small = r.small
    if planar:
        small_sum = r.small_sum
        tiny = [
            remote(
                small if s == 0 else small_sum.at[s - 1],
                r.small_in.at[s],
                r.small_send.at[s],
                r.small_recv.at[s],
                dp=(across, over_x, over_y)[s],
            )
            for s in range(3)
        ]

    def tiny_step(s):
        if planar:
            tiny[s].wait_recv()
            small_sum[s] = (small if s == 0 else small_sum.at[s - 1])[...] + r.small_in[s]
            if s < 2:
                tiny[s + 1].start()

    norms = LineSwap(at, *r.norms)
    if planar:
        o_swap = LineSwap(at, *r.o_swap)

    def feed_step(i):
        if i == 0:
            put_grad(gfeed, hidden_width, dot(gf[...], act[...], 0, 0))
        elif i == 1:
            put_grad(gfeed, 0, dot(hl[...], il[...], 0, 0))
        elif planar and i == 2:
            feed.start()
        elif planar and i == 3:
            feed.step_one()
        elif planar and i == 4:
            feed.step_two()
        elif planar and i == 5:
            feed_sum = feed.finish()
            r.in_grad[...] = feed_sum[:, :hidden_width]
            r.out_grad[...] = feed_sum[:, hidden_width : 2 * hidden_width]
            for j in range(LINE):
                begin = 2 * hidden_width + j * local_width
                o_swap.sent[j] = feed_sum[:, begin : begin + local_width].astype(low)
            o_swap.start()
            stores["in_grad"].start()
            stores["out_grad"].start()

    def share_norms():
        for i in range(8):
            norms.sent[0, i : i + 1, :] = jnp.sum(acc[i], axis=0, keepdims=True)
        for j in range(1, LINE):
            norms.sent[j] = norms.sent[0]
        norms.start()
        put_grad(gfeed, 2 * hidden_width, dot(gbown[...], mown[...], 0, 0))

    def key_grads():
        norms.wait()
        small[...] = norms.sent[0]
        small[0:3, :] = norms.got[0, 0:3] + norms.got[1, 0:3] + norms.got[2, 0:3] + norms.got[3, 0:3]
        if planar:
            tiny[0].start()
        d_keys = [
            jnp.where(kind_wide[:, :HD] == 1, dk_sum[h, :, HD:], dk_sum[h, :, :HD]).astype(low)
            for h in range(heads)
        ]
        d_values = [dv_sum[h].astype(low) for h in range(heads)]
        dkv[...] = jnp.concatenate(d_keys + d_values, axis=1)

    def input_share(q):
        start, size = spans[q]
        here = pl.ds(start, size)
        share = dot(dqa[here, :], wa[...]) + dot(dqb[here, :], wb[...])
        share = share + dot(dkv[here, :local_width], r.k_weight[...]) + dot(dkv[here, local_width:], r.v_weight[...])
        r.grad_part[here, :] = share.astype(low)
        grad[q].start()

    def attn_step(i):
        if i == 0:
            put_grad(gattn, 0, dot(tok_t[...], dqa[...]))
            put_grad(gattn, 2 * local_width, dot(tok_t[...], dqb[...]))
        elif i == 1:
            put_grad(gattn, 4 * local_width, dot(tok_t[...], dkv[...]))
        elif planar and i == 2:
            attn.start()
            tiny_step(0)
        elif planar and i == 3:
            attn.step_one()
            tiny_step(1)
        elif planar and i == 4:
            attn.step_two()
            tiny_step(2)

    attend(0)
    attend(1)
    attend(2)
    attend(3)
    gathers[0].relay(0)
    swap_plane()
    gathers[0].relay(1)
    attend(4)
    gathers[3].relay(0)
    gathers[2].relay(0)
    gathers[3].relay(1)
    gathers[4].relay(0)
    gathers[0].relay(2)
    gathers[1].relay(0)
    gathers[3].relay(2)
    gathers[2].relay(1)
    gathers[1].relay(1)
    gathers[4].relay(1)
    turn()
    swap_chip()
    own_weights()
    gathers[1].relay(2)
    forward(0)
    ffn[0].forward(0)
    gathers[2].relay(2)
    forward(3)
    gathers[4].relay(2)
    ffn[0].forward(1)
    ffn[3].forward(0)
    forward(1)
    ffn[3].forward(1)
    ffn[0].settle()
    ffn[1].forward(0)
    forward(2)
    ffn[1].forward(1)
    ffn[0].relay(0)
    ffn[2].forward(0)
    ffn[3].settle()
    ffn[2].forward(1)
    ffn[0].relay(1)
    forward(4)
    ffn[3].relay(0)
    ffn[4].forward(0)
    ffn[0].relay(2)
    ffn[4].forward(1)
    ffn[1].settle()
    ffn[2].settle()
    ffn[3].relay(1)
    ffn[3].relay(2)
    ffn[1].relay(0)
    ffn[2].relay(0)
    ffn[1].relay(1)
    ffn[4].settle()
    ffn[4].relay(0)
    ffn[1].relay(2)
    ffn[2].relay(1)
    need("cotangent")
    backward(0)
    ffn[2].relay(2)
    ffn[4].relay(1)
    backward(3)
    back[0].forward(0)
    back[0].forward(1)
    ffn[4].relay(2)
    backward(1)
    back[3].forward(0)
    backward(2)
    back[1].forward(0)
    settle_back(0)
    back[2].forward(0)
    back[1].forward(1)
    back[3].forward(1)
    backward(4)
    stores["layer_out"].start()
    back[2].forward(1)
    feed_step(0)
    back[4].forward(0)
    settle_back(1)
    back[4].forward(1)
    feed_step(1)
    settle_back(2)
    settle_back(3)
    finish_rows(0)
    settle_back(4)
    share_norms()
    feed_step(2)
    finish_rows(1)
    finish_rows(2)
    finish_rows(3)
    finish_rows(4)
    key_grads()
    input_share(0)
    feed_step(3)
    input_share(1)
    input_share(2)
    grad[0].forward(0)
    input_share(3)
    input_share(4)
    grad[0].forward(1)
    attn_step(0)
    grad[1].forward(0)
    grad[1].forward(1)
    attn_step(1)
    grad[2].forward(0)
    grad[2].forward(1)
    attn_step(2)
    grad[3].forward(0)
    grad[3].forward(1)
    grad[2].settle(dr2)
    grad[4].forward(0)
    grad[0].settle(dr2)
    feed_step(4)
    grad[4].forward(1)
    attn_step(3)
    grad[3].settle(dr2)
    grad[2].relay(0)
    grad[2].relay(1)
    grad[1].settle(dr2)
    grad[0].relay(0)
    grad[0].relay(1)
    grad[4].settle(dr2)
    grad[1].relay(0)
    grad[3].relay(0)
    grad[3].relay(1)
    grad[2].relay(2)
    grad[4].relay(0)
    grad[1].relay(1)
    feed_step(5)
    grad[4].relay(1)
    attn_step(4)
    grad[1].relay(2)
    grad[3].relay(2)
    grad[4].relay(2)
    grad[0].relay(2)
    if planar:
        attn_sum = attn.finish()
        for part in range(4):
            base = (part // 2) * 2 * local_width + (part % 2) * HD
            r.q_grad[part] = jnp.concatenate(
                [attn_sum[:, base + h * pair : base + h * pair + HD] for h in range(heads)], axis=1
            )
        both_grads = attn_sum[:, 4 * local_width : 6 * local_width]
        r.k_grad[...] = both_grads[:, :local_width]
        r.v_grad[...] = both_grads[:, local_width:]
        o_swap.wait()
        o_sum = o_swap.got[0].astype(wide) + o_swap.got[1].astype(wide)
        r.o_grad[...] = (o_sum + o_swap.got[2].astype(wide) + o_swap.got[3].astype(wide)).T
        o_swap.drain()
        r.small_out[...] = small_sum[2]
        for name in ("q_grad", "k_grad", "v_grad", "o_grad", "small_out"):
            stores[name].start()
    else:
        r.small_out[...] = small[...]
        r.feed_out[...] = gfeed[...]
        r.attn_out[...] = gattn[...]
        for name in ("small_out", "feed_out", "attn_out"):
            stores[name].start()
    for line in grad:
        line.arrive()
    stores["tokens_grad"].start()

    def sent_all(i, held):
        remote(held, held, r.line_send.at[i], r.mx_recv.at[0, 0], mp=at.mid).wait_send()

    blocks_out = rows // LINE * 3

    @pl.when(at.is_end)
    def _():
        sent_all(0, vt)
        sent_all(1, hl)
        sent_all(2, hl.at[:blocks_out])
        sent_all(3, hl)

    @pl.when(at.is_mid)
    def _():
        sent_all(0, xh1.at[: 5 * rows * local_width // (2 * width)])
        sent_all(1, xh1)
        sent_all(2, hl.at[:blocks_out])
        sent_all(3, xh1)

    for swap in swaps + [norms]:
        swap.drain()
    for copy in ow_line + ow_plane + ow_chip:
        copy.wait_send()
    if planar:
        for copy in tiny:
            copy.wait_send()
    for copy in stores.values():
        copy.wait()


def hand_on(layout, *refs):
    sources, targets, held, lines, sems = jax.tree.unflatten(layout, refs)
    count = len(sources) - 1
    small = held[0]
    fetch = [pltpu.make_async_copy(source, kept, sems.at[0, i]) for i, (source, kept) in enumerate(zip(sources, held))]
    store = [
        pltpu.make_async_copy(kept, target, sems.at[1, i])
        for i, (kept, target) in enumerate(zip(list(held[1:]) + list(lines), targets))
    ]
    for copy in fetch:
        copy.start()
    fetch[0].wait()
    for i, line in enumerate(lines):
        line[...] = small[i, :]
        store[count + i].start()
    for i in range(count):
        fetch[1 + i].wait()
        store[i].start()
    for copy in store:
        copy.wait()


def local(
    tokens,
    segment_ids,
    token_types,
    q_weight,
    k_weight,
    v_weight,
    o_weight,
    o_bias,
    norm1_gain,
    norm1_shift,
    in_weight,
    in_bias,
    out_weight,
    out_bias,
    norm2_gain,
    norm2_shift,
    cotangent,
):
    rows, width = tokens.shape
    local_width = k_weight.shape[1]
    heads = local_width // HD
    hidden_width = in_weight.shape[1]
    n_dp = lax.axis_size("dp")
    planar = n_dp == 8
    blocks = 8
    per_block = width // blocks
    spans = portions_of(rows)
    largest = max(size for _, size in spans)
    low, wide = jnp.bfloat16, jnp.float32
    attn_width = 6 * local_width
    feed_width = 2 * hidden_width + LINE * local_width
    args = dict(
        tokens=tokens,
        seg_row=segment_ids,
        kind_row=token_types,
        q_weight=q_weight.swapaxes(1, 2),
        k_weight=k_weight.T,
        v_weight=v_weight.T,
        o_weight=o_weight,
        o_bias=o_bias,
        gain1=norm1_gain,
        shift1=norm1_shift,
        in_bias=in_bias,
        out_bias=out_bias,
        gain2=norm2_gain,
        shift2=norm2_shift,
        in_weight=in_weight,
        out_weight=out_weight,
        cotangent=cotangent,
    )
    shaped = jax.ShapeDtypeStruct
    outs = dict(
        layer_out=shaped((rows, width), low),
        tokens_grad=shaped((rows, width), low),
        small_out=shaped((8, width), wide),
    )
    if planar:
        outs |= dict(
            q_grad=shaped((4, per_block, local_width), wide),
            k_grad=shaped((per_block, local_width), wide),
            v_grad=shaped((per_block, local_width), wide),
            o_grad=shaped((local_width, per_block), wide),
            in_grad=shaped((per_block, hidden_width), wide),
            out_grad=shaped((per_block, hidden_width), wide),
        )
    else:
        outs |= dict(
            feed_out=shaped((blocks, per_block, feed_width), low),
            attn_out=shaped((blocks, per_block, attn_width), low),
        )
    dma = pltpu.SemaphoreType.DMA
    scratch = dict(
        ow=pltpu.VMEM((LINE, local_width, width), low),
        ow_send=dma((9,)),
        ow_recv=dma((9,)),
        wa=pltpu.VMEM((2 * local_width, width), low),
        wb=pltpu.VMEM((2 * local_width, width), low),
        wk=pltpu.VMEM((2 * local_width, width), low),
        kind_wide=pltpu.VMEM((rows, 2 * HD), jnp.int32),
        seg_wide=pltpu.VMEM((rows, 2 * HD), jnp.int32),
        qcat=pltpu.VMEM((rows, 2 * local_width), low),
        kcat=pltpu.VMEM((rows, 2 * local_width), low),
        vt=pltpu.VMEM((local_width, rows), low),
        pt=pltpu.VMEM((heads, rows, rows), low),
        mx=[pltpu.VMEM((LINE, local_width, size), low) for _, size in spans],
        st=pltpu.VMEM((rows, largest), wide),
        ds=pltpu.VMEM((rows, largest), low),
        line_send=dma((4,)),
        mx_recv=dma((len(spans), LINE)),
        tok_t=pltpu.VMEM((width, rows), low),
        xh1=pltpu.VMEM((rows, width), wide),
        rstd1=pltpu.VMEM((rows, 128), wide),
        hl=pltpu.VMEM((rows, width), low),
        act=pltpu.VMEM((rows, hidden_width), low),
        gp=pltpu.VMEM((rows, hidden_width), wide),
        dr2=pltpu.VMEM((rows, width), wide),
        gf=pltpu.VMEM((rows, width), low),
        il=pltpu.VMEM((rows, hidden_width), low),
        tmp=pltpu.VMEM((largest, width), wide),
        vec=pltpu.VMEM((8, width), wide),
        acc=pltpu.VMEM((8, 8, width), wide),
        mnat=pltpu.VMEM((largest, LINE * local_width), low),
        mown=pltpu.VMEM((rows // LINE, LINE * local_width), low),
        gbown=pltpu.VMEM((rows // LINE, width), low),
        swap=[swap_scratch(size // LINE, local_width, low) for _, size in spans],
        norms=swap_scratch(8, width, wide),
        ffn_part=pltpu.VMEM((rows, width), low),
        back_part=pltpu.VMEM((rows, width), low),
        grad_part=pltpu.VMEM((rows, width), low),
        ffn_out=pltpu.VMEM((rows, width), low),
        gfeed=pltpu.VMEM((blocks, per_block, feed_width), low),
        gattn=pltpu.VMEM((blocks, per_block, attn_width), low),
        small=pltpu.VMEM((8, width), wide),
        kct=pltpu.VMEM((2 * local_width, rows), low),
        vn=pltpu.VMEM((heads, rows, HD), low),
        dmt=pltpu.VMEM((heads, largest, HD), low),
        dk_sum=pltpu.VMEM((heads, rows, 2 * HD), wide),
        dv_sum=pltpu.VMEM((heads, rows, HD), wide),
        dqa=pltpu.VMEM((rows, 2 * local_width), low),
        dqb=pltpu.VMEM((rows, 2 * local_width), low),
        dkv=pltpu.VMEM((rows, 2 * local_width), low),
    )
    for name in ("ffn", "back", "grad"):
        scratch[name] = [line_scratch(size // LINE, width) for _, size in spans]
    if planar:
        scratch |= dict(
            feed=plane_scratch(per_block, feed_width),
            o_swap=swap_scratch(per_block, local_width, low),
            attn=plane_scratch(per_block, attn_width),
            small_in=pltpu.VMEM((3, 8, width), wide),
            small_sum=pltpu.VMEM((3, 8, width), wide),
            small_send=dma((3,)),
            small_recv=dma((3,)),
        )
    scratch |= dict(
        held={name: pltpu.VMEM(a.shape, a.dtype) for name, a in args.items()},
        made={name: pltpu.VMEM(a.shape, a.dtype) for name, a in outs.items()},
        load_sem=dma((len(args),)),
        store_sem=dma((len(outs),)),
    )
    layout = jax.tree.structure((args, outs, scratch))
    vm, far = pl.BlockSpec(memory_space=pltpu.VMEM), pl.BlockSpec(memory_space=pl.ANY)
    results = pl.pallas_call(
        functools.partial(layer_kernel, planar, layout),
        out_shape=jax.tree.leaves(outs),
        in_specs=[far] * len(args),
        out_specs=[far] * len(outs),
        scratch_shapes=jax.tree.leaves(scratch),
        compiler_params=pltpu.CompilerParams(
            collective_id=0, has_side_effects=True, vmem_limit_bytes=VMEM_LIMIT
        ),
    )(*jax.tree.leaves(args))
    results = dict(zip(sorted(outs), results))
    if planar:
        small = results.pop("small_out")
        flat, tree = jax.tree.flatten(results)
        vectors = small.shape[0] - 1
        line = (width,)
        targets = [shaped(a.shape, a.dtype) for a in flat] + [shaped(line, wide)] * vectors
        held = [pltpu.VMEM(a.shape, a.dtype) for a in [small] + flat]
        lines = [pltpu.VMEM(line, wide)] * vectors
        sems = dma((2, len(targets)))
        pieces = ([small] + flat, targets, held, lines, sems)
        flat = pl.pallas_call(
            functools.partial(hand_on, jax.tree.structure(pieces)),
            out_shape=targets,
            in_specs=[far] * (1 + len(flat)),
            out_specs=[far] * len(targets),
            scratch_shapes=held + lines + [sems],
            compiler_params=pltpu.CompilerParams(vmem_limit_bytes=VMEM_LIMIT),
        )(small, *flat)
        small = flat[len(results) :]
        results = jax.tree.unflatten(tree, flat[: len(results)])
    res = types.SimpleNamespace(**results)
    if planar:
        grads = (res.q_grad, res.k_grad, res.v_grad, res.o_grad, res.in_grad, res.out_grad.T)
    else:
        feed = res.feed_out.astype(wide).reshape(width, feed_width)
        attn = res.attn_out.astype(wide).reshape(width, attn_width)
        feed = lax.psum_scatter(feed, "dp", scatter_dimension=0, tiled=True)
        attn = lax.psum_scatter(attn, "dp", scatter_dimension=0, tiled=True)
        small = lax.psum(res.small_out, "dp")
        per = feed.shape[0]
        o_part = lax.psum_scatter(feed[:, 2 * hidden_width :], "mp", scatter_dimension=1, tiled=True)
        queries = attn[:, : 4 * local_width].reshape(per, 2, heads, 2, HD)
        queries = queries.transpose(1, 3, 0, 2, 4).reshape(4, per, local_width)
        grads = (
            queries,
            attn[:, 4 * local_width : 5 * local_width],
            attn[:, 5 * local_width : 6 * local_width],
            o_part.T,
            feed[:, :hidden_width],
            feed[:, hidden_width : 2 * hidden_width].T,
        )
    d_q, d_k, d_v, d_o, d_in, d_out = grads
    return (
        res.layer_out,
        res.tokens_grad,
        d_q,
        d_k,
        d_v,
        d_o,
        small[0],
        small[1],
        small[2],
        d_in,
        small[3],
        d_out,
        small[4],
        small[5],
        small[6],
    )


def solution(mesh):
    return jax.shard_map(
        local,
        mesh=mesh,
        in_specs=(
            P("dp", None),
            P("dp", None),
            P("dp", None),
            P(None, None, "mp"),
            P(None, "mp"),
            P(None, "mp"),
            P("mp", None),
            P(),
            P(),
            P(),
            P(None, "mp"),
            P("mp"),
            P("mp", None),
            P(),
            P(),
            P(),
            P("dp", None),
        ),
        out_specs=(
            P("dp", None),
            P("dp", None),
            P(None, "dp", "mp"),
            P("dp", "mp"),
            P("dp", "mp"),
            P("mp", "dp"),
            P(),
            P(),
            P(),
            P("dp", "mp"),
            P("mp"),
            P("mp", "dp"),
            P(),
            P(),
            P(),
        ),
        check_vma=False,
    )
```

```python
import functools
import math
import operator
import types

import jax
import jax.numpy as jnp
from jax import lax
from jax.experimental import pallas as pl
from jax.experimental.pallas import tpu as pltpu
from jax.sharding import PartitionSpec as P

HD = 64
LINE = 4
PORTIONS = (1, 1, 1, 1, 1)
LANES = 128
CHUNK = 32
VMEM_LIMIT = 67043328

norm_epsilon = 1e-05


def remote(src, dst, send_sem, recv_sem, **axes):
    return pltpu.make_async_remote_copy(
        src_ref=src,
        dst_ref=dst,
        send_sem=send_sem,
        recv_sem=recv_sem,
        device_id=axes,
        device_id_type=pl.DeviceIdType.MESH,
    )


class Place:
    def __init__(self):
        me = lax.axis_index("mp")
        self.me = me
        self.is_mid = jnp.logical_or(me == 1, me == 2)
        self.is_end = jnp.logical_not(self.is_mid)
        left = me < 2
        self.mid = jnp.where(left, 1, 2)
        self.end = jnp.where(left, 0, 3)
        self.far_mid = 3 - self.mid
        self.far_end = 3 - self.end


class LineGather:
    def __init__(self, place, send, recv, out):
        self.at, self.send, self.recv, self.out = place, send, recv, out

    def copy(self, block, slot, target):
        return remote(self.out(block), self.out(block), self.send, self.recv.at[block], mp=target)

    def spread(self):
        at = self.at

        @pl.when(at.is_end)
        def _():
            self.copy(at.me, 0, at.mid).start()

        @pl.when(at.is_mid)
        def _():
            self.copy(at.me, 0, at.end).start()
            self.copy(at.me, 1, at.far_mid).start()

    def relay(self, step):
        at = self.at
        block = (at.end, at.far_mid, at.far_end)[step]
        target = (at.far_mid, at.end, at.end)[step]

        @pl.when(at.is_mid)
        def _():
            self.copy(block, 2 + step, target).wait_recv()
            self.copy(block, 2 + step, target).start()

    def arrive(self):
        at = self.at

        @pl.when(at.is_end)
        def _():
            self.copy(at.mid, 0, at.mid).wait_recv()
            self.copy(at.far_mid, 0, at.mid).wait_recv()
            self.copy(at.far_end, 0, at.mid).wait_recv()


class LineReduce:
    def __init__(self, place, part, carry, single, summed, send, recv, start, block_rows, out):
        self.at, self.carry, self.single, self.summed = place, carry, single, summed
        self.send, self.recv = send, recv

        def rows_of(block):
            return pl.ds(pl.multiple_of(start + block * block_rows, 16), block_rows)

        self.rows_of, self.part_ref, self.out_ref = rows_of, part, out
        self.gather = LineGather(place, send, recv.at[1], lambda block: out.at[rows_of(block)])

    def part(self, block):
        return self.part_ref.at[self.rows_of(block)]

    def end_sends(self):
        at, send, recv = self.at, self.send, self.recv
        return (
            remote(self.part(at.far_end), self.carry.at[0], send, recv.at[0, 2], mp=at.mid),
            remote(self.part(at.far_mid), self.carry.at[1], send, recv.at[0, 3], mp=at.mid),
            remote(self.part(at.mid), self.single, send, recv.at[0, 0], mp=at.mid),
        )

    def mid_sends(self):
        at, send, recv = self.at, self.send, self.recv
        return (
            remote(self.carry.at[0], self.summed, send, recv.at[0, 1], mp=at.far_end),
            remote(self.carry.at[1], self.summed, send, recv.at[0, 1], mp=at.far_mid),
            remote(self.part(at.end), self.single, send, recv.at[0, 0], mp=at.end),
        )

    def start(self):
        @pl.when(self.at.is_end)
        def _():
            for copy in self.end_sends():
                copy.start()

        @pl.when(self.at.is_mid)
        def _():
            self.mid_sends()[2].start()

    def forward(self, step):
        at = self.at

        @pl.when(at.is_mid)
        def _():
            block = (at.far_end, at.far_mid)[step]
            self.end_sends()[step].wait_recv()
            total = self.carry[step].astype(jnp.float32) + self.part(block)[...].astype(jnp.float32)
            self.carry[step] = total.astype(jnp.bfloat16)
            self.mid_sends()[step].start()

    def total(self):
        self.end_sends()[2].wait_recv()
        self.mid_sends()[0].wait_recv()
        return (
            self.part(self.at.me)[...].astype(jnp.float32)
            + self.single[...].astype(jnp.float32)
            + self.summed[...].astype(jnp.float32)
        )

    def settle(self, extra=None):
        at = self.at
        total = self.total()
        if extra is not None:
            total = total + extra[self.rows_of(at.me), :]
        self.out_ref[self.rows_of(at.me), :] = total.astype(jnp.bfloat16)
        self.gather.spread()

    def relay(self, step):
        self.gather.relay(step)

    def arrive(self):
        self.gather.arrive()


class LineSwap:
    def __init__(self, place, sent, got, send, recv):
        me = place.me
        self.me, self.sent, self.got = me, sent, got
        targets = [lax.rem(me + step, LINE) for step in range(1, LINE)]
        self.outward = [
            remote(sent.at[j], got.at[me], send.at[i], recv.at[me], mp=j) for i, j in enumerate(targets)
        ]
        self.inward = [remote(got.at[j], got.at[j], send.at[i], recv.at[j], mp=j) for i, j in enumerate(targets)]

    def start(self):
        for copy in self.outward:
            copy.start()
        self.got[self.me] = self.sent[self.me]

    def wait(self):
        for copy in self.inward:
            copy.wait_recv()

    def drain(self):
        for copy in self.outward:
            copy.wait_send()


def swap_scratch(rows, width, kind):
    return [
        pltpu.VMEM((LINE, rows, width), kind),
        pltpu.VMEM((LINE, rows, width), kind),
        pltpu.SemaphoreType.DMA((LINE - 1,)),
        pltpu.SemaphoreType.DMA((LINE,)),
    ]


def line_scratch(rows, width):
    return [
        pltpu.VMEM((2, rows, width), jnp.bfloat16),
        pltpu.VMEM((rows, width), jnp.bfloat16),
        pltpu.VMEM((rows, width), jnp.bfloat16),
        pltpu.SemaphoreType.DMA((2, 4)),
    ]


class PlaneReduce:
    def __init__(self, grads, r1, sums, mid2, r2a, r2b, s3a, s3b, r3a, r3b, send, recv):
        self.grads, self.r1, self.sums, self.mid2 = grads, r1, sums, mid2
        self.r2a, self.r2b, self.s3a, self.s3b, self.r3a, self.r3b = r2a, r2b, s3a, s3b, r3a, r3b
        dp = lax.axis_index("dp")
        self.core, self.x, self.y = lax.rem(dp, 2), lax.rem(dp // 2, 2), dp // 4
        across = dp + 1 - 2 * self.core
        over_x = dp + 2 - 4 * self.x
        over_y = dp + 4 - 8 * self.y
        half = r2a.shape[2]
        self.low, self.high = pl.ds(0, half), pl.ds(half, grads.shape[2] - half)
        self.first = [
            remote(grads.at[2 * k + 1 - self.core], r1.at[k], send.at[k], recv.at[k], dp=across) for k in range(4)
        ]
        self.second = [
            remote(mid2.at[2 * j + 1 - self.x, :, self.low], r2a.at[j], send.at[4 + j], recv.at[4 + j], dp=over_x)
            for j in range(2)
        ] + [
            remote(mid2.at[2 * (1 - self.y) + j, :, self.high], r2b.at[j], send.at[6 + j], recv.at[6 + j], dp=over_y)
            for j in range(2)
        ]
        self.third = [
            remote(s3a, r3a, send.at[8], recv.at[8], dp=over_y),
            remote(s3b, r3b, send.at[9], recv.at[9], dp=over_x),
        ]

    def start(self):
        for copy in self.first:
            copy.start()

    def step_one(self):
        for copy in self.first:
            copy.wait_recv()

        def body(k, carry):
            total = self.grads[2 * k + self.core].astype(jnp.float32) + self.r1[k].astype(jnp.float32)
            self.sums[k] = total
            self.mid2[k] = total.astype(jnp.bfloat16)
            return carry

        lax.fori_loop(0, 4, body, 0)
        for copy in self.second:
            copy.start()

    def step_two(self):
        for copy in self.second:
            copy.wait_recv()
        x, y = self.x, self.y
        self.s3a[...] = (
            self.sums[2 * (1 - y) + x, :, self.low] + self.r2a[1 - y].astype(jnp.float32)
        ).astype(jnp.bfloat16)
        self.third[0].start()
        self.s3b[...] = (
            self.sums[2 * y + 1 - x, :, self.high] + self.r2b[1 - x].astype(jnp.float32)
        ).astype(jnp.bfloat16)
        self.third[1].start()

    def finish(self):
        x, y = self.x, self.y
        for copy in self.third:
            copy.wait_recv()
        own = self.sums.at[2 * y + x]
        own[:, self.low] = own[:, self.low] + self.r2a[y].astype(jnp.float32) + self.r3a[...].astype(jnp.float32)
        own[:, self.high] = own[:, self.high] + self.r2b[x].astype(jnp.float32) + self.r3b[...].astype(jnp.float32)
        for copy in self.first + self.second + self.third:
            copy.wait_send()
        return own


def plane_scratch(rows, width):
    half = (width // 128 + 1) // 2 * 128
    rest = width - half
    low = jnp.bfloat16
    return [
        pltpu.VMEM((4, rows, width), low),
        pltpu.VMEM((4, rows, width), jnp.float32),
        pltpu.VMEM((4, rows, width), low),
        pltpu.VMEM((2, rows, half), low),
        pltpu.VMEM((2, rows, rest), low),
        pltpu.VMEM((rows, half), low),
        pltpu.VMEM((rows, rest), low),
        pltpu.VMEM((rows, half), low),
        pltpu.VMEM((rows, rest), low),
        pltpu.SemaphoreType.DMA((10,)),
        pltpu.SemaphoreType.DMA((10,)),
    ]


def dot(left, right, left_dim=1, right_dim=0):
    return lax.dot_general(
        left, right, (((left_dim,), (right_dim,)), ((), ())), preferred_element_type=jnp.float32
    )


def rows_loop(start, count, body):
    def step(i, carry):
        inside = pl.ds(pl.multiple_of(i * CHUNK, CHUNK), CHUNK)
        body(pl.ds(pl.multiple_of(start + i * CHUNK, CHUNK), CHUNK), inside)
        return carry

    lax.fori_loop(0, count // CHUNK, step, 0, unroll=True)


def fold(value):
    return jnp.sum(value.reshape(value.shape[0] // 8, 8, value.shape[1]), axis=0)


def row_mean(value):
    return jnp.mean(value, axis=-1, keepdims=True)


def portions_of(rows):
    unit = rows // sum(PORTIONS)
    return [(unit * sum(PORTIONS[:i]), unit * size) for i, size in enumerate(PORTIONS)]


def layer_kernel(planar, layout, *refs):
    given, wanted, scratch = jax.tree.unflatten(layout, refs)
    r = types.SimpleNamespace(**scratch, **scratch["held"], **scratch["made"])
    loads = {
        name: pltpu.make_async_copy(given[name], r.held[name], r.load_sem.at[i]) for i, name in enumerate(given)
    }
    stores = {
        name: pltpu.make_async_copy(r.made[name], wanted[name], r.store_sem.at[i]) for i, name in enumerate(wanted)
    }

    def need(*names):
        for name in names:
            loads[name].wait()

    tokens, rows, width = r.tokens, r.tokens.shape[0], r.tokens.shape[1]
    local_width = r.k_weight.shape[0]
    heads = local_width // HD
    pair = 2 * HD
    hidden_width = r.in_weight.shape[1]
    spans = portions_of(rows)
    low, wide = jnp.bfloat16, jnp.float32
    at = Place()
    me = at.me
    dp = lax.axis_index("dp")
    core = lax.rem(dp, 2)
    across = dp + 1 - 2 * core

    barrier = pltpu.get_barrier_semaphore()
    near = lax.rem(dp // 2, 2)
    over_x = dp + 2 - 4 * near
    peers = [{"mp": lax.rem(me + step, LINE)} for step in range(1, LINE)] + [{"dp": across}, {"dp": over_x}]
    if planar:
        over_y = dp + 4 - 8 * (dp // 4)
        peers += [{"dp": over_y}]
    for peer in peers:
        pl.semaphore_signal(barrier, inc=1, device_id=peer, device_id_type=pl.DeviceIdType.MESH)

    first = ("k_weight", "tokens", "kind_row", "seg_row", "v_weight", "q_weight", "o_weight")
    for name in first + tuple(name for name in loads if name not in first):
        loads[name].start()

    wa, wb, wk = r.wa, r.wb, r.wk
    need("k_weight", "q_weight")
    for h in range(heads):
        cols = slice(h * HD, (h + 1) * HD)
        both = slice(h * pair, (h + 1) * pair)
        wa[both, :] = jnp.concatenate([r.q_weight[0, cols, :], r.q_weight[1, cols, :]], axis=0)
        wb[both, :] = jnp.concatenate([r.q_weight[2, cols, :], r.q_weight[3, cols, :]], axis=0)
        key_part = r.k_weight[cols, :]
        wk[both, :] = jnp.concatenate([key_part, key_part], axis=0)
    need("o_weight")
    pl.semaphore_wait(barrier, len(peers))

    ow, ow_send, ow_recv = r.ow, r.ow_send, r.ow_recv
    vec = r.vec
    o_bias, gain1, shift1, in_bias, out_bias, gain2, shift2 = (vec.at[i : i + 1] for i in range(7))
    share = local_width // 4
    quarter = pl.ds(pl.multiple_of((2 * core + near) * share, 16), share)
    pairs = pl.ds(pl.multiple_of(2 * core * share, 16), 2 * share)
    ow_line, ow_plane, ow_chip = [], [], []
    for step in range(1, LINE):
        source, i = lax.rem(me + LINE - step, LINE), step - 1
        ow_line.append(
            remote(
                r.o_weight.at[quarter], ow.at[me, quarter], ow_send.at[i], ow_recv.at[i], mp=lax.rem(me + step, LINE)
            )
        )
        held = ow.at[source, quarter]
        ow_plane.append(remote(held, held, ow_send.at[3 + i], ow_recv.at[3 + i], dp=over_x))
        held = ow.at[source, pairs]
        ow_chip.append(remote(held, held, ow_send.at[6 + i], ow_recv.at[6 + i], dp=across))
    for copy in ow_line:
        copy.start()

    need("kind_row", "seg_row")
    kind_wide, seg_wide = r.kind_wide, r.seg_wide
    kind_wide[...] = jnp.broadcast_to(r.kind_row[...], (pair, rows)).T
    seg_wide[...] = jnp.broadcast_to(r.seg_row[...], (pair, rows)).T
    qcat, kcat, vt = r.qcat, r.kcat, r.vt
    need("tokens", "v_weight")
    tok = tokens[...]
    entity = kind_wide[...] == 1
    upper = lax.broadcasted_iota(jnp.int32, (rows, pair), 1) >= HD
    keys = dot(tok, wk[...], 1, 1)
    for h in range(heads):
        both = slice(h * pair, (h + 1) * pair)
        kcat[:, both] = jnp.where(entity == upper, keys[:, both], 0.0).astype(low)
    vt[...] = dot(r.v_weight[...], tok, 1, 1).astype(low)
    q_plain = dot(tok, wa[...], 1, 1)
    q_entity = dot(tok, wb[...], 1, 1)
    for h in range(heads):
        both = slice(h * pair, (h + 1) * pair)
        qcat[:, both] = jnp.where(entity, q_entity[:, both], q_plain[:, both]).astype(low)

    pt, mx, st = r.pt, r.mx, r.st
    scale = HD ** (-0.5)
    gathers = [
        LineGather(at, r.line_send.at[0], r.mx_recv.at[q], lambda block, q=q: mx[q].at[block])
        for q in range(len(spans))
    ]

    def pair_of(h):
        return pl.ds(pl.multiple_of(h * pair, pair), pair)

    def head_of(h):
        return pl.ds(pl.multiple_of(h * HD, HD), HD)

    def attend(q):
        start, size = spans[q]
        here = pl.ds(start, size)

        def head_step(h, carry):
            st[:, :size] = dot(kcat[:, pair_of(h)], qcat[here, pair_of(h)], 1, 1)

            def soften(i, carry):
                cols = pl.ds(pl.multiple_of(i * LANES, LANES), LANES)
                span = pl.ds(pl.multiple_of(start + i * LANES, LANES), LANES)
                scores = jnp.where(seg_wide[...] == r.seg_row[:, span], st[:, cols] * scale, -1000000000.0)
                shifted = jnp.exp(scores - jnp.max(scores, axis=0, keepdims=True))
                total = jnp.sum(shifted, axis=0, keepdims=True)
                pt[h, :, span] = (shifted * (1.0 / total)).astype(low)
                return carry

            lax.fori_loop(0, size // LANES, soften, 0, unroll=True)
            mixed = dot(vt[head_of(h), :], pt[h, :, here]).astype(low)
            mx[q][me, head_of(h), :] = mixed
            return carry

        lax.fori_loop(0, heads, head_step, 0, unroll=True)
        gathers[q].spread()

    def swap_plane():
        ow[me] = r.o_weight[...]
        for copy in ow_line:
            copy.wait_recv()
        for copy in ow_plane:
            copy.start()

    def swap_chip():
        for copy in ow_plane:
            copy.wait_recv()
        for copy in ow_chip:
            copy.start()

    def own_weights():
        for copy in ow_chip:
            copy.wait_recv()
        need("in_weight", "out_weight", "o_bias", "gain1", "shift1", "in_bias", "out_bias", "gain2", "shift2")
        for i, name in enumerate((r.o_bias, r.gain1, r.shift1, r.in_bias, r.out_bias, r.gain2, r.shift2)):
            vec[i, :] = name[...]

    tok_t, kct, vn = r.tok_t, r.kct, r.vn

    def turn():
        tok_t[...] = tokens[...].T
        kct[...] = kcat[...].T
        for h in range(heads):
            vn[h] = vt[h * HD : (h + 1) * HD, :].T

    xh1, rstd1, hl, mnat, mown, gbown = r.xh1, r.rstd1, r.hl, r.mnat, r.mown, r.gbown
    act, gp, dr2, gf, il, tmp, acc = r.act, r.gp, r.dr2, r.gf, r.il, r.tmp, r.acc
    acc[...] = jnp.zeros_like(acc)

    def make_lines(parts, send, part, out):
        lines = []
        for q, (start, size) in enumerate(spans):
            carry, single, summed, recv = parts[q]
            lines.append(LineReduce(at, part, carry, single, summed, send, recv, start, size // LINE, out))
        return lines

    ffn = make_lines(r.ffn, r.line_send.at[1], r.ffn_part, r.ffn_out)
    back = make_lines(r.back, r.line_send.at[2], r.back_part, r.back_part)
    swaps = [LineSwap(at, *parts) for parts in r.swap]
    grad = make_lines(r.grad, r.line_send.at[3], r.grad_part, r.tokens_grad)

    root_half = math.sqrt(0.5)
    density = 1.0 / math.sqrt(2.0 * math.pi)

    def forward(q):
        gathers[q].arrive()
        start, size = spans[q]
        here = pl.ds(start, size)
        mnat[:size, :] = mx[q][...].reshape(LINE * local_width, size).T
        tmp[:size, :] = dot(mnat[:size, :], ow[...].reshape(LINE * local_width, width))
        quarter_rows = size // LINE
        own = pl.ds(pl.multiple_of(me * quarter_rows, 16), quarter_rows)
        mown[start // LINE : (start + size) // LINE, :] = mnat[own, :]

        def first_norm(at_rows, inside):
            value = tmp[inside, :] + tokens[at_rows, :].astype(wide) + o_bias[...]
            centred = value - row_mean(value)
            scaled = lax.rsqrt(row_mean(centred * centred) + norm_epsilon)
            normal = centred * scaled
            xh1[at_rows, :] = normal
            rstd1[at_rows, :] = jnp.broadcast_to(scaled, (CHUNK, 128))
            hl[at_rows, :] = (normal * gain1[...] + shift1[...]).astype(low)

        rows_loop(start, size, first_norm)
        tmp[:size, :] = dot(hl[here, :], r.in_weight[...])

        def activate(at_rows, inside):
            inner = tmp[inside, :] + in_bias[...]
            gate = 0.5 + 0.5 * lax.erf(inner * root_half)
            act[at_rows, :] = (inner * gate).astype(low)
            gp[at_rows, :] = gate + inner * (density * jnp.exp(-0.5 * inner * inner))

        rows_loop(start, size, activate)
        r.ffn_part[here, :] = dot(act[here, :], r.out_weight[...]).astype(low)
        ffn[q].start()

    def backward(q):
        ffn[q].arrive()
        start, size = spans[q]
        here = pl.ds(start, size)

        def second_norm(at_rows, inside):
            value = xh1[at_rows, :] * gain1[...] + shift1[...]
            value = value + r.ffn_out[at_rows, :].astype(wide) + out_bias[...]
            centred = value - row_mean(value)
            scaled = lax.rsqrt(row_mean(centred * centred) + norm_epsilon)
            normal = centred * scaled
            r.layer_out[at_rows, :] = (normal * gain2[...] + shift2[...]).astype(low)
            cot = r.cotangent[at_rows, :].astype(wide)
            acc[6] += fold(cot)
            acc[5] += fold(cot * normal)
            grown = cot * gain2[...]
            grad_in = scaled * (grown - row_mean(grown) - normal * row_mean(grown * normal))
            acc[4] += fold(grad_in)
            dr2[at_rows, :] = grad_in
            gf[at_rows, :] = grad_in.astype(low)

        rows_loop(start, size, second_norm)
        tmp[:size, :] = dot(gf[here, :], r.out_weight[...], 1, 1)

        def inner_step(at_rows, inside):
            d_inner = tmp[inside, :] * gp[at_rows, :]
            acc[3] += fold(d_inner)
            il[at_rows, :] = d_inner.astype(low)

        rows_loop(start, size, inner_step)
        r.back_part[here, :] = dot(il[here, :], r.in_weight[...], 1, 1).astype(low)
        back[q].start()

    dqa, dqb, dkv, dk_sum, dv_sum = r.dqa, r.dqb, r.dkv, r.dk_sum, r.dv_sum
    dmt, ds = r.dmt, r.ds

    def settle_back(q):
        start, size = spans[q]
        own = back[q].rows_of(me)
        d_hidden = dr2[own, :] + back[q].total()
        normal = xh1[own, :]
        acc[2] += fold(d_hidden)
        acc[1] += fold(d_hidden * normal)
        grown = d_hidden * gain1[...]
        grad_in = rstd1[own, 0:1] * (grown - row_mean(grown) - normal * row_mean(grown * normal))
        acc[0] += fold(grad_in)
        dr2[own, :] = grad_in
        grad_low = grad_in.astype(low)
        gbown[start // LINE : (start + size) // LINE, :] = grad_low
        for j in range(LINE):
            swaps[q].sent[j] = dot(grad_low, ow[j], 1, 1).astype(low)
        swaps[q].start()

    def finish_rows(q):
        swaps[q].wait()
        start, size = spans[q]
        here = pl.ds(start, size)
        for h in range(heads):
            dmt[h, :size, :] = swaps[q].got[:, :, h * HD : (h + 1) * HD].reshape(size, HD)

        def head_step(h, carry):
            d_mixed = dmt[h, :size, :]
            st[:, :size] = dot(vn[h], d_mixed, 1, 1)

            def harden(i, carry):
                cols = pl.ds(pl.multiple_of(i * LANES, LANES), LANES)
                span = pl.ds(pl.multiple_of(start + i * LANES, LANES), LANES)
                prob = pt[h, :, span].astype(wide)
                d_prob = st[:, cols]
                delta = jnp.sum(prob * d_prob, axis=0, keepdims=True)
                ds[:, cols] = (prob * (d_prob - delta) * scale).astype(low)
                return carry

            lax.fori_loop(0, size // LANES, harden, 0, unroll=True)
            d_score = ds[:, :size]
            d_value = dot(pt[h, :, here], d_mixed)
            d_key = dot(d_score, qcat[here, pair_of(h)])
            if q == 0:
                dv_sum[h] = d_value
                dk_sum[h] = d_key
            else:
                dv_sum[h] += d_value
                dk_sum[h] += d_key
            d_query = dot(kct[pair_of(h), :], d_score).T
            row_entity = kind_wide[here, :] == 1
            dqa[here, pair_of(h)] = jnp.where(row_entity, 0.0, d_query).astype(low)
            dqb[here, pair_of(h)] = jnp.where(row_entity, d_query, 0.0).astype(low)
            return carry

        lax.fori_loop(0, heads, head_step, 0, unroll=True)

    gfeed, gattn = r.gfeed, r.gattn
    blocks, per_block = gfeed.shape[0], gfeed.shape[1]

    def put_grad(packed, start, value):
        packed[:, :, start : start + value.shape[1]] = value.astype(low).reshape(blocks, per_block, value.shape[1])

    if planar:
        feed = PlaneReduce(gfeed, *r.feed)
        attn = PlaneReduce(gattn, *r.attn)

    small = r.small
    if planar:
        small_sum = r.small_sum
        tiny = [
            remote(
                small if s == 0 else small_sum.at[s - 1],
                r.small_in.at[s],
                r.small_send.at[s],
                r.small_recv.at[s],
                dp=(across, over_x, over_y)[s],
            )
            for s in range(3)
        ]

    def tiny_step(s):
        if planar:
            tiny[s].wait_recv()
            small_sum[s] = (small if s == 0 else small_sum.at[s - 1])[...] + r.small_in[s]
            if s < 2:
                tiny[s + 1].start()

    norms = LineSwap(at, *r.norms)
    if planar:
        o_swap = LineSwap(at, *r.o_swap)

    def feed_step(i):
        if i == 0:
            put_grad(gfeed, hidden_width, dot(gf[...], act[...], 0, 0))
        elif i == 1:
            put_grad(gfeed, 0, dot(hl[...], il[...], 0, 0))
        elif planar and i == 2:
            feed.start()
        elif planar and i == 3:
            feed.step_one()
        elif planar and i == 4:
            feed.step_two()
        elif planar and i == 5:
            feed_sum = feed.finish()
            r.in_grad[...] = feed_sum[:, :hidden_width]
            r.out_grad[...] = feed_sum[:, hidden_width : 2 * hidden_width]
            for j in range(LINE):
                begin = 2 * hidden_width + j * local_width
                o_swap.sent[j] = feed_sum[:, begin : begin + local_width].astype(low)
            o_swap.start()
            stores["in_grad"].start()
            stores["out_grad"].start()

    def share_norms():
        for i in range(8):
            norms.sent[0, i : i + 1, :] = jnp.sum(acc[i], axis=0, keepdims=True)
        for j in range(1, LINE):
            norms.sent[j] = norms.sent[0]
        norms.start()
        put_grad(gfeed, 2 * hidden_width, dot(gbown[...], mown[...], 0, 0))

    def key_grads():
        norms.wait()
        small[...] = norms.sent[0]
        small[0:3, :] = norms.got[0, 0:3] + norms.got[1, 0:3] + norms.got[2, 0:3] + norms.got[3, 0:3]
        if planar:
            tiny[0].start()
        d_keys = [
            jnp.where(kind_wide[:, :HD] == 1, dk_sum[h, :, HD:], dk_sum[h, :, :HD]).astype(low)
            for h in range(heads)
        ]
        d_values = [dv_sum[h].astype(low) for h in range(heads)]
        dkv[...] = jnp.concatenate(d_keys + d_values, axis=1)

    def input_share(q):
        start, size = spans[q]
        here = pl.ds(start, size)
        share = dot(dqa[here, :], wa[...]) + dot(dqb[here, :], wb[...])
        share = share + dot(dkv[here, :local_width], r.k_weight[...]) + dot(dkv[here, local_width:], r.v_weight[...])
        r.grad_part[here, :] = share.astype(low)
        grad[q].start()

    def attn_step(i):
        if i == 0:
            put_grad(gattn, 0, dot(tok_t[...], dqa[...]))
            put_grad(gattn, 2 * local_width, dot(tok_t[...], dqb[...]))
        elif i == 1:
            put_grad(gattn, 4 * local_width, dot(tok_t[...], dkv[...]))
        elif planar and i == 2:
            attn.start()
            tiny_step(0)
        elif planar and i == 3:
            attn.step_one()
            tiny_step(1)
        elif planar and i == 4:
            attn.step_two()
            tiny_step(2)

    attend(0)
    attend(1)
    attend(2)
    attend(3)
    gathers[0].relay(0)
    gathers[2].relay(0)
    gathers[0].relay(1)
    gathers[1].relay(0)
    swap_plane()
    attend(4)
    gathers[1].relay(1)
    gathers[4].relay(0)
    gathers[3].relay(0)
    gathers[0].relay(2)
    gathers[2].relay(1)
    gathers[1].relay(2)
    swap_chip()
    gathers[2].relay(2)
    gathers[4].relay(1)
    gathers[4].relay(2)
    own_weights()
    forward(0)
    gathers[3].relay(1)
    ffn[0].forward(0)
    gathers[3].relay(2)
    forward(2)
    ffn[0].forward(1)
    ffn[2].forward(0)
    forward(1)
    ffn[0].settle()
    ffn[1].forward(0)
    forward(4)
    ffn[2].forward(1)
    ffn[1].forward(1)
    forward(3)
    ffn[0].relay(0)
    ffn[4].forward(0)
    ffn[4].forward(1)
    ffn[0].relay(1)
    ffn[1].settle()
    ffn[3].forward(0)
    ffn[3].forward(1)
    ffn[0].relay(2)
    ffn[1].relay(0)
    ffn[1].relay(1)
    ffn[4].settle()
    ffn[2].settle()
    turn()
    ffn[4].relay(0)
    ffn[1].relay(2)
    ffn[3].settle()
    ffn[2].relay(0)
    ffn[4].relay(1)
    need("cotangent")
    backward(0)
    ffn[3].relay(0)
    ffn[4].relay(2)
    ffn[2].relay(1)
    ffn[2].relay(2)
    ffn[3].relay(1)
    backward(1)
    back[0].forward(0)
    back[0].forward(1)
    ffn[3].relay(2)
    backward(4)
    back[1].forward(0)
    backward(2)
    back[1].forward(1)
    settle_back(0)
    backward(3)
    stores["layer_out"].start()
    back[4].forward(0)
    feed_step(0)
    back[2].forward(0)
    back[2].forward(1)
    settle_back(1)
    back[3].forward(0)
    feed_step(1)
    back[3].forward(1)
    back[4].forward(1)
    finish_rows(0)
    settle_back(2)
    settle_back(3)
    settle_back(4)
    share_norms()
    feed_step(2)
    finish_rows(1)
    finish_rows(2)
    finish_rows(3)
    finish_rows(4)
    key_grads()
    input_share(0)
    feed_step(3)
    input_share(1)
    input_share(2)
    grad[0].forward(0)
    input_share(3)
    input_share(4)
    grad[0].forward(1)
    attn_step(0)
    grad[1].forward(0)
    grad[1].forward(1)
    attn_step(1)
    attn_step(2)
    grad[0].settle(dr2)
    grad[2].forward(0)
    grad[2].forward(1)
    feed_step(4)
    grad[3].forward(0)
    grad[3].forward(1)
    grad[1].settle(dr2)
    attn_step(3)
    grad[4].forward(0)
    grad[2].settle(dr2)
    grad[4].forward(1)
    grad[3].settle(dr2)
    feed_step(5)
    grad[1].relay(0)
    grad[1].relay(1)
    grad[0].relay(0)
    grad[2].relay(0)
    grad[0].relay(1)
    grad[2].relay(1)
    grad[3].relay(0)
    grad[4].settle(dr2)
    grad[1].relay(2)
    grad[4].relay(0)
    grad[3].relay(1)
    grad[0].relay(2)
    attn_step(4)
    grad[3].relay(2)
    grad[4].relay(1)
    grad[4].relay(2)
    grad[2].relay(2)
    if planar:
        attn_sum = attn.finish()
        for part in range(4):
            base = (part // 2) * 2 * local_width + (part % 2) * HD
            r.q_grad[part] = jnp.concatenate(
                [attn_sum[:, base + h * pair : base + h * pair + HD] for h in range(heads)], axis=1
            )
        both_grads = attn_sum[:, 4 * local_width : 6 * local_width]
        r.k_grad[...] = both_grads[:, :local_width]
        r.v_grad[...] = both_grads[:, local_width:]
        o_swap.wait()
        o_sum = o_swap.got[0].astype(wide) + o_swap.got[1].astype(wide)
        r.o_grad[...] = (o_sum + o_swap.got[2].astype(wide) + o_swap.got[3].astype(wide)).T
        o_swap.drain()
        r.small_out[...] = small_sum[2]
        for name in ("q_grad", "k_grad", "v_grad", "o_grad", "small_out"):
            stores[name].start()
    else:
        r.small_out[...] = small[...]
        r.feed_out[...] = gfeed[...]
        r.attn_out[...] = gattn[...]
        for name in ("small_out", "feed_out", "attn_out"):
            stores[name].start()
    for line in grad:
        line.arrive()
    stores["tokens_grad"].start()

    def sent_all(i, held):
        remote(held, held, r.line_send.at[i], r.mx_recv.at[0, 0], mp=at.mid).wait_send()

    blocks_out = rows // LINE * 3

    @pl.when(at.is_end)
    def _():
        sent_all(0, vt)
        sent_all(1, hl)
        sent_all(2, hl.at[:blocks_out])
        sent_all(3, hl)

    @pl.when(at.is_mid)
    def _():
        sent_all(0, xh1.at[: 5 * rows * local_width // (2 * width)])
        sent_all(1, xh1)
        sent_all(2, hl.at[:blocks_out])
        sent_all(3, xh1)

    for swap in swaps + [norms]:
        swap.drain()
    for copy in ow_line + ow_plane + ow_chip:
        copy.wait_send()
    if planar:
        for copy in tiny:
            copy.wait_send()
    for copy in stores.values():
        copy.wait()


def hand_on(layout, *refs):
    sources, targets, held, lines, sems = jax.tree.unflatten(layout, refs)
    count = len(sources) - 1
    small = held[0]
    fetch = [pltpu.make_async_copy(source, kept, sems.at[0, i]) for i, (source, kept) in enumerate(zip(sources, held))]
    store = [
        pltpu.make_async_copy(kept, target, sems.at[1, i])
        for i, (kept, target) in enumerate(zip(list(held[1:]) + list(lines), targets))
    ]
    for copy in fetch:
        copy.start()
    fetch[0].wait()
    for i, line in enumerate(lines):
        line[...] = small[i, :]
        store[count + i].start()
    for i in range(count):
        fetch[1 + i].wait()
        store[i].start()
    for copy in store:
        copy.wait()


def local(
    tokens,
    segment_ids,
    token_types,
    q_weight,
    k_weight,
    v_weight,
    o_weight,
    o_bias,
    norm1_gain,
    norm1_shift,
    in_weight,
    in_bias,
    out_weight,
    out_bias,
    norm2_gain,
    norm2_shift,
    cotangent,
):
    rows, width = tokens.shape
    local_width = k_weight.shape[1]
    heads = local_width // HD
    hidden_width = in_weight.shape[1]
    n_dp = lax.axis_size("dp")
    planar = n_dp == 8
    blocks = 8
    per_block = width // blocks
    spans = portions_of(rows)
    largest = max(size for _, size in spans)
    low, wide = jnp.bfloat16, jnp.float32
    attn_width = 6 * local_width
    feed_width = 2 * hidden_width + LINE * local_width
    args = dict(
        tokens=tokens,
        seg_row=segment_ids,
        kind_row=token_types,
        q_weight=q_weight.swapaxes(1, 2),
        k_weight=k_weight.T,
        v_weight=v_weight.T,
        o_weight=o_weight,
        o_bias=o_bias,
        gain1=norm1_gain,
        shift1=norm1_shift,
        in_bias=in_bias,
        out_bias=out_bias,
        gain2=norm2_gain,
        shift2=norm2_shift,
        in_weight=in_weight,
        out_weight=out_weight,
        cotangent=cotangent,
    )
    shaped = jax.ShapeDtypeStruct
    outs = dict(
        layer_out=shaped((rows, width), low),
        tokens_grad=shaped((rows, width), low),
        small_out=shaped((8, width), wide),
    )
    if planar:
        outs |= dict(
            q_grad=shaped((4, per_block, local_width), wide),
            k_grad=shaped((per_block, local_width), wide),
            v_grad=shaped((per_block, local_width), wide),
            o_grad=shaped((local_width, per_block), wide),
            in_grad=shaped((per_block, hidden_width), wide),
            out_grad=shaped((per_block, hidden_width), wide),
        )
    else:
        outs |= dict(
            feed_out=shaped((blocks, per_block, feed_width), low),
            attn_out=shaped((blocks, per_block, attn_width), low),
        )
    dma = pltpu.SemaphoreType.DMA
    scratch = dict(
        ow=pltpu.VMEM((LINE, local_width, width), low),
        ow_send=dma((9,)),
        ow_recv=dma((9,)),
        wa=pltpu.VMEM((2 * local_width, width), low),
        wb=pltpu.VMEM((2 * local_width, width), low),
        wk=pltpu.VMEM((2 * local_width, width), low),
        kind_wide=pltpu.VMEM((rows, 2 * HD), jnp.int32),
        seg_wide=pltpu.VMEM((rows, 2 * HD), jnp.int32),
        qcat=pltpu.VMEM((rows, 2 * local_width), low),
        kcat=pltpu.VMEM((rows, 2 * local_width), low),
        vt=pltpu.VMEM((local_width, rows), low),
        pt=pltpu.VMEM((heads, rows, rows), low),
        mx=[pltpu.VMEM((LINE, local_width, size), low) for _, size in spans],
        st=pltpu.VMEM((rows, largest), wide),
        ds=pltpu.VMEM((rows, largest), low),
        line_send=dma((4,)),
        mx_recv=dma((len(spans), LINE)),
        tok_t=pltpu.VMEM((width, rows), low),
        xh1=pltpu.VMEM((rows, width), wide),
        rstd1=pltpu.VMEM((rows, 128), wide),
        hl=pltpu.VMEM((rows, width), low),
        act=pltpu.VMEM((rows, hidden_width), low),
        gp=pltpu.VMEM((rows, hidden_width), wide),
        dr2=pltpu.VMEM((rows, width), wide),
        gf=pltpu.VMEM((rows, width), low),
        il=pltpu.VMEM((rows, hidden_width), low),
        tmp=pltpu.VMEM((largest, width), wide),
        vec=pltpu.VMEM((8, width), wide),
        acc=pltpu.VMEM((8, 8, width), wide),
        mnat=pltpu.VMEM((largest, LINE * local_width), low),
        mown=pltpu.VMEM((rows // LINE, LINE * local_width), low),
        gbown=pltpu.VMEM((rows // LINE, width), low),
        swap=[swap_scratch(size // LINE, local_width, low) for _, size in spans],
        norms=swap_scratch(8, width, wide),
        ffn_part=pltpu.VMEM((rows, width), low),
        back_part=pltpu.VMEM((rows, width), low),
        grad_part=pltpu.VMEM((rows, width), low),
        ffn_out=pltpu.VMEM((rows, width), low),
        gfeed=pltpu.VMEM((blocks, per_block, feed_width), low),
        gattn=pltpu.VMEM((blocks, per_block, attn_width), low),
        small=pltpu.VMEM((8, width), wide),
        kct=pltpu.VMEM((2 * local_width, rows), low),
        vn=pltpu.VMEM((heads, rows, HD), low),
        dmt=pltpu.VMEM((heads, largest, HD), low),
        dk_sum=pltpu.VMEM((heads, rows, 2 * HD), wide),
        dv_sum=pltpu.VMEM((heads, rows, HD), wide),
        dqa=pltpu.VMEM((rows, 2 * local_width), low),
        dqb=pltpu.VMEM((rows, 2 * local_width), low),
        dkv=pltpu.VMEM((rows, 2 * local_width), low),
    )
    for name in ("ffn", "back", "grad"):
        scratch[name] = [line_scratch(size // LINE, width) for _, size in spans]
    if planar:
        scratch |= dict(
            feed=plane_scratch(per_block, feed_width),
            o_swap=swap_scratch(per_block, local_width, low),
            attn=plane_scratch(per_block, attn_width),
            small_in=pltpu.VMEM((3, 8, width), wide),
            small_sum=pltpu.VMEM((3, 8, width), wide),
            small_send=dma((3,)),
            small_recv=dma((3,)),
        )
    scratch |= dict(
        held={name: pltpu.VMEM(a.shape, a.dtype) for name, a in args.items()},
        made={name: pltpu.VMEM(a.shape, a.dtype) for name, a in outs.items()},
        load_sem=dma((len(args),)),
        store_sem=dma((len(outs),)),
    )
    layout = jax.tree.structure((args, outs, scratch))
    vm, far = pl.BlockSpec(memory_space=pltpu.VMEM), pl.BlockSpec(memory_space=pl.ANY)
    results = pl.pallas_call(
        functools.partial(layer_kernel, planar, layout),
        out_shape=jax.tree.leaves(outs),
        in_specs=[far] * len(args),
        out_specs=[far] * len(outs),
        scratch_shapes=jax.tree.leaves(scratch),
        compiler_params=pltpu.CompilerParams(
            collective_id=0, has_side_effects=True, vmem_limit_bytes=VMEM_LIMIT
        ),
    )(*jax.tree.leaves(args))
    results = dict(zip(sorted(outs), results))
    if planar:
        small = results.pop("small_out")
        flat, tree = jax.tree.flatten(results)
        vectors = small.shape[0] - 1
        line = (width,)
        targets = [shaped(a.shape, a.dtype) for a in flat] + [shaped(line, wide)] * vectors
        held = [pltpu.VMEM(a.shape, a.dtype) for a in [small] + flat]
        lines = [pltpu.VMEM(line, wide)] * vectors
        sems = dma((2, len(targets)))
        pieces = ([small] + flat, targets, held, lines, sems)
        flat = pl.pallas_call(
            functools.partial(hand_on, jax.tree.structure(pieces)),
            out_shape=targets,
            in_specs=[far] * (1 + len(flat)),
            out_specs=[far] * len(targets),
            scratch_shapes=held + lines + [sems],
            compiler_params=pltpu.CompilerParams(vmem_limit_bytes=VMEM_LIMIT),
        )(small, *flat)
        small = flat[len(results) :]
        results = jax.tree.unflatten(tree, flat[: len(results)])
    res = types.SimpleNamespace(**results)
    if planar:
        grads = (res.q_grad, res.k_grad, res.v_grad, res.o_grad, res.in_grad, res.out_grad.T)
    else:
        feed = res.feed_out.astype(wide).reshape(width, feed_width)
        attn = res.attn_out.astype(wide).reshape(width, attn_width)
        feed = lax.psum_scatter(feed, "dp", scatter_dimension=0, tiled=True)
        attn = lax.psum_scatter(attn, "dp", scatter_dimension=0, tiled=True)
        small = lax.psum(res.small_out, "dp")
        per = feed.shape[0]
        o_part = lax.psum_scatter(feed[:, 2 * hidden_width :], "mp", scatter_dimension=1, tiled=True)
        queries = attn[:, : 4 * local_width].reshape(per, 2, heads, 2, HD)
        queries = queries.transpose(1, 3, 0, 2, 4).reshape(4, per, local_width)
        grads = (
            queries,
            attn[:, 4 * local_width : 5 * local_width],
            attn[:, 5 * local_width : 6 * local_width],
            o_part.T,
            feed[:, :hidden_width],
            feed[:, hidden_width : 2 * hidden_width].T,
        )
    d_q, d_k, d_v, d_o, d_in, d_out = grads
    return (
        res.layer_out,
        res.tokens_grad,
        d_q,
        d_k,
        d_v,
        d_o,
        small[0],
        small[1],
        small[2],
        d_in,
        small[3],
        d_out,
        small[4],
        small[5],
        small[6],
    )


def solution(mesh):
    return jax.shard_map(
        local,
        mesh=mesh,
        in_specs=(
            P("dp", None),
            P("dp", None),
            P("dp", None),
            P(None, None, "mp"),
            P(None, "mp"),
            P(None, "mp"),
            P("mp", None),
            P(),
            P(),
            P(),
            P(None, "mp"),
            P("mp"),
            P("mp", None),
            P(),
            P(),
            P(),
            P("dp", None),
        ),
        out_specs=(
            P("dp", None),
            P("dp", None),
            P(None, "dp", "mp"),
            P("dp", "mp"),
            P("dp", "mp"),
            P("mp", "dp"),
            P(),
            P(),
            P(),
            P("dp", "mp"),
            P("mp"),
            P("mp", "dp"),
            P(),
            P(),
            P(),
        ),
        check_vma=False,
    )
```
